8 devices in a mesh: dp: 1 (over z), tp: 8 (over x, y, core).
Axes of the slice: x: 2, y: 2, z: 1, core: 2. Of those that a mesh axis runs over, the one named last changes fastest.
Arguments:
- x: bfloat16 [4096, 2048], P(('dp', 'tp'))
- dy: bfloat16 [4096, 2048], P(('dp', 'tp'))
- gate: bfloat16 [4096, 5120], P('dp', 'tp')
- up: bfloat16 [4096, 5120], P('dp', 'tp')
- w_gate: bfloat16 [2048, 5120], P(None, 'tp')
- w_up: bfloat16 [2048, 5120], P(None, 'tp')
- w_down: bfloat16 [5120, 2048], P('tp')
Outputs:
- output 1: bfloat16 [4096, 2048], P(('dp', 'tp'))
- output 2: bfloat16 [2048, 5120], P('dp', 'tp')
- output 3: bfloat16 [2048, 5120], P('dp', 'tp')
- output 4: bfloat16 [5120, 2048], P(('dp', 'tp'))
All inputs are finite; a program needn't handle non-finite values.
Results may differ from the reference program's by a relative error of at most 0.012.
Values are sent between devices in bfloat16 or wider.
A program may use at most 2 GiB of HBM per device.

```python
import jax
import jax.numpy as jnp

ROWS = 4096
D = 2048
FF = 5120


def act(gate, up):
    return jax.nn.gelu(gate) * up


def setup_inputs(seed: int = 0, part: int = 0) -> dict:
    kx, ky, ka, kb, kg, ku, kd = jax.random.split(jax.random.key(seed), 7)
    kx, ky, ka, kb = (jax.random.fold_in(k, part) for k in (kx, ky, ka, kb))
    drawn = {
        "x": jax.random.normal(kx, (ROWS, D), jnp.float32),
        "dy": jax.random.normal(ky, (ROWS, D), jnp.float32),
        "gate": jax.random.normal(ka, (ROWS, FF), jnp.float32),
        "up": jax.random.normal(kb, (ROWS, FF), jnp.float32),
        "w_gate": jax.random.normal(kg, (D, FF), jnp.float32) * D**-0.5,
        "w_up": jax.random.normal(ku, (D, FF), jnp.float32) * D**-0.5,
        "w_down": jax.random.normal(kd, (FF, D), jnp.float32) * FF**-0.5,
    }
    return {k: v.astype(jnp.bfloat16) for k, v in drawn.items()}


def reference(x, dy, gate, up, w_gate, w_up, w_down):
    hidden, back = jax.vjp(act, gate.astype(jnp.float32), up.astype(jnp.float32))
    d_hidden = jnp.dot(dy, w_down.T, preferred_element_type=jnp.float32)
    d_gate, d_up = (g.astype(jnp.bfloat16) for g in back(d_hidden))
    dx = jnp.dot(d_gate, w_gate.T, preferred_element_type=jnp.float32) + jnp.dot(d_up, w_up.T, preferred_element_type=jnp.float32)
    dw_gate = jnp.dot(x.T, d_gate, preferred_element_type=jnp.float32)
    dw_up = jnp.dot(x.T, d_up, preferred_element_type=jnp.float32)
    dw_down = jnp.dot(hidden.astype(jnp.bfloat16).T, dy, preferred_element_type=jnp.float32)
    return tuple(g.astype(jnp.bfloat16) for g in (dx, dw_gate, dw_up, dw_down))
```

```python
import functools

import jax
import jax.numpy as jnp
from jax import lax
from jax.experimental import pallas as pl
from jax.experimental.pallas import tpu as pltpu
from jax.sharding import PartitionSpec as P

D = 2048
F = 640
B = 512
H = 256
F32 = jnp.float32
BF16 = jnp.bfloat16
NT = (((1,), (1,)), ((), ()))
TN = (((0,), (0,)), ((), ()))
C0 = 0.7978845608028654
C1 = 0.7978845608028654 * 0.044715


def kernel(
    x_ref, dy_ref, gate_ref, up_ref, wg_ref, wu_ref, wd_ref,
    dx_ref, dwg_ref, dwu_ref, dwd_ref, dy_all, x_all, rs_in,
    wd, wgu, dgu, dwd_acc, dwgu_acc, own, tok, gv, uv, dh, hid, p_in, p_out, rs_out,
    dy_ss, dy_rs, dyp_ss, dyp_rs, x_ss, x_rs, xp_ss, xp_rs, p_ss, p_rs, r_ss, r_rs, w_sem, t_sem, g_sem, o_sem,
):
    me = lax.axis_index("tp")
    core, iy, ix = me % 2, (me // 2) % 2, me // 4
    other = 1 - 2 * core
    partner = me + other
    ny = me + 2 - 4 * iy
    nx = me + 4 - 8 * ix
    nd = ny + 4 - 8 * ix

    barrier = pltpu.get_barrier_semaphore()
    for d in (partner, nx, ny):
        pl.semaphore_signal(barrier, inc=1, device_id={"tp": d}, device_id_type=pl.DeviceIdType.MESH)
    pl.semaphore_wait(barrier, 3)

    def owner(g):
        return jnp.where(g < 2, me, jnp.where(g >= 6, nd, jnp.where(g % 2 == 0, nx, ny)))

    def half(g):
        return jnp.where(g == 4, 1, jnp.where(g == 5, 0, g % 2))

    def rows(dev, h):
        return pl.ds(pl.multiple_of(dev * B + h * H, H), H)

    def remote(src, dst, ss, rs, dev):
        return pltpu.make_async_remote_copy(
            src_ref=src, dst_ref=dst, send_sem=ss, recv_sem=rs, device_id={"tp": dev}, device_id_type=pl.DeviceIdType.MESH
        )

    def send_own(ref, full, ss, rs, h, g, dev):
        return remote(ref.at[pl.ds(h * H, H)], full.at[rows(me, h)], ss.at[g], rs.at[g], dev)

    def send_on(full, ss, rs, g_in, g_out, dev):
        r = rows(owner(g_in), half(g_in))
        return remote(full.at[r], full.at[r], ss.at[g_out], rs.at[g_out], dev)

    def start_own(ref, full, ss, rs, pss, prs):
        send_own(ref, full, ss, rs, 0, 2, nx).start()
        send_own(ref, full, ss, rs, 1, 3, ny).start()
        send_own(ref, full, pss, prs, 0, 0, partner).start()
        send_own(ref, full, ss, rs, 1, 4, nx).start()
        send_own(ref, full, ss, rs, 0, 5, ny).start()
        send_own(ref, full, pss, prs, 1, 1, partner).start()

    def arrived(full, ss, rs, g):
        send_on(full, ss, rs, g, g, partner).wait_recv()

    def relay(full, ss, rs, pss, prs, g, onward):
        arrived(full, ss, rs, g)
        if onward == "y":
            send_on(full, ss, rs, g, 6, ny).start()
        if onward == "x":
            send_on(full, ss, rs, g, 7, nx).start()
        send_on(full, pss, prs, g, g, partner).start()

    def load_tokens(ref, full, g):
        o, h = owner(g), half(g)
        p = pltpu.make_async_copy(full.at[rows(o + other, h)], tok.at[pl.ds(0, H)], t_sem.at[0])
        p.start()

        @pl.when(g < 2)
        def _():
            pltpu.make_async_copy(ref.at[pl.ds(pl.multiple_of(h * H, H), H)], tok.at[pl.ds(H, H)], t_sem.at[1]).start()

        @pl.when(g >= 2)
        def _():
            pltpu.make_async_copy(full.at[rows(o, h)], tok.at[pl.ds(H, H)], t_sem.at[1]).start()

        p.wait()
        pltpu.make_async_copy(full.at[rows(o, h)], tok.at[pl.ds(H, H)], t_sem.at[1]).wait()

    def gate_copies(g):
        o, h = owner(g), half(g)
        for i, (src, dst) in enumerate(((gate_ref, gv), (up_ref, uv))):
            yield pltpu.make_async_copy(src.at[rows(o + other, h)], dst.at[pl.ds(0, H)], g_sem.at[2 * i])
            yield pltpu.make_async_copy(src.at[rows(o, h)], dst.at[pl.ds(H, H)], g_sem.at[2 * i + 1])

    start_own(dy_ref, dy_all, dy_ss, dy_rs, dyp_ss, dyp_rs)
    weights = (
        pltpu.make_async_copy(wd_ref, wd, w_sem.at[0]),
        pltpu.make_async_copy(wg_ref, wgu.at[:, pl.ds(0, F)], w_sem.at[1]),
        pltpu.make_async_copy(wu_ref, wgu.at[:, pl.ds(F, F)], w_sem.at[2]),
    )
    for w in weights:
        w.start()
    for c in gate_copies(0):
        c.start()
    dwd_acc[...] = jnp.zeros_like(dwd_acc)
    dwgu_acc[...] = jnp.zeros_like(dwgu_acc)
    for w in weights:
        w.wait()

    def send_p(g):
        return remote(p_out.at[g % 2], p_in.at[g], p_ss.at[g], p_rs.at[g], partner)

    def send_r(stage, slot, dev):
        return remote(rs_out.at[stage], rs_in.at[slot], r_ss.at[slot], r_rs.at[slot], dev)

    def dx_tile(g, r0, j):
        a = dgu[pl.ds(pl.multiple_of(g * B + r0, H), H), :]
        w = wgu[pl.ds(pl.multiple_of(j * 512, 512), 512), :]
        return lax.dot_general(a, w, NT, preferred_element_type=F32)

    def first_pass(g, carry):
        @pl.when(g == 2)
        def _():
            relay(dy_all, dy_ss, dy_rs, dyp_ss, dyp_rs, 2, "y")
            relay(dy_all, dy_ss, dy_rs, dyp_ss, dyp_rs, 3, "x")
            start_own(x_ref, x_all, x_ss, x_rs, xp_ss, xp_rs)

        for k in (4, 6):
            @pl.when(g == k)
            def _():
                relay(dy_all, dy_ss, dy_rs, dyp_ss, dyp_rs, k, None)
                relay(dy_all, dy_ss, dy_rs, dyp_ss, dyp_rs, k + 1, None)

        arrived(dy_all, dyp_ss, dyp_rs, g)
        load_tokens(dy_ref, dy_all, g)
        for c in gate_copies(g):
            c.wait()

        for n0, n in ((0, 256), (256, 256), (512, 128)):
            dh[:, n0:n0 + n] = lax.dot_general(tok[...], wd[n0:n0 + n, :], NT, preferred_element_type=F32)

        def gates(i, carry):
            r = pl.ds(pl.multiple_of(i * 32, 32), 32)
            a, u, d = gv[r, :].astype(F32), uv[r, :].astype(F32), dh[r, :]
            a2 = a * a
            t = jnp.tanh(a * (C0 + C1 * a2))
            cdf = 0.5 + 0.5 * t
            gelu = a * cdf
            slope = cdf + (0.5 * a) * ((1.0 - t * t) * (C0 + (3.0 * C1) * a2))
            hid[r, :] = (gelu * u).astype(BF16)
            q = pl.ds(pl.multiple_of(g * B + i * 32, 32), 32)
            dgu[q, 0:F] = (d * u * slope).astype(BF16)
            dgu[q, F:2 * F] = (d * gelu).astype(BF16)
            return carry

        lax.fori_loop(0, B // 32, gates, 0)

        @pl.when(g < 7)
        def _():
            for c in gate_copies(g + 1):
                c.start()

        @pl.when(g >= 2)
        def _():
            send_p(g - 2).wait_send()

        def p_rows(j, carry):
            p_out[g % 2, :, pl.ds(pl.multiple_of(j * 512, 512), 512)] = dx_tile(g, 0, j).astype(BF16)
            return carry

        lax.fori_loop(0, 4, p_rows, 0)
        send_p(g).start()

        def down(j, carry):
            s = pl.ds(pl.multiple_of(j * 512, 512), 512)
            dwd_acc[:, s] += lax.dot_general(hid[...], tok[:, s], TN, preferred_element_type=F32)
            return carry

        lax.fori_loop(0, 4, down, 0)

        send_p(g).wait_recv()

        @pl.when(jnp.logical_or(g < 4, g >= 6))
        def _():
            stage = jnp.where(g >= 6, g - 4, g % 2)

            def m_rows(j, carry):
                s = pl.ds(pl.multiple_of(j * 512, 512), 512)
                total = dx_tile(g, H, j) + p_in[g, :, s].astype(F32)

                @pl.when(g < 2)
                def _():
                    own[pl.ds(pl.multiple_of((g % 2) * H, H), H), s] = total

                @pl.when(g >= 2)
                def _():
                    rs_out[stage, :, s] = total.astype(BF16)

                return carry

            lax.fori_loop(0, 4, m_rows, 0)

        @pl.when(g == 2)
        def _():
            send_r(0, 2, nx).start()

        @pl.when(g == 3)
        def _():
            send_r(1, 3, ny).start()

        @pl.when(g == 6)
        def _():
            send_r(2, 0, nx).start()

        @pl.when(g == 7)
        def _():
            send_r(3, 1, ny).start()

        return carry

    lax.fori_loop(0, 8, first_pass, 0)

    def down_out(k, carry):
        for i in range(5):
            p_in[i // 2, (i % 2) * 128:(i % 2) * 128 + 128, pl.ds(pl.multiple_of(k * 256, 256), 256)] = dwd_acc[
                i * 128:i * 128 + 128, pl.ds(pl.multiple_of(k * 256, 256), 256)
            ].astype(BF16)
        return carry

    lax.fori_loop(0, 8, down_out, 0)
    down_copies = [
        pltpu.make_async_copy(p_in.at[i, pl.ds(0, n)], dwd_ref.at[pl.ds(i * H, n)], o_sem.at[i])
        for i, n in enumerate((H, H, 128))
    ]
    for c in down_copies:
        c.start()

    relay(x_all, x_ss, x_rs, xp_ss, xp_rs, 2, "y")
    relay(x_all, x_ss, x_rs, xp_ss, xp_rs, 3, "x")

    def fetch(slot, k):
        c = pltpu.make_async_copy(rs_in.at[slot], tok.at[pl.ds(k * H, H)], t_sem.at[k])
        c.start()
        return c

    def add_own(pairs):
        for slot, h in pairs:
            send_r(0, slot, nx).wait_recv()
            fetch(slot, h).wait()

    def second_pass(g, carry):
        @pl.when(g == 4)
        def _():
            relay(x_all, x_ss, x_rs, xp_ss, xp_rs, 4, None)
            relay(x_all, x_ss, x_rs, xp_ss, xp_rs, 5, None)

        @pl.when(g == 6)
        def _():
            add_own(((2, 0), (3, 1)))

            def add(i, carry):
                r = pl.ds(pl.multiple_of(i * 32, 32), 32)
                own[r, :] += tok[r, :].astype(F32)
                return carry

            lax.fori_loop(0, B // 32, add, 0)

            send_r(0, 2, nx).wait_send()
            send_r(1, 3, ny).wait_send()
            for group, slot, k in ((4, 1, 0), (5, 0, 1)):
                send_r(0, slot, nx).wait_recv()
                fetch(slot, k).wait()

                def late(j, carry):
                    s = pl.ds(pl.multiple_of(j * 512, 512), 512)
                    total = dx_tile(group, H, j) + p_in[group, :, s].astype(F32) + tok[k * H:(k + 1) * H, s].astype(F32)
                    rs_out[k, :, s] = total.astype(BF16)
                    return carry

                lax.fori_loop(0, 4, late, 0)
                send_r(k, 4 + k, (nx, ny)[k]).start()

            relay(x_all, x_ss, x_rs, xp_ss, xp_rs, 6, None)
            relay(x_all, x_ss, x_rs, xp_ss, xp_rs, 7, None)

        arrived(x_all, xp_ss, xp_rs, g)
        load_tokens(x_ref, x_all, g)

        def weight(j, carry):
            s = pl.ds(pl.multiple_of(j * 512, 512), 512)
            d = dgu[pl.ds(pl.multiple_of(g * B, B), B), :]
            dwgu_acc[s, :] += lax.dot_general(tok[:, s], d, TN, preferred_element_type=F32)
            return carry

        lax.fori_loop(0, 4, weight, 0)
        return carry

    lax.fori_loop(0, 8, second_pass, 0)

    def weight_out(i, carry):
        r = pl.ds(pl.multiple_of(i * 32, 32), 32)
        dgu[r, :] = dwgu_acc[r, :].astype(BF16)
        return carry

    lax.fori_loop(0, D // 32, weight_out, 0)
    weight_copies = (
        pltpu.make_async_copy(dgu.at[pl.ds(0, D), pl.ds(0, F)], dwg_ref, o_sem.at[3]),
        pltpu.make_async_copy(dgu.at[pl.ds(0, D), pl.ds(F, F)], dwu_ref, o_sem.at[4]),
    )
    for c in weight_copies:
        c.start()

    add_own(((5, 0), (4, 1)))

    def finish(i, carry):
        r = pl.ds(pl.multiple_of(i * 32, 32), 32)
        tok[r, :] = (own[r, :] + tok[r, :].astype(F32)).astype(BF16)
        return carry

    lax.fori_loop(0, B // 32, finish, 0)
    out = pltpu.make_async_copy(tok, dx_ref, o_sem.at[5])
    out.start()

    for c in down_copies + list(weight_copies) + [out]:
        c.wait()
    for full, ss, rs, pss, prs in ((dy_all, dy_ss, dy_rs, dyp_ss, dyp_rs), (x_all, x_ss, x_rs, xp_ss, xp_rs)):
        for g in range(8):
            send_on(full, pss, prs, g, g, partner).wait_send()
            if g >= 2:
                send_on(full, ss, rs, g, g, partner).wait_send()
    for g in (6, 7):
        send_p(g).wait_send()
    for stage, slot in ((2, 0), (3, 1), (0, 4), (1, 5)):
        send_r(stage, slot, nx).wait_send()


def solution(mesh):
    def local(*args):
        any_ = pl.BlockSpec(memory_space=pl.ANY)
        dma = pltpu.SemaphoreType.DMA
        shapes = [(B, D), (D, F), (D, F), (F, D), (8 * B, D), (8 * B, D), (6, H, D)]
        outs = pl.pallas_call(
            kernel,
            out_shape=[jax.ShapeDtypeStruct(s, BF16) for s in shapes],
            in_specs=[any_] * 7,
            out_specs=[any_] * 7,
            scratch_shapes=[
                pltpu.VMEM((F, D), BF16),
                pltpu.VMEM((D, 2 * F), BF16),
                pltpu.VMEM((8 * B, 2 * F), BF16),
                pltpu.VMEM((F, D), F32),
                pltpu.VMEM((D, 2 * F), F32),
                pltpu.VMEM((B, D), F32),
                pltpu.VMEM((B, D), BF16),
                pltpu.VMEM((B, F), BF16),
                pltpu.VMEM((B, F), BF16),
                pltpu.VMEM((B, F), F32),
                pltpu.VMEM((B, F), BF16),
                pltpu.VMEM((8, H, D), BF16),
                pltpu.VMEM((2, H, D), BF16),
                pltpu.VMEM((4, H, D), BF16),
            ]
            + [dma((8,))] * 12
            + [dma((3,)), dma((2,)), dma((4,)), dma((6,))],
            compiler_params=pltpu.CompilerParams(collective_id=0, has_side_effects=True, vmem_limit_bytes=67043328),
            name="backward",
        )(*args)
        return tuple(outs[:4])

    rows, cols = P(("dp", "tp"), None), P("dp", "tp")
    return jax.shard_map(
        local,
        mesh=mesh,
        in_specs=(rows, rows, cols, cols, P(None, "tp"), P(None, "tp"), P("tp", None)),
        out_specs=(rows, cols, cols, rows),
        check_vma=False,
    )
```

```python
import functools

import jax
import jax.numpy as jnp
from jax import lax
from jax.experimental import pallas as pl
from jax.experimental.pallas import tpu as pltpu
from jax.sharding import PartitionSpec as P

D = 2048
F = 640
B = 512
H = 256
LAST = 128
F32 = jnp.float32
BF16 = jnp.bfloat16
NT = (((1,), (1,)), ((), ()))
TN = (((0,), (0,)), ((), ()))
C0 = 0.7978845608028654
C1 = 0.7978845608028654 * 0.044715


def kernel(
    x_ref, dy_ref, gate_ref, up_ref, wg_ref, wu_ref, wd_ref,
    dx_ref, dwg_ref, dwu_ref, dwd_ref, dy_all, x_all, rs_in,
    wd, wgu, dgu, acc, own, tok, gv, uv, dh, hid, p_in, p_out, rs_out, last,
    dy_ss, dy_rs, dyp_ss, dyp_rs, x_ss, x_rs, xp_ss, xp_rs, p_ss, p_rs, r_ss, r_rs, l_ss, l_rs, w_sem, t_sem, g_sem,
):
    me = lax.axis_index("tp")
    core, iy, ix = me % 2, (me // 2) % 2, me // 4
    other = 1 - 2 * core
    partner = me + other
    ny = me + 2 - 4 * iy
    nx = me + 4 - 8 * ix
    nd = ny + 4 - 8 * ix

    barrier = pltpu.get_barrier_semaphore()
    for d in (partner, nx, ny):
        pl.semaphore_signal(barrier, inc=1, device_id={"tp": d}, device_id_type=pl.DeviceIdType.MESH)
    pl.semaphore_wait(barrier, 3)

    def owner(g):
        return jnp.where(g < 2, me, jnp.where(g >= 6, nd, jnp.where(g % 2 == 0, nx, ny)))

    def half(g):
        return jnp.where(g == 4, 1, jnp.where(g == 5, 0, g % 2))

    def rows(dev, h):
        return pl.ds(pl.multiple_of(dev * B + h * H, H), H)

    def remote(src, dst, ss, rs, dev):
        return pltpu.make_async_remote_copy(
            src_ref=src, dst_ref=dst, send_sem=ss, recv_sem=rs, device_id={"tp": dev}, device_id_type=pl.DeviceIdType.MESH
        )

    def send_own(ref, full, ss, rs, h, g, dev):
        return remote(ref.at[pl.ds(h * H, H)], full.at[rows(me, h)], ss.at[g], rs.at[g], dev)

    def send_on(full, ss, rs, g_in, g_out, dev):
        r = rows(owner(g_in), half(g_in))
        return remote(full.at[r], full.at[r], ss.at[g_out], rs.at[g_out], dev)

    def start_own(ref, full, ss, rs, pss, prs):
        send_own(ref, full, ss, rs, 0, 2, nx).start()
        send_own(ref, full, ss, rs, 1, 3, ny).start()
        send_own(ref, full, pss, prs, 0, 0, partner).start()
        send_own(ref, full, ss, rs, 1, 4, nx).start()
        send_own(ref, full, ss, rs, 0, 5, ny).start()
        send_own(ref, full, pss, prs, 1, 1, partner).start()

    def arrived(full, ss, rs, g):
        send_on(full, ss, rs, g, g, partner).wait_recv()

    def relay(full, ss, rs, pss, prs, g, onward):
        arrived(full, ss, rs, g)
        if onward == "y":
            send_on(full, ss, rs, g, 6, ny).start()
        if onward == "x":
            send_on(full, ss, rs, g, 7, nx).start()
        send_on(full, pss, prs, g, g, partner).start()

    def load_tokens(ref, full, g):
        o, h = owner(g), half(g)
        p = pltpu.make_async_copy(full.at[rows(o + other, h)], tok.at[pl.ds(0, H)], t_sem.at[0])
        p.start()

        @pl.when(g < 2)
        def _():
            pltpu.make_async_copy(ref.at[pl.ds(pl.multiple_of(h * H, H), H)], tok.at[pl.ds(H, H)], t_sem.at[1]).start()

        @pl.when(g >= 2)
        def _():
            pltpu.make_async_copy(full.at[rows(o, h)], tok.at[pl.ds(H, H)], t_sem.at[1]).start()

        p.wait()
        pltpu.make_async_copy(full.at[rows(o, h)], tok.at[pl.ds(H, H)], t_sem.at[1]).wait()

    def gate_copies(g):
        o, h = owner(g), half(g)
        for i, (src, dst) in enumerate(((gate_ref, gv), (up_ref, uv))):
            yield pltpu.make_async_copy(src.at[rows(o + other, h)], dst.at[pl.ds(0, H)], g_sem.at[2 * i])
            yield pltpu.make_async_copy(src.at[rows(o, h)], dst.at[pl.ds(H, H)], g_sem.at[2 * i + 1])

    start_own(dy_ref, dy_all, dy_ss, dy_rs, dyp_ss, dyp_rs)
    weights = (
        pltpu.make_async_copy(wd_ref, wd, w_sem.at[0]),
        pltpu.make_async_copy(wg_ref, wgu.at[:, pl.ds(0, F)], w_sem.at[1]),
        pltpu.make_async_copy(wu_ref, wgu.at[:, pl.ds(F, F)], w_sem.at[2]),
    )
    for w in weights:
        w.start()
    for c in gate_copies(0):
        c.start()
    acc[...] = jnp.zeros_like(acc)
    for w in weights:
        w.wait()

    def send_p(g):
        return remote(p_out.at[g % 2], p_in.at[g], p_ss.at[g], p_rs.at[g], partner)

    def send_r(src, slot, dev):
        return remote(src, rs_in.at[slot], r_ss.at[slot], r_rs.at[slot], dev)

    def send_last(k, i, dev):
        r = pl.ds(i * LAST, LAST)
        return remote(rs_out.at[k, r], last.at[k, r], l_ss.at[2 * k + i], l_rs.at[2 * k + i], dev)

    def dx_tile(g, r0, j):
        a = dgu[pl.ds(pl.multiple_of(g * B + r0, H), H), :]
        w = wgu[pl.ds(pl.multiple_of(j * 512, 512), 512), :]
        return lax.dot_general(a, w, NT, preferred_element_type=F32)

    def first_pass(g, carry):
        @pl.when(g == 2)
        def _():
            relay(dy_all, dy_ss, dy_rs, dyp_ss, dyp_rs, 2, "y")
            relay(dy_all, dy_ss, dy_rs, dyp_ss, dyp_rs, 3, "x")
            start_own(x_ref, x_all, x_ss, x_rs, xp_ss, xp_rs)

        for k in (4, 6):
            @pl.when(g == k)
            def _():
                relay(dy_all, dy_ss, dy_rs, dyp_ss, dyp_rs, k, None)
                relay(dy_all, dy_ss, dy_rs, dyp_ss, dyp_rs, k + 1, None)

        arrived(dy_all, dyp_ss, dyp_rs, g)
        load_tokens(dy_ref, dy_all, g)
        for c in gate_copies(g):
            c.wait()

        for n0, n in ((0, 256), (256, 256), (512, 128)):
            dh[:, n0:n0 + n] = lax.dot_general(tok[...], wd[n0:n0 + n, :], NT, preferred_element_type=F32)

        def gates(i, carry):
            r = pl.ds(pl.multiple_of(i * 32, 32), 32)
            a, u, d = gv[r, :].astype(F32), uv[r, :].astype(F32), dh[r, :]
            a2 = a * a
            t = jnp.tanh(a * (C0 + C1 * a2))
            cdf = 0.5 + 0.5 * t
            gelu = a * cdf
            slope = cdf + (0.5 * a) * ((1.0 - t * t) * (C0 + (3.0 * C1) * a2))
            hid[r, :] = (gelu * u).astype(BF16)
            q = pl.ds(pl.multiple_of(g * B + i * 32, 32), 32)
            dgu[q, 0:F] = (d * u * slope).astype(BF16)
            dgu[q, F:2 * F] = (d * gelu).astype(BF16)
            return carry

        lax.fori_loop(0, B // 32, gates, 0)

        @pl.when(g < 7)
        def _():
            for c in gate_copies(g + 1):
                c.start()

        @pl.when(g >= 2)
        def _():
            send_p(g - 2).wait_send()

        def p_rows(j, carry):
            p_out[g % 2, :, pl.ds(pl.multiple_of(j * 512, 512), 512)] = dx_tile(g, 0, j).astype(BF16)
            return carry

        lax.fori_loop(0, 4, p_rows, 0)
        send_p(g).start()

        def down(j, carry):
            s = pl.ds(pl.multiple_of(j * 512, 512), 512)
            r, c = pl.ds(pl.multiple_of((j // 2) * F, F), F), pl.ds(pl.multiple_of((j % 2) * 512, 512), 512)
            acc[r, c] += lax.dot_general(hid[...], tok[:, s], TN, preferred_element_type=F32)
            return carry

        lax.fori_loop(0, 4, down, 0)

        send_p(g).wait_recv()

        @pl.when(jnp.logical_or(g < 4, g >= 6))
        def _():
            def m_rows(j, carry):
                s = pl.ds(pl.multiple_of(j * 512, 512), 512)
                total = dx_tile(g, H, j) + p_in[g, :, s].astype(F32)

                @pl.when(g < 2)
                def _():
                    own[pl.ds(pl.multiple_of((g % 2) * H, H), H), s] = total

                @pl.when(jnp.logical_and(g >= 2, g < 4))
                def _():
                    rs_out[g % 2, :, s] = total.astype(BF16)

                @pl.when(g >= 6)
                def _():
                    dx_ref[pl.ds(pl.multiple_of((g % 2) * H, H), H), s] = total.astype(BF16)

                return carry

            lax.fori_loop(0, 4, m_rows, 0)

        @pl.when(g == 2)
        def _():
            send_r(rs_out.at[0], 2, nx).start()

        @pl.when(g == 3)
        def _():
            send_r(rs_out.at[1], 3, ny).start()

        @pl.when(g == 6)
        def _():
            send_r(dx_ref.at[pl.ds(0, H)], 0, nx).start()

        @pl.when(g == 7)
        def _():
            send_r(dx_ref.at[pl.ds(H, H)], 1, ny).start()

        return carry

    lax.fori_loop(0, 8, first_pass, 0)

    for j in range(4):
        dwd_ref[:, j * 512:j * 512 + 512] = acc[j // 2 * F:j // 2 * F + F, j % 2 * 512:j % 2 * 512 + 512].astype(BF16)
    acc[...] = jnp.zeros_like(acc)

    relay(x_all, x_ss, x_rs, xp_ss, xp_rs, 2, "y")
    relay(x_all, x_ss, x_rs, xp_ss, xp_rs, 3, "x")

    def fetch(slot, k):
        c = pltpu.make_async_copy(rs_in.at[slot], tok.at[pl.ds(k * H, H)], t_sem.at[k])
        c.start()
        return c

    def second_pass(g, carry):
        @pl.when(g == 4)
        def _():
            relay(x_all, x_ss, x_rs, xp_ss, xp_rs, 4, None)
            relay(x_all, x_ss, x_rs, xp_ss, xp_rs, 5, None)

        @pl.when(g == 6)
        def _():
            for slot, h in ((2, 0), (3, 1)):
                send_r(rs_out.at[0], slot, nx).wait_recv()
                fetch(slot, h).wait()

            def add(i, carry):
                r = pl.ds(pl.multiple_of(i * 32, 32), 32)
                own[r, :] += tok[r, :].astype(F32)
                return carry

            lax.fori_loop(0, B // 32, add, 0)

            send_r(rs_out.at[0], 2, nx).wait_send()
            send_r(rs_out.at[1], 3, ny).wait_send()
            for group, slot, k in ((4, 1, 0), (5, 0, 1)):
                send_r(rs_out.at[0], slot, nx).wait_recv()
                fetch(slot, k).wait()

                def late(j, carry):
                    s = pl.ds(pl.multiple_of(j * 512, 512), 512)
                    total = dx_tile(group, H, j) + p_in[group, :, s].astype(F32) + tok[k * H:(k + 1) * H, s].astype(F32)
                    rs_out[k, :, s] = total.astype(BF16)
                    return carry

                lax.fori_loop(0, 4, late, 0)

            for i in range(H // LAST):
                send_last(0, i, nx).start()
                send_last(1, i, ny).start()

            relay(x_all, x_ss, x_rs, xp_ss, xp_rs, 6, None)
            relay(x_all, x_ss, x_rs, xp_ss, xp_rs, 7, None)

        arrived(x_all, xp_ss, xp_rs, g)
        load_tokens(x_ref, x_all, g)

        def weight(j, carry):
            s = pl.ds(pl.multiple_of(j * 512, 512), 512)
            d = dgu[pl.ds(pl.multiple_of(g * B, B), B), :]
            acc[s, :] += lax.dot_general(tok[:, s], d, TN, preferred_element_type=F32)
            return carry

        lax.fori_loop(0, 4, weight, 0)
        return carry

    lax.fori_loop(0, 8, second_pass, 0)

    def weight_out(i, carry):
        r = pl.ds(pl.multiple_of(i * 32, 32), 32)
        dwg_ref[r, :] = acc[r, 0:F].astype(BF16)
        dwu_ref[r, :] = acc[r, F:2 * F].astype(BF16)
        return carry

    lax.fori_loop(0, D // 32, weight_out, 0)

    send_r(dx_ref.at[pl.ds(0, H)], 0, nx).wait_send()
    send_r(dx_ref.at[pl.ds(H, H)], 1, ny).wait_send()
    for i in range(H // LAST):
        for k in range(2):
            send_last(k, i, nx).wait_recv()

            def finish(n, carry):
                q = pl.ds(pl.multiple_of(i * LAST + n * 32, 32), 32)
                r = pl.ds(pl.multiple_of((1 - k) * H + i * LAST + n * 32, 32), 32)
                dx_ref[r, :] = (own[r, :] + last[k, q, :].astype(F32)).astype(BF16)
                return carry

            lax.fori_loop(0, LAST // 32, finish, 0)

    for full, ss, rs, pss, prs in ((dy_all, dy_ss, dy_rs, dyp_ss, dyp_rs), (x_all, x_ss, x_rs, xp_ss, xp_rs)):
        for g in range(8):
            send_on(full, pss, prs, g, g, partner).wait_send()
            if g >= 2:
                send_on(full, ss, rs, g, g, partner).wait_send()
    for g in (6, 7):
        send_p(g).wait_send()
    for i in range(H // LAST):
        send_last(0, i, nx).wait_send()
        send_last(1, i, ny).wait_send()


def solution(mesh):
    def local(*args):
        any_ = pl.BlockSpec(memory_space=pl.ANY)
        dma = pltpu.SemaphoreType.DMA
        shapes = [(B, D), (D, F), (D, F), (F, D), (8 * B, D), (8 * B, D), (4, H, D)]
        outs = pl.pallas_call(
            kernel,
            out_shape=[pltpu.VMEM(s, BF16) for s in shapes[:4]] + [jax.ShapeDtypeStruct(s, BF16) for s in shapes[4:]],
            in_specs=[any_] * 7,
            out_specs=[pl.BlockSpec(memory_space=pltpu.VMEM)] * 4 + [any_] * 3,
            scratch_shapes=[
                pltpu.VMEM((F, D), BF16),
                pltpu.VMEM((D, 2 * F), BF16),
                pltpu.VMEM((8 * B, 2 * F), BF16),
                pltpu.VMEM((D, 2 * F), F32),
                pltpu.VMEM((B, D), F32),
                pltpu.VMEM((B, D), BF16),
                pltpu.VMEM((B, F), BF16),
                pltpu.VMEM((B, F), BF16),
                pltpu.VMEM((B, F), F32),
                pltpu.VMEM((B, F), BF16),
                pltpu.VMEM((8, H, D), BF16),
                pltpu.VMEM((2, H, D), BF16),
                pltpu.VMEM((2, H, D), BF16),
                pltpu.VMEM((2, H, D), BF16),
            ]
            + [dma((8,))] * 12
            + [dma((4,)), dma((4,)), dma((3,)), dma((2,)), dma((4,))],
            compiler_params=pltpu.CompilerParams(collective_id=0, has_side_effects=True, vmem_limit_bytes=53*1048576),
            name="backward",
        )(*args)
        return tuple(outs[:4])

    rows, cols = P(("dp", "tp"), None), P("dp", "tp")
    return jax.shard_map(
        local,
        mesh=mesh,
        in_specs=(rows, rows, cols, cols, P(None, "tp"), P(None, "tp"), P("tp", None)),
        out_specs=(rows, cols, cols, rows),
        check_vma=False,
    )
```

```python
import functools

import jax
import jax.numpy as jnp
from jax import lax
from jax.experimental import pallas as pl
from jax.experimental.pallas import tpu as pltpu
from jax.sharding import PartitionSpec as P

D = 2048
F = 640
B = 512
H = 256
LAST = 128
F32 = jnp.float32
BF16 = jnp.bfloat16
NT = (((1,), (1,)), ((), ()))
TN = (((0,), (0,)), ((), ()))
C0 = 0.7978845608028654
C1 = 0.7978845608028654 * 0.044715


def kernel(
    x_ref, dy_ref, gate_ref, up_ref, wg_ref, wu_ref, wd_ref,
    own, last, dwg_ref, dwu_ref, dwd_ref, dy_all, x_all, rs_in,
    wd, wgu, dgu, acc, tok, gv, uv, dh, hid, p_in, p_out, rs_out,
    dy_ss, dy_rs, dyp_ss, dyp_rs, x_ss, x_rs, xp_ss, xp_rs, p_ss, p_rs, r_ss, r_rs, l_ss, l_rs, w_sem, t_sem, g_sem,
):
    me = lax.axis_index("tp")
    core, iy, ix = me % 2, (me // 2) % 2, me // 4
    other = 1 - 2 * core
    partner = me + other
    ny = me + 2 - 4 * iy
    nx = me + 4 - 8 * ix
    nd = ny + 4 - 8 * ix

    barrier = pltpu.get_barrier_semaphore()
    for d in (partner, nx, ny):
        pl.semaphore_signal(barrier, inc=1, device_id={"tp": d}, device_id_type=pl.DeviceIdType.MESH)
    pl.semaphore_wait(barrier, 3)

    def owner(g):
        return jnp.where(g < 2, me, jnp.where(g >= 6, nd, jnp.where(g % 2 == 0, nx, ny)))

    def half(g):
        return jnp.where(g == 4, 1, jnp.where(g == 5, 0, g % 2))

    def rows(dev, h):
        return pl.ds(pl.multiple_of(dev * B + h * H, H), H)

    def remote(src, dst, ss, rs, dev):
        return pltpu.make_async_remote_copy(
            src_ref=src, dst_ref=dst, send_sem=ss, recv_sem=rs, device_id={"tp": dev}, device_id_type=pl.DeviceIdType.MESH
        )

    def send_own(ref, full, ss, rs, h, g, dev):
        return remote(ref.at[pl.ds(h * H, H)], full.at[rows(me, h)], ss.at[g], rs.at[g], dev)

    def send_on(full, ss, rs, g_in, g_out, dev):
        r = rows(owner(g_in), half(g_in))
        return remote(full.at[r], full.at[r], ss.at[g_out], rs.at[g_out], dev)

    def start_own(ref, full, ss, rs, pss, prs):
        send_own(ref, full, ss, rs, 0, 2, nx).start()
        send_own(ref, full, ss, rs, 1, 3, ny).start()
        send_own(ref, full, pss, prs, 0, 0, partner).start()
        send_own(ref, full, ss, rs, 1, 4, nx).start()
        send_own(ref, full, ss, rs, 0, 5, ny).start()
        send_own(ref, full, pss, prs, 1, 1, partner).start()

    def arrived(full, ss, rs, g):
        send_on(full, ss, rs, g, g, partner).wait_recv()

    def relay(full, ss, rs, pss, prs, g, onward):
        arrived(full, ss, rs, g)
        if onward == "y":
            send_on(full, ss, rs, g, 6, ny).start()
        if onward == "x":
            send_on(full, ss, rs, g, 7, nx).start()
        send_on(full, pss, prs, g, g, partner).start()

    def load_tokens(ref, full, g):
        o, h = owner(g), half(g)
        p = pltpu.make_async_copy(full.at[rows(o + other, h)], tok.at[pl.ds(0, H)], t_sem.at[0])
        p.start()

        @pl.when(g < 2)
        def _():
            pltpu.make_async_copy(ref.at[pl.ds(pl.multiple_of(h * H, H), H)], tok.at[pl.ds(H, H)], t_sem.at[1]).start()

        @pl.when(g >= 2)
        def _():
            pltpu.make_async_copy(full.at[rows(o, h)], tok.at[pl.ds(H, H)], t_sem.at[1]).start()

        p.wait()
        pltpu.make_async_copy(full.at[rows(o, h)], tok.at[pl.ds(H, H)], t_sem.at[1]).wait()

    def gate_copies(g):
        o, h = owner(g), half(g)
        for i, (src, dst) in enumerate(((gate_ref, gv), (up_ref, uv))):
            yield pltpu.make_async_copy(src.at[rows(o + other, h)], dst.at[pl.ds(0, H)], g_sem.at[2 * i])
            yield pltpu.make_async_copy(src.at[rows(o, h)], dst.at[pl.ds(H, H)], g_sem.at[2 * i + 1])

    start_own(dy_ref, dy_all, dy_ss, dy_rs, dyp_ss, dyp_rs)
    weights = (
        pltpu.make_async_copy(wd_ref, wd, w_sem.at[0]),
        pltpu.make_async_copy(wg_ref, wgu.at[:, pl.ds(0, F)], w_sem.at[1]),
        pltpu.make_async_copy(wu_ref, wgu.at[:, pl.ds(F, F)], w_sem.at[2]),
    )
    for w in weights:
        w.start()
    for c in gate_copies(0):
        c.start()
    acc[...] = jnp.zeros_like(acc)
    for w in weights:
        w.wait()

    def send_p(g):
        return remote(p_out.at[g % 2], p_in.at[g], p_ss.at[g], p_rs.at[g], partner)

    def send_r(src, slot, dev):
        return remote(src, rs_in.at[slot], r_ss.at[slot], r_rs.at[slot], dev)

    def send_last(k, i, dev):
        r = pl.ds(i * LAST, LAST)
        return remote(rs_out.at[k, r], last.at[k, r], l_ss.at[2 * k + i], l_rs.at[2 * k + i], dev)

    def dx_tile(g, r0, j):
        a = dgu[pl.ds(pl.multiple_of(g * B + r0, H), H), :]
        w = wgu[pl.ds(pl.multiple_of(j * 512, 512), 512), :]
        return lax.dot_general(a, w, NT, preferred_element_type=F32)

    def first_pass(g, carry):
        @pl.when(g == 2)
        def _():
            relay(dy_all, dy_ss, dy_rs, dyp_ss, dyp_rs, 2, "y")
            relay(dy_all, dy_ss, dy_rs, dyp_ss, dyp_rs, 3, "x")
            start_own(x_ref, x_all, x_ss, x_rs, xp_ss, xp_rs)

        for k in (4, 6):
            @pl.when(g == k)
            def _():
                relay(dy_all, dy_ss, dy_rs, dyp_ss, dyp_rs, k, None)
                relay(dy_all, dy_ss, dy_rs, dyp_ss, dyp_rs, k + 1, None)

        arrived(dy_all, dyp_ss, dyp_rs, g)
        load_tokens(dy_ref, dy_all, g)
        for c in gate_copies(g):
            c.wait()

        for n0, n in ((0, 256), (256, 256), (512, 128)):
            dh[:, n0:n0 + n] = lax.dot_general(tok[...], wd[n0:n0 + n, :], NT, preferred_element_type=F32)

        def gates(i, carry):
            r = pl.ds(pl.multiple_of(i * 32, 32), 32)
            a, u, d = gv[r, :].astype(F32), uv[r, :].astype(F32), dh[r, :]
            a2 = a * a
            t = jnp.tanh(a * (C0 + C1 * a2))
            cdf = 0.5 + 0.5 * t
            gelu = a * cdf
            slope = cdf + (0.5 * a) * ((1.0 - t * t) * (C0 + (3.0 * C1) * a2))
            hid[r, :] = (gelu * u).astype(BF16)
            q = pl.ds(pl.multiple_of(g * B + i * 32, 32), 32)
            dgu[q, 0:F] = (d * u * slope).astype(BF16)
            dgu[q, F:2 * F] = (d * gelu).astype(BF16)
            return carry

        lax.fori_loop(0, B // 32, gates, 0)

        @pl.when(g < 7)
        def _():
            for c in gate_copies(g + 1):
                c.start()

        @pl.when(g >= 2)
        def _():
            send_p(g - 2).wait_send()

        def p_rows(j, carry):
            p_out[g % 2, :, pl.ds(pl.multiple_of(j * 512, 512), 512)] = dx_tile(g, 0, j).astype(BF16)
            return carry

        lax.fori_loop(0, 4, p_rows, 0)
        send_p(g).start()

        def down(j, carry):
            s = pl.ds(pl.multiple_of(j * 512, 512), 512)
            r, c = pl.ds(pl.multiple_of((j // 2) * F, F), F), pl.ds(pl.multiple_of((j % 2) * 512, 512), 512)
            acc[r, c] += lax.dot_general(hid[...], tok[:, s], TN, preferred_element_type=F32)
            return carry

        lax.fori_loop(0, 4, down, 0)

        send_p(g).wait_recv()

        @pl.when(jnp.logical_or(g < 4, g >= 6))
        def _():
            def m_rows(j, carry):
                s = pl.ds(pl.multiple_of(j * 512, 512), 512)
                total = dx_tile(g, H, j) + p_in[g, :, s].astype(F32)

                @pl.when(g < 2)
                def _():
                    own[pl.ds(pl.multiple_of((g % 2) * H, H), H), s] = total

                @pl.when(g >= 2)
                def _():
                    rs_out[jnp.where(g >= 6, g - 4, g % 2), :, s] = total.astype(BF16)

                return carry

            lax.fori_loop(0, 4, m_rows, 0)

        @pl.when(g == 2)
        def _():
            send_r(rs_out.at[0], 2, nx).start()

        @pl.when(g == 3)
        def _():
            send_r(rs_out.at[1], 3, ny).start()

        @pl.when(g == 6)
        def _():
            send_r(rs_out.at[2], 0, nx).start()

        @pl.when(g == 7)
        def _():
            send_r(rs_out.at[3], 1, ny).start()

        return carry

    lax.fori_loop(0, 8, first_pass, 0)

    for j in range(4):
        dwd_ref[:, j * 512:j * 512 + 512] = acc[j // 2 * F:j // 2 * F + F, j % 2 * 512:j % 2 * 512 + 512].astype(BF16)
    acc[...] = jnp.zeros_like(acc)

    relay(x_all, x_ss, x_rs, xp_ss, xp_rs, 2, "y")
    relay(x_all, x_ss, x_rs, xp_ss, xp_rs, 3, "x")

    def fetch(slot, k):
        c = pltpu.make_async_copy(rs_in.at[slot], tok.at[pl.ds(k * H, H)], t_sem.at[k])
        c.start()
        return c

    def second_pass(g, carry):
        @pl.when(g == 4)
        def _():
            relay(x_all, x_ss, x_rs, xp_ss, xp_rs, 4, None)
            relay(x_all, x_ss, x_rs, xp_ss, xp_rs, 5, None)

        @pl.when(g == 6)
        def _():
            for slot, h in ((2, 0), (3, 1)):
                send_r(rs_out.at[0], slot, nx).wait_recv()
                fetch(slot, h).wait()

            def add(i, carry):
                r = pl.ds(pl.multiple_of(i * 32, 32), 32)
                own[r, :] += tok[r, :].astype(F32)
                return carry

            lax.fori_loop(0, B // 32, add, 0)

            send_r(rs_out.at[0], 2, nx).wait_send()
            send_r(rs_out.at[1], 3, ny).wait_send()
            for group, slot, k in ((4, 1, 0), (5, 0, 1)):
                send_r(rs_out.at[0], slot, nx).wait_recv()
                fetch(slot, k).wait()

                def late(j, carry):
                    s = pl.ds(pl.multiple_of(j * 512, 512), 512)
                    total = dx_tile(group, H, j) + p_in[group, :, s].astype(F32) + tok[k * H:(k + 1) * H, s].astype(F32)
                    rs_out[k, :, s] = total.astype(BF16)
                    return carry

                lax.fori_loop(0, 4, late, 0)

            for i in range(H // LAST):
                send_last(0, i, nx).start()
                send_last(1, i, ny).start()

            relay(x_all, x_ss, x_rs, xp_ss, xp_rs, 6, None)
            relay(x_all, x_ss, x_rs, xp_ss, xp_rs, 7, None)

        arrived(x_all, xp_ss, xp_rs, g)
        load_tokens(x_ref, x_all, g)

        def weight(j, carry):
            s = pl.ds(pl.multiple_of(j * 512, 512), 512)
            d = dgu[pl.ds(pl.multiple_of(g * B, B), B), :]
            acc[s, :] += lax.dot_general(tok[:, s], d, TN, preferred_element_type=F32)
            return carry

        lax.fori_loop(0, 4, weight, 0)
        return carry

    lax.fori_loop(0, 8, second_pass, 0)

    def weight_out(i, carry):
        r = pl.ds(pl.multiple_of(i * 32, 32), 32)
        dwg_ref[r, :] = acc[r, 0:F].astype(BF16)
        dwu_ref[r, :] = acc[r, F:2 * F].astype(BF16)
        return carry

    lax.fori_loop(0, D // 32, weight_out, 0)

    send_r(rs_out.at[2], 0, nx).wait_send()
    send_r(rs_out.at[3], 1, ny).wait_send()
    for i in range(H // LAST):
        for k in range(2):
            send_last(k, i, nx).wait_recv()
    for full, ss, rs, pss, prs in ((dy_all, dy_ss, dy_rs, dyp_ss, dyp_rs), (x_all, x_ss, x_rs, xp_ss, xp_rs)):
        for g in range(8):
            send_on(full, pss, prs, g, g, partner).wait_send()
            if g >= 2:
                send_on(full, ss, rs, g, g, partner).wait_send()
    for g in (6, 7):
        send_p(g).wait_send()
    for i in range(H // LAST):
        send_last(0, i, nx).wait_send()
        send_last(1, i, ny).wait_send()


def finish(own, last, dwg, dwu, dwd, dx_ref, dwg_ref, dwu_ref, dwd_ref, dx, sem, dx_sem):
    copies = [
        pltpu.make_async_copy(src, dst, sem.at[i])
        for i, (src, dst) in enumerate(((dwd, dwd_ref), (dwg, dwg_ref), (dwu, dwu_ref)))
    ]
    for c in copies:
        c.start()
    for q in range(B // LAST):
        k, i = 1 - q * LAST // H, q * LAST % H

        def add(n, carry):
            r = pl.ds(pl.multiple_of(q * LAST + n * 32, 32), 32)
            dx[r, :] = (own[r, :] + last[k, pl.ds(pl.multiple_of(i + n * 32, 32), 32), :].astype(F32)).astype(BF16)
            return carry

        lax.fori_loop(0, LAST // 32, add, 0)
        r = pl.ds(q * LAST, LAST)
        copies.append(pltpu.make_async_copy(dx.at[r], dx_ref.at[r], dx_sem.at[q]))
        copies[-1].start()
    for c in copies:
        c.wait()


def solution(mesh):
    def local(*args):
        any_ = pl.BlockSpec(memory_space=pl.ANY)
        dma = pltpu.SemaphoreType.DMA
        vmem = pl.BlockSpec(memory_space=pltpu.VMEM)
        grads = [(D, F), (D, F), (F, D)]
        kept = pl.pallas_call(
            kernel,
            out_shape=[pltpu.VMEM((B, D), F32), pltpu.VMEM((2, H, D), BF16)]
            + [pltpu.VMEM(s, BF16) for s in grads]
            + [jax.ShapeDtypeStruct(s, BF16) for s in ((8 * B, D), (8 * B, D), (4, H, D))],
            in_specs=[any_] * 7,
            out_specs=[vmem] * 5 + [any_] * 3,
            scratch_shapes=[
                pltpu.VMEM((F, D), BF16),
                pltpu.VMEM((D, 2 * F), BF16),
                pltpu.VMEM((8 * B, 2 * F), BF16),
                pltpu.VMEM((D, 2 * F), F32),
                pltpu.VMEM((B, D), BF16),
                pltpu.VMEM((B, F), BF16),
                pltpu.VMEM((B, F), BF16),
                pltpu.VMEM((B, F), F32),
                pltpu.VMEM((B, F), BF16),
                pltpu.VMEM((8, H, D), BF16),
                pltpu.VMEM((2, H, D), BF16),
                pltpu.VMEM((4, H, D), BF16),
            ]
            + [dma((8,))] * 12
            + [dma((4,)), dma((4,)), dma((3,)), dma((2,)), dma((4,))],
            compiler_params=pltpu.CompilerParams(collective_id=0, has_side_effects=True, vmem_limit_bytes=49 * 2**20),
            name="backward",
        )(*args)
        return tuple(
            pl.pallas_call(
                finish,
                out_shape=[jax.ShapeDtypeStruct(s, BF16) for s in [(B, D), *grads]],
                in_specs=[vmem] * 5,
                out_specs=[any_] * 4,
                scratch_shapes=[pltpu.VMEM((B, D), BF16), dma((3,)), dma((B // LAST,))],
                compiler_params=pltpu.CompilerParams(vmem_limit_bytes=24 * 2**20),
                name="finish",
            )(*kept[:5])
        )

    rows, cols = P(("dp", "tp"), None), P("dp", "tp")
    return jax.shard_map(
        local,
        mesh=mesh,
        in_specs=(rows, rows, cols, cols, P(None, "tp"), P(None, "tp"), P("tp", None)),
        out_specs=(rows, cols, cols, rows),
        check_vma=False,
    )
```

```python
import functools

import jax
import jax.numpy as jnp
from jax import lax
from jax.experimental import pallas as pl
from jax.experimental.pallas import tpu as pltpu
from jax.sharding import PartitionSpec as P

D = 2048
F = 640
B = 512
H = 256
LAST = 256
SHIFT = 32
F32 = jnp.float32
BF16 = jnp.bfloat16
NT = (((1,), (1,)), ((), ()))
TN = (((0,), (0,)), ((), ()))
C0 = 0.7978845608028654
C1 = 0.7978845608028654 * 0.044715


def kernel(
    x_ref, dy_ref, gate_ref, up_ref, wg_ref, wu_ref, wd_ref,
    own, last, dwg_ref, dwu_ref, dwd_ref, dy_all, x_all, rs_in,
    wd, wgu, dgu, acc, tok, gv, uv, dh, hid, p_in, p_out, rs_out,
    dy_ss, dy_rs, dyp_ss, dyp_rs, x_ss, x_rs, xp_ss, xp_rs, p_ss, p_rs, r_ss, r_rs, l_ss, l_rs, e_ss, e_rs, ep_ss, ep_rs, w_sem, t_sem, g_sem,
):
    me = lax.axis_index("tp")
    core, iy, ix = me % 2, (me // 2) % 2, me // 4
    other = 1 - 2 * core
    partner = me + other
    ny = me + 2 - 4 * iy
    nx = me + 4 - 8 * ix
    nd = ny + 4 - 8 * ix

    barrier = pltpu.get_barrier_semaphore()
    for d in (partner, nx, ny):
        pl.semaphore_signal(barrier, inc=1, device_id={"tp": d}, device_id_type=pl.DeviceIdType.MESH)
    pl.semaphore_wait(barrier, 3)

    def owner(g):
        return jnp.where(g < 2, me, jnp.where(g >= 6, nd, jnp.where(g % 2 == 0, nx, ny)))

    def half(g):
        return jnp.where(g == 4, 1, jnp.where(g == 5, 0, g % 2))

    def rows(dev, h):
        return pl.ds(pl.multiple_of(dev * B + h * H, H), H)

    def remote(src, dst, ss, rs, dev):
        return pltpu.make_async_remote_copy(
            src_ref=src, dst_ref=dst, send_sem=ss, recv_sem=rs, device_id={"tp": dev}, device_id_type=pl.DeviceIdType.MESH
        )

    def send_own(ref, full, ss, rs, h, g, dev):
        return remote(ref.at[pl.ds(h * H, H)], full.at[rows(me, h)], ss.at[g], rs.at[g], dev)

    def send_on(full, ss, rs, g_in, g_out, dev):
        r = rows(owner(g_in), half(g_in))
        return remote(full.at[r], full.at[r], ss.at[g_out], rs.at[g_out], dev)

    def start_own(ref, full, ss, rs, pss, prs):
        send_own(ref, full, ss, rs, 0, 2, nx).start()
        send_own(ref, full, ss, rs, 1, 3, ny).start()
        send_own(ref, full, pss, prs, 0, 0, partner).start()
        send_own(ref, full, ss, rs, 1, 4, nx).start()
        send_own(ref, full, ss, rs, 0, 5, ny).start()
        send_own(ref, full, pss, prs, 1, 1, partner).start()

    def arrived(full, ss, rs, g):
        send_on(full, ss, rs, g, g, partner).wait_recv()

    def relay(full, ss, rs, pss, prs, g, onward):
        arrived(full, ss, rs, g)
        if onward == "y":
            send_on(full, ss, rs, g, 6, ny).start()
        if onward == "x":
            send_on(full, ss, rs, g, 7, nx).start()
        send_on(full, pss, prs, g, g, partner).start()

    def load_tokens(ref, full, g):
        o, h = owner(g), half(g)
        p = pltpu.make_async_copy(full.at[rows(o + other, h)], tok.at[pl.ds(0, H)], t_sem.at[0])
        p.start()

        @pl.when(g < 2)
        def _():
            pltpu.make_async_copy(ref.at[pl.ds(pl.multiple_of(h * H, H), H)], tok.at[pl.ds(H, H)], t_sem.at[1]).start()

        @pl.when(g >= 2)
        def _():
            pltpu.make_async_copy(full.at[rows(o, h)], tok.at[pl.ds(H, H)], t_sem.at[1]).start()

        p.wait()
        pltpu.make_async_copy(full.at[rows(o, h)], tok.at[pl.ds(H, H)], t_sem.at[1]).wait()

    def gate_copies(g):
        o, h = owner(g), half(g)
        for i, (src, dst) in enumerate(((gate_ref, gv), (up_ref, uv))):
            yield pltpu.make_async_copy(src.at[rows(o + other, h)], dst.at[pl.ds(0, H)], g_sem.at[2 * i])
            yield pltpu.make_async_copy(src.at[rows(o, h)], dst.at[pl.ds(H, H)], g_sem.at[2 * i + 1])

    start_own(dy_ref, dy_all, dy_ss, dy_rs, dyp_ss, dyp_rs)
    weights = (
        pltpu.make_async_copy(wd_ref, wd, w_sem.at[0]),
        pltpu.make_async_copy(wg_ref, wgu.at[:, pl.ds(0, F)], w_sem.at[1]),
        pltpu.make_async_copy(wu_ref, wgu.at[:, pl.ds(F, F)], w_sem.at[2]),
    )
    for w in weights:
        w.start()
    for c in gate_copies(0):
        c.start()
    acc[...] = jnp.zeros_like(acc)
    for w in weights:
        w.wait()

    def send_p(g):
        return remote(p_out.at[g % 2], p_in.at[g], p_ss.at[g], p_rs.at[g], partner)

    def send_r(src, slot, dev):
        return remote(src, rs_in.at[slot], r_ss.at[slot], r_rs.at[slot], dev)

    def send_last(k, i, dev):
        r = pl.ds(i * LAST, LAST)
        return remote(rs_out.at[k, r], last.at[k, r], l_ss.at[k * (H // LAST) + i], l_rs.at[k * (H // LAST) + i], dev)

    def dx_tile(g, r0, j):
        a = dgu[pl.ds(pl.multiple_of(g * B + r0, H), H), :]
        w = wgu[pl.ds(pl.multiple_of(j * 512, 512), 512), :]
        return lax.dot_general(a, w, NT, preferred_element_type=F32)

    def first_pass(g, carry):
        @pl.when(g == 2)
        def _():
            relay(dy_all, dy_ss, dy_rs, dyp_ss, dyp_rs, 2, "y")
            relay(dy_all, dy_ss, dy_rs, dyp_ss, dyp_rs, 3, "x")
            start_own(x_ref, x_all, x_ss, x_rs, xp_ss, xp_rs)

        for k in (4, 6):
            @pl.when(g == k)
            def _():
                relay(dy_all, dy_ss, dy_rs, dyp_ss, dyp_rs, k, None)
                relay(dy_all, dy_ss, dy_rs, dyp_ss, dyp_rs, k + 1, None)

        arrived(dy_all, dyp_ss, dyp_rs, g)
        load_tokens(dy_ref, dy_all, g)
        for c in gate_copies(g):
            c.wait()

        for n0, n in ((0, 256), (256, 256), (512, 128)):
            dh[:, n0:n0 + n] = lax.dot_general(tok[...], wd[n0:n0 + n, :], NT, preferred_element_type=F32)

        def gates(i, carry):
            r = pl.ds(pl.multiple_of(i * 32, 32), 32)
            a, u, d = gv[r, :].astype(F32), uv[r, :].astype(F32), dh[r, :]
            a2 = a * a
            t = jnp.tanh(a * (C0 + C1 * a2))
            cdf = 0.5 + 0.5 * t
            gelu = a * cdf
            slope = cdf + (0.5 * a) * ((1.0 - t * t) * (C0 + (3.0 * C1) * a2))
            hid[r, :] = (gelu * u).astype(BF16)
            q = pl.ds(pl.multiple_of(g * B + i * 32, 32), 32)
            dgu[q, 0:F] = (d * u * slope).astype(BF16)
            dgu[q, F:2 * F] = (d * gelu).astype(BF16)
            return carry

        lax.fori_loop(0, B // 32, gates, 0)

        @pl.when(g < 7)
        def _():
            for c in gate_copies(g + 1):
                c.start()

        @pl.when(g >= 2)
        def _():
            send_p(g - 2).wait_send()

        def p_rows(j, carry):
            p_out[g % 2, :, pl.ds(pl.multiple_of(j * 512, 512), 512)] = dx_tile(g, 0, j).astype(BF16)
            return carry

        lax.fori_loop(0, 4, p_rows, 0)
        send_p(g).start()

        def down(j, carry):
            s = pl.ds(pl.multiple_of(j * 512, 512), 512)
            r, c = pl.ds(pl.multiple_of((j // 2) * F, F), F), pl.ds(pl.multiple_of((j % 2) * 512, 512), 512)
            acc[r, c] += lax.dot_general(hid[...], tok[:, s], TN, preferred_element_type=F32)
            return carry

        lax.fori_loop(0, 4, down, 0)

        send_p(g).wait_recv()

        @pl.when(jnp.logical_or(g < 4, g >= 6))
        def _():
            def m_rows(j, carry):
                s = pl.ds(pl.multiple_of(j * 512, 512), 512)
                total = dx_tile(g, H, j) + p_in[g, :, s].astype(F32)

                @pl.when(g < 2)
                def _():
                    own[pl.ds(pl.multiple_of((g % 2) * H, H), H), s] = total

                @pl.when(g >= 2)
                def _():
                    rs_out[jnp.where(g >= 6, g - 4, g % 2), :, s] = total.astype(BF16)

                return carry

            lax.fori_loop(0, 4, m_rows, 0)

        @pl.when(g == 2)
        def _():
            send_r(rs_out.at[0], 2, nx).start()

        @pl.when(g == 3)
        def _():
            send_r(rs_out.at[1], 3, ny).start()

        @pl.when(g == 6)
        def _():
            send_r(rs_out.at[2], 0, nx).start()

        @pl.when(g == 7)
        def _():
            send_r(rs_out.at[3], 1, ny).start()

        return carry

    lax.fori_loop(0, 8, first_pass, 0)

    for j in range(4):
        dwd_ref[:, j * 512:j * 512 + 512] = acc[j // 2 * F:j // 2 * F + F, j % 2 * 512:j % 2 * 512 + 512].astype(BF16)
    acc[...] = jnp.zeros_like(acc)

    def onward(k, n):
        g = 2 + k
        r = pl.ds(pl.multiple_of(owner(g) * B + half(g) * H, H), n)
        return remote(x_all.at[r], x_all.at[r], x_ss.at[6 + k], x_rs.at[6 + k], (ny, nx)[k])

    def tail(g):
        return pl.ds(pl.multiple_of((owner(g) - core) * B + half(g) * H + H - SHIFT, 8), SHIFT)

    def onward_tail(k):
        r = tail(2 + k)
        return remote(x_all.at[r], x_all.at[r], e_ss.at[k], e_rs.at[k], (ny, nx)[k])

    def to_partner(k, n):
        g = 6 + k
        r = pl.ds(pl.multiple_of(owner(g) * B + half(g) * H, H), n)
        return remote(x_all.at[r], x_all.at[r], xp_ss.at[g], xp_rs.at[g], partner)

    def to_partner_tail(k):
        r = tail(6 + k)
        return remote(x_all.at[r], x_all.at[r], ep_ss.at[k], ep_rs.at[k], partner)

    for k in range(2):
        arrived(x_all, x_ss, x_rs, 2 + k)

        @pl.when(core == 0)
        def _():
            onward(k, H - SHIFT).start()

        @pl.when(core == 1)
        def _():
            onward(k, H).start()

        send_on(x_all, xp_ss, xp_rs, 2 + k, 2 + k, partner).start()
    for k in range(2):
        arrived(x_all, xp_ss, xp_rs, 2 + k)

        @pl.when(core == 1)
        def _():
            onward_tail(k).start()

    def fetch(slot, k):
        c = pltpu.make_async_copy(rs_in.at[slot], tok.at[pl.ds(k * H, H)], t_sem.at[k])
        c.start()
        return c

    def second_pass(g, carry):
        @pl.when(g == 4)
        def _():
            relay(x_all, x_ss, x_rs, xp_ss, xp_rs, 4, None)
            relay(x_all, x_ss, x_rs, xp_ss, xp_rs, 5, None)

        @pl.when(g == 6)
        def _():
            for slot, h in ((2, 0), (3, 1)):
                send_r(rs_out.at[0], slot, nx).wait_recv()
                fetch(slot, h).wait()

            def add(i, carry):
                r = pl.ds(pl.multiple_of(i * 32, 32), 32)
                own[r, :] += tok[r, :].astype(F32)
                return carry

            lax.fori_loop(0, B // 32, add, 0)

            send_r(rs_out.at[0], 2, nx).wait_send()
            send_r(rs_out.at[1], 3, ny).wait_send()
            for group, slot, k in ((4, 1, 0), (5, 0, 1)):
                send_r(rs_out.at[0], slot, nx).wait_recv()
                fetch(slot, k).wait()

                def late(j, carry):
                    s = pl.ds(pl.multiple_of(j * 512, 512), 512)
                    total = dx_tile(group, H, j) + p_in[group, :, s].astype(F32) + tok[k * H:(k + 1) * H, s].astype(F32)
                    rs_out[k, :, s] = total.astype(BF16)
                    return carry

                lax.fori_loop(0, 4, late, 0)

            for i in range(H // LAST):
                send_last(0, i, nx).start()
                send_last(1, i, ny).start()

            @pl.when(core == 0)
            def _():
                for k in range(2):
                    onward(k, H - SHIFT).wait_recv()
                    to_partner(k, H - SHIFT).start()
                for k in range(2):
                    to_partner(k, H).wait_recv()
                    to_partner_tail(k).wait_recv()

            @pl.when(core == 1)
            def _():
                for k in range(2):
                    onward(k, H).wait_recv()
                    to_partner(k, H).start()
                for k in range(2):
                    onward_tail(k).wait_recv()
                    to_partner_tail(k).start()
                for k in range(2):
                    to_partner(k, H - SHIFT).wait_recv()

        @pl.when(jnp.logical_or(g < 2, jnp.logical_or(g == 4, g == 5)))
        def _():
            arrived(x_all, xp_ss, xp_rs, g)

        load_tokens(x_ref, x_all, g)

        def weight(j, carry):
            s = pl.ds(pl.multiple_of(j * 512, 512), 512)
            d = dgu[pl.ds(pl.multiple_of(g * B, B), B), :]
            acc[s, :] += lax.dot_general(tok[:, s], d, TN, preferred_element_type=F32)
            return carry

        lax.fori_loop(0, 4, weight, 0)
        return carry

    lax.fori_loop(0, 8, second_pass, 0)

    def weight_out(i, carry):
        r = pl.ds(pl.multiple_of(i * 32, 32), 32)
        dwg_ref[r, :] = acc[r, 0:F].astype(BF16)
        dwu_ref[r, :] = acc[r, F:2 * F].astype(BF16)
        return carry

    lax.fori_loop(0, D // 32, weight_out, 0)

    send_r(rs_out.at[2], 0, nx).wait_send()
    send_r(rs_out.at[3], 1, ny).wait_send()
    for full, ss, rs, pss, prs, n in (
        (dy_all, dy_ss, dy_rs, dyp_ss, dyp_rs, 8),
        (x_all, x_ss, x_rs, xp_ss, xp_rs, 6),
    ):
        for g in range(n):
            send_on(full, pss, prs, g, g, partner).wait_send()
            if g >= 2:
                send_on(full, ss, rs, g, g, partner).wait_send()
    for g in (6, 7):
        send_p(g).wait_send()

    @pl.when(core == 0)
    def _():
        for k in range(2):
            onward(k, H - SHIFT).wait_send()
            to_partner(k, H - SHIFT).wait_send()

    @pl.when(core == 1)
    def _():
        for k in range(2):
            onward(k, H).wait_send()
            to_partner(k, H).wait_send()
            onward_tail(k).wait_send()
            to_partner_tail(k).wait_send()

    for i in range(H // LAST):
        for k in range(2):
            send_last(k, i, nx).wait_send()
    for i in range(H // LAST):
        for k in range(2):
            send_last(k, i, nx).wait_recv()


def finish(own, last, dwg, dwu, dwd, dx_ref, dwg_ref, dwu_ref, dwd_ref, dx, sem, dx_sem):
    copies = [
        pltpu.make_async_copy(src, dst, sem.at[i])
        for i, (src, dst) in enumerate(((dwd, dwd_ref), (dwg, dwg_ref), (dwu, dwu_ref)))
    ]
    for c in copies:
        c.start()
    for q in range(B // LAST):
        k, i = 1 - q * LAST // H, q * LAST % H

        def add(n, carry):
            r = pl.ds(pl.multiple_of(q * LAST + n * 32, 32), 32)
            dx[r, :] = (own[r, :] + last[k, pl.ds(pl.multiple_of(i + n * 32, 32), 32), :].astype(F32)).astype(BF16)
            return carry

        lax.fori_loop(0, LAST // 32, add, 0)
        r = pl.ds(q * LAST, LAST)
        copies.append(pltpu.make_async_copy(dx.at[r], dx_ref.at[r], dx_sem.at[q]))
        copies[-1].start()
    for c in copies:
        c.wait()


def solution(mesh):
    def local(*args):
        any_ = pl.BlockSpec(memory_space=pl.ANY)
        dma = pltpu.SemaphoreType.DMA
        vmem = pl.BlockSpec(memory_space=pltpu.VMEM)
        grads = [(D, F), (D, F), (F, D)]
        kept = pl.pallas_call(
            kernel,
            out_shape=[pltpu.VMEM((B, D), F32), pltpu.VMEM((2, H, D), BF16)]
            + [pltpu.VMEM(s, BF16) for s in grads]
            + [jax.ShapeDtypeStruct(s, BF16) for s in ((8 * B, D), (8 * B, D), (4, H, D))],
            in_specs=[any_] * 7,
            out_specs=[vmem] * 5 + [any_] * 3,
            scratch_shapes=[
                pltpu.VMEM((F, D), BF16),
                pltpu.VMEM((D, 2 * F), BF16),
                pltpu.VMEM((8 * B, 2 * F), BF16),
                pltpu.VMEM((D, 2 * F), F32),
                pltpu.VMEM((B, D), BF16),
                pltpu.VMEM((B, F), BF16),
                pltpu.VMEM((B, F), BF16),
                pltpu.VMEM((B, F), F32),
                pltpu.VMEM((B, F), BF16),
                pltpu.VMEM((8, H, D), BF16),
                pltpu.VMEM((2, H, D), BF16),
                pltpu.VMEM((4, H, D), BF16),
            ]
            + [dma((8,))] * 12
            + [dma((2 * H // LAST,))] * 2
            + [dma((2,))] * 4
            + [dma((3,)), dma((2,)), dma((4,))],
            compiler_params=pltpu.CompilerParams(collective_id=0, has_side_effects=True, vmem_limit_bytes=49 * 2**20),
            name="backward",
        )(*args)
        return tuple(
            pl.pallas_call(
                finish,
                out_shape=[jax.ShapeDtypeStruct(s, BF16) for s in [(B, D), *grads]],
                in_specs=[vmem] * 5,
                out_specs=[any_] * 4,
                scratch_shapes=[pltpu.VMEM((B, D), BF16), dma((3,)), dma((B // LAST,))],
                compiler_params=pltpu.CompilerParams(vmem_limit_bytes=24 * 2**20),
                name="finish",
            )(*kept[:5])
        )

    rows, cols = P(("dp", "tp"), None), P("dp", "tp")
    return jax.shard_map(
        local,
        mesh=mesh,
        in_specs=(rows, rows, cols, cols, P(None, "tp"), P(None, "tp"), P("tp", None)),
        out_specs=(rows, cols, cols, rows),
        check_vma=False,
    )
```

```python
import functools

import jax
import jax.numpy as jnp
from jax import lax
from jax.experimental import pallas as pl
from jax.experimental.pallas import tpu as pltpu
from jax.sharding import PartitionSpec as P

D = 2048
F = 640
B = 512
H = 256
LAST = 128
SHIFT = 32
F32 = jnp.float32
BF16 = jnp.bfloat16
NT = (((1,), (1,)), ((), ()))
TN = (((0,), (0,)), ((), ()))
C0 = 0.7978845608028654
C1 = 0.7978845608028654 * 0.044715


def kernel(
    x_ref, dy_ref, gate_ref, up_ref, wg_ref, wu_ref, wd_ref,
    own, last, dwg_ref, dwu_ref, dwd_ref, dy_all, x_all, rs_in,
    wd, wgu, dgu, acc, tok, guv, dh, hid, p_in, p_out, rs_out,
    dy_s, dy_r, dyp_r, x_s, x_r, xp_r, p_s, p_r, r_s, r_r, l_s, l_r, w_sem, t_sem, g_sem,
):
    me = lax.axis_index("tp")
    core, iy, ix = me % 2, (me // 2) % 2, me // 4
    other = 1 - 2 * core
    partner = me + other
    ny = me + 2 - 4 * iy
    nx = me + 4 - 8 * ix
    nd = ny + 4 - 8 * ix

    barrier = pltpu.get_barrier_semaphore()
    for d in (partner, nx, ny):
        pl.semaphore_signal(barrier, inc=1, device_id={"tp": d}, device_id_type=pl.DeviceIdType.MESH)
    pl.semaphore_wait(barrier, 3)

    def owner(g):
        return jnp.where(g < 2, me, jnp.where(g >= 6, nd, jnp.where(g % 2 == 0, nx, ny)))

    def half(g):
        return jnp.where(g == 4, 1, jnp.where(g == 5, 0, g % 2))

    def rows(dev, h, n=H):
        return pl.ds(pl.multiple_of(dev * B + h * H, H), n)

    def remote(src, dst, ss, rs, dev):
        return pltpu.make_async_remote_copy(
            src_ref=src, dst_ref=dst, send_sem=ss, recv_sem=rs, device_id={"tp": dev}, device_id_type=pl.DeviceIdType.MESH
        )

    def of_rows(full, n, ss, rs):
        return remote(full.at[pl.ds(0, n)], full.at[pl.ds(0, n)], ss, rs, partner)

    def start_own(ref, full, s, r, pr):
        for h, p, dev in ((0, 0, nx), (1, 0, ny), (0, None, partner), (1, 1, nx), (0, 1, ny), (1, None, partner)):
            remote(ref.at[pl.ds(h * H, H)], full.at[rows(me, h)], s.at[0], pr.at[0] if p is None else r.at[p], dev).start()

    def send_on(full, s, r, g, n, dev):
        q = rows(owner(g), half(g), n)
        remote(full.at[q], full.at[q], s.at[0], r, dev).start()

    def relay(full, s, r, pr, p, onward):
        of_rows(full, 2 * H, s.at[0], r.at[p - 1]).wait_recv()
        if onward:
            send_on(full, s, r.at[2], 2, H, ny)
            send_on(full, s, r.at[2], 3, H, nx)
        for g in (2 * p, 2 * p + 1):
            send_on(full, s, pr.at[p], g, H, partner)

    def from_partner(full, s, pr, p):
        of_rows(full, 2 * H, s.at[0], pr.at[p]).wait_recv()

    def load(ref, full, g):
        o, h, slot = owner(g), half(g), g % 2
        pltpu.make_async_copy(full.at[rows(o + other, h)], tok.at[slot, pl.ds(0, H)], t_sem.at[slot]).start()

        @pl.when(g < 2)
        def _():
            src = ref.at[pl.ds(pl.multiple_of(h * H, H), H)]
            pltpu.make_async_copy(src, tok.at[slot, pl.ds(H, H)], t_sem.at[slot]).start()

        @pl.when(g >= 2)
        def _():
            pltpu.make_async_copy(full.at[rows(o, h)], tok.at[slot, pl.ds(H, H)], t_sem.at[slot]).start()

    def loaded(slot):
        pltpu.make_async_copy(dy_all.at[pl.ds(0, B)], tok.at[slot], t_sem.at[slot]).wait()

    def load_gates(g):
        o, h = owner(g), half(g)
        for i, src in enumerate((gate_ref, up_ref)):
            pltpu.make_async_copy(src.at[rows(o + other, h)], guv.at[i, pl.ds(0, H)], g_sem.at[0]).start()
            pltpu.make_async_copy(src.at[rows(o, h)], guv.at[i, pl.ds(H, H)], g_sem.at[0]).start()

    start_own(dy_ref, dy_all, dy_s, dy_r, dyp_r)
    pltpu.make_async_copy(wd_ref, wd, w_sem.at[0]).start()
    load_gates(0)
    pltpu.make_async_copy(wg_ref, wgu.at[:, pl.ds(0, F)], w_sem.at[1]).start()
    pltpu.make_async_copy(wu_ref, wgu.at[:, pl.ds(F, F)], w_sem.at[1]).start()
    from_partner(dy_all, dy_s, dyp_r, 0)
    load(dy_ref, dy_all, 0)
    acc[...] = jnp.zeros_like(acc)
    pltpu.make_async_copy(wd_ref, wd, w_sem.at[0]).wait()
    pltpu.make_async_copy(wgu, wgu, w_sem.at[1]).wait()

    def p_slot(g):
        return jnp.where(jnp.logical_or(g == 4, g == 5), g - 2, g % 2)

    def send_p(g):
        return remote(p_out.at[g % 2], p_in.at[p_slot(g)], p_s.at[g % 2], p_r.at[g % 2], partner)

    def send_r(stage, kind, k, dev):
        return remote(rs_out.at[stage], rs_in.at[kind, pl.ds(k * H, H)], r_s.at[kind], r_r.at[kind], dev)

    def both_r(kind):
        return remote(rs_in.at[kind], rs_in.at[kind], r_s.at[kind], r_r.at[kind], nx)

    def send_last(k, dev):
        return remote(rs_out.at[k], last.at[k], l_s.at[0], l_r.at[0], dev)

    def dx_tile(g, r0, j):
        a = dgu[pl.ds(pl.multiple_of(g * B + r0, H), H), :]
        w = wgu[pl.ds(pl.multiple_of(j * 512, 512), 512), :]
        return lax.dot_general(a, w, NT, preferred_element_type=F32)

    def first_pass(g, carry):
        slot = g % 2
        loaded(slot)
        pltpu.make_async_copy(guv, guv, g_sem.at[0]).wait()

        @pl.when(slot == 0)
        def _():
            load(dy_ref, dy_all, g + 1)

        for n0, n in ((0, 256), (256, 256), (512, 128)):
            dh[:, n0:n0 + n] = lax.dot_general(tok[slot], wd[n0:n0 + n, :], NT, preferred_element_type=F32)

        def gates(i, carry):
            r = pl.ds(pl.multiple_of(i * 32, 32), 32)
            a, u, d = guv[0, r, :].astype(F32), guv[1, r, :].astype(F32), dh[r, :]
            a2 = a * a
            t = jnp.tanh(a * (C0 + C1 * a2))
            cdf = 0.5 + 0.5 * t
            gelu = a * cdf
            slope = cdf + (0.5 * a) * ((1.0 - t * t) * (C0 + (3.0 * C1) * a2))
            hid[r, :] = (gelu * u).astype(BF16)
            q = pl.ds(pl.multiple_of(g * B + i * 32, 32), 32)
            dgu[q, 0:F] = (d * u * slope).astype(BF16)
            dgu[q, F:2 * F] = (d * gelu).astype(BF16)
            return carry

        lax.fori_loop(0, B // 32, gates, 0)

        @pl.when(g < 7)
        def _():
            load_gates(g + 1)

        @pl.when(g >= 2)
        def _():
            send_p(g - 2).wait_send()

        def p_rows(j, carry):
            p_out[slot, :, pl.ds(pl.multiple_of(j * 512, 512), 512)] = dx_tile(g, 0, j).astype(BF16)
            return carry

        lax.fori_loop(0, 4, p_rows, 0)
        send_p(g).start()

        def down(j, carry):
            s = pl.ds(pl.multiple_of(j * 512, 512), 512)
            r, c = pl.ds(pl.multiple_of((j // 2) * F, F), F), pl.ds(pl.multiple_of((j % 2) * 512, 512), 512)
            acc[r, c] += lax.dot_general(hid[...], tok[slot, :, s], TN, preferred_element_type=F32)
            return carry

        lax.fori_loop(0, 4, down, 0)

        for p in (1, 2, 3):
            @pl.when(g == 2 * p - 1)
            def _():
                relay(dy_all, dy_s, dy_r, dyp_r, p, p == 1)
                if p == 1:
                    start_own(x_ref, x_all, x_s, x_r, xp_r)
                from_partner(dy_all, dy_s, dyp_r, p)
                load(dy_ref, dy_all, g + 1)

        @pl.when(g == 7)
        def _():
            from_partner(x_all, x_s, xp_r, 0)
            load(x_ref, x_all, 0)

        send_p(g).wait_recv()

        @pl.when(jnp.logical_or(g < 4, g >= 6))
        def _():
            def m_rows(j, carry):
                s = pl.ds(pl.multiple_of(j * 512, 512), 512)
                total = dx_tile(g, H, j) + p_in[p_slot(g), :, s].astype(F32)

                @pl.when(g < 2)
                def _():
                    own[pl.ds(pl.multiple_of(slot * H, H), H), s] = total

                @pl.when(g >= 2)
                def _():
                    rs_out[jnp.where(g >= 6, g - 4, slot), :, s] = total.astype(BF16)

                return carry

            lax.fori_loop(0, 4, m_rows, 0)

        for group, stage, kind, k, dev in ((2, 0, 0, 0, nx), (3, 1, 0, 1, ny), (6, 2, 1, 1, nx), (7, 3, 1, 0, ny)):
            @pl.when(g == group)
            def _():
                send_r(stage, kind, k, dev).start()

        return carry

    lax.fori_loop(0, 8, first_pass, 0)

    for j in range(4):
        dwd_ref[:, j * 512:j * 512 + 512] = acc[j // 2 * F:j // 2 * F + F, j % 2 * 512:j % 2 * 512 + 512].astype(BF16)
    acc[...] = jnp.zeros_like(acc)

    def tail(g):
        return pl.ds(pl.multiple_of((owner(g) - core) * B + half(g) * H + H - SHIFT, 8), SHIFT)

    def send_tail(g, r, dev):
        remote(x_all.at[tail(g)], x_all.at[tail(g)], x_s.at[0], r, dev).start()

    def second_pass(g, carry):
        slot = g % 2
        loaded(slot)

        @pl.when(slot == 0)
        def _():
            load(x_ref, x_all, g + 1)

        @pl.when(g == 1)
        def _():
            relay(x_all, x_s, x_r, xp_r, 1, False)
            for c, n in ((0, H - SHIFT), (1, H)):
                @pl.when(core == c)
                def _():
                    send_on(x_all, x_s, x_r.at[2], 2, n, ny)
                    send_on(x_all, x_s, x_r.at[2], 3, n, nx)

            from_partner(x_all, x_s, xp_r, 1)

            @pl.when(core == 1)
            def _():
                send_tail(2, x_r.at[2], ny)
                send_tail(3, x_r.at[2], nx)

            load(x_ref, x_all, 2)

        @pl.when(g == 3)
        def _():
            relay(x_all, x_s, x_r, xp_r, 2, False)
            from_partner(x_all, x_s, xp_r, 2)
            load(x_ref, x_all, 4)

        def weight(j, carry):
            s = pl.ds(pl.multiple_of(j * 512, 512), 512)
            d = dgu[pl.ds(pl.multiple_of(g * B, B), B), :]
            acc[s, :] += lax.dot_general(tok[slot, :, s], d, TN, preferred_element_type=F32)
            return carry

        lax.fori_loop(0, 4, weight, 0)

        @pl.when(g == 5)
        def _():
            for kind in range(2):
                both_r(kind).wait_recv()
                pltpu.make_async_copy(rs_in.at[kind], tok.at[kind], t_sem.at[kind]).start()
            both_r(0).wait_send()
            loaded(0)

            def add(i, carry):
                r = pl.ds(pl.multiple_of(i * 32, 32), 32)
                own[r, :] += tok[0, r, :].astype(F32)
                return carry

            lax.fori_loop(0, B // 32, add, 0)
            loaded(1)
            for k, dev in enumerate((nx, ny)):
                def late(j, carry):
                    s = pl.ds(pl.multiple_of(j * 512, 512), 512)
                    total = dx_tile(4 + k, H, j) + p_in[2 + k, :, s].astype(F32) + tok[1, k * H:(k + 1) * H, s].astype(F32)
                    rs_out[k, :, s] = total.astype(BF16)
                    return carry

                lax.fori_loop(0, 4, late, 0)
                send_last(k, dev).start()

            for c, n, m in ((0, H - SHIFT, 2 * H + 2 * SHIFT), (1, H, 2 * H - 2 * SHIFT)):
                @pl.when(core == c)
                def _():
                    of_rows(x_all, 4 * H - m, x_s.at[0], x_r.at[2]).wait_recv()
                    send_on(x_all, x_s, xp_r.at[3], 6, n, partner)
                    send_on(x_all, x_s, xp_r.at[3], 7, n, partner)
                    if c == 1:
                        send_tail(6, xp_r.at[3], partner)
                        send_tail(7, xp_r.at[3], partner)
                    of_rows(x_all, m, x_s.at[0], xp_r.at[3]).wait_recv()

            load(x_ref, x_all, 6)

        return carry

    lax.fori_loop(0, 8, second_pass, 0)

    def weight_out(i, carry):
        r = pl.ds(pl.multiple_of(i * 32, 32), 32)
        dwg_ref[r, :] = acc[r, 0:F].astype(BF16)
        dwu_ref[r, :] = acc[r, F:2 * F].astype(BF16)
        return carry

    lax.fori_loop(0, D // 32, weight_out, 0)

    both_r(1).wait_send()
    for g in (6, 7):
        send_p(g).wait_send()
    of_rows(dy_all, 14 * H, dy_s.at[0], dy_r.at[0]).wait_send()
    for c, m in ((0, 14 * H - 4 * SHIFT), (1, 14 * H + 4 * SHIFT)):
        @pl.when(core == c)
        def _():
            of_rows(x_all, m, x_s.at[0], x_r.at[0]).wait_send()

    ends = remote(last, last, l_s.at[0], l_r.at[0], nx)
    ends.wait_send()
    ends.wait_recv()


def finish(own, last, dwg, dwu, dwd, dx_ref, dwg_ref, dwu_ref, dwd_ref, dx, sem, dx_sem):
    copies = [
        pltpu.make_async_copy(src, dst, sem.at[i])
        for i, (src, dst) in enumerate(((dwd, dwd_ref), (dwg, dwg_ref), (dwu, dwu_ref)))
    ]
    for c in copies:
        c.start()
    for q in range(B // LAST):
        k, i = 1 - q * LAST // H, q * LAST % H

        def add(n, carry):
            r = pl.ds(pl.multiple_of(q * LAST + n * 32, 32), 32)
            dx[r, :] = (own[r, :] + last[k, pl.ds(pl.multiple_of(i + n * 32, 32), 32), :].astype(F32)).astype(BF16)
            return carry

        lax.fori_loop(0, LAST // 32, add, 0)
        r = pl.ds(q * LAST, LAST)
        copies.append(pltpu.make_async_copy(dx.at[r], dx_ref.at[r], dx_sem.at[q]))
        copies[-1].start()
    for c in copies:
        c.wait()


def solution(mesh):
    def local(*args):
        any_ = pl.BlockSpec(memory_space=pl.ANY)
        dma = pltpu.SemaphoreType.DMA
        vmem = pl.BlockSpec(memory_space=pltpu.VMEM)
        grads = [(D, F), (D, F), (F, D)]
        kept = pl.pallas_call(
            kernel,
            out_shape=[pltpu.VMEM((B, D), F32), pltpu.VMEM((2, H, D), BF16)]
            + [pltpu.VMEM(s, BF16) for s in grads]
            + [jax.ShapeDtypeStruct(s, BF16) for s in ((8 * B, D), (8 * B, D), (2, B, D))],
            in_specs=[any_] * 7,
            out_specs=[vmem] * 5 + [any_] * 3,
            scratch_shapes=[
                pltpu.VMEM((F, D), BF16),
                pltpu.VMEM((D, 2 * F), BF16),
                pltpu.VMEM((8 * B, 2 * F), BF16),
                pltpu.VMEM((D, 2 * F), F32),
                pltpu.VMEM((2, B, D), BF16),
                pltpu.VMEM((2, B, F), BF16),
                pltpu.VMEM((B, F), F32),
                pltpu.VMEM((B, F), BF16),
                pltpu.VMEM((4, H, D), BF16),
                pltpu.VMEM((2, H, D), BF16),
                pltpu.VMEM((4, H, D), BF16),
            ]
            + [dma((n,)) for n in (1, 3, 4, 1, 3, 4, 2, 2, 2, 2, 1, 1, 2, 2, 1)],
            compiler_params=pltpu.CompilerParams(collective_id=0, has_side_effects=True, vmem_limit_bytes=50 * 2**20),
            name="backward",
        )(*args)
        return tuple(
            pl.pallas_call(
                finish,
                out_shape=[jax.ShapeDtypeStruct(s, BF16) for s in [(B, D), *grads]],
                in_specs=[vmem] * 5,
                out_specs=[any_] * 4,
                scratch_shapes=[pltpu.VMEM((B, D), BF16), dma((3,)), dma((B // LAST,))],
                compiler_params=pltpu.CompilerParams(vmem_limit_bytes=24 * 2**20),
                name="finish",
            )(*kept[:5])
        )

    rows, cols = P(("dp", "tp"), None), P("dp", "tp")
    return jax.shard_map(
        local,
        mesh=mesh,
        in_specs=(rows, rows, cols, cols, P(None, "tp"), P(None, "tp"), P("tp", None)),
        out_specs=(rows, cols, cols, rows),
        check_vma=False,
    )
```

```python
import functools

import jax
import jax.numpy as jnp
from jax import lax
from jax.experimental import pallas as pl
from jax.experimental.pallas import tpu as pltpu
from jax.sharding import PartitionSpec as P

D = 2048
F = 640
B = 512
H = 256
LAST = 128
SHIFT = 24
F32 = jnp.float32
BF16 = jnp.bfloat16
NT = (((1,), (1,)), ((), ()))
TN = (((0,), (0,)), ((), ()))
C0 = 0.7978845608028654
C1 = 0.7978845608028654 * 0.044715


def kernel(
    x_ref, dy_ref, gate_ref, up_ref, wg_ref, wu_ref, wd_ref,
    own, last, dwg_ref, dwu_ref, dwd_ref, dy_all, x_all, rs_in,
    wd, wgu, dgu, acc, tok, guv, dh, hid, p_in, p_out, rs_out,
    dy_s, dy_r, dyp_r, x_s, x_r, xp_r, p_s, p_r, r_s, r_r, l_s, l_r, w_sem, t_sem, g_sem, go,
):
    me = lax.axis_index("tp")
    core, iy, ix = me % 2, (me // 2) % 2, me // 4
    other = 1 - 2 * core
    partner = me + other
    ny = me + 2 - 4 * iy
    nx = me + 4 - 8 * ix
    nd = ny + 4 - 8 * ix

    place = ix + iy
    barrier = pltpu.get_barrier_semaphore()

    def signal(sem, devs):
        for d in devs:
            pl.semaphore_signal(sem, inc=1, device_id={"tp": d}, device_id_type=pl.DeviceIdType.MESH)

    signal(barrier, (partner,))

    @pl.when(place < 2)
    def _():
        signal(barrier, (nx, ny))

    pl.semaphore_wait(barrier, jnp.where(place == 1, 2, 3))

    @pl.when(place == 2)
    def _():
        signal(go, (nx, ny))

    def owner(g):
        return jnp.where(g < 2, me, jnp.where(g >= 6, nd, jnp.where(g % 2 == 0, nx, ny)))

    def half(g):
        return jnp.where(g == 4, 1, jnp.where(g == 5, 0, g % 2))

    def rows(dev, h, n=H):
        return pl.ds(pl.multiple_of(dev * B + h * H, H), n)

    def remote(src, dst, ss, rs, dev):
        return pltpu.make_async_remote_copy(
            src_ref=src, dst_ref=dst, send_sem=ss, recv_sem=rs, device_id={"tp": dev}, device_id_type=pl.DeviceIdType.MESH
        )

    def of_rows(full, n, ss, rs):
        return remote(full.at[pl.ds(0, n)], full.at[pl.ds(0, n)], ss, rs, partner)

    def start_own(ref, full, s, r, pr, to="xyp"):
        for n in range(2):
            for t in to:
                h = 1 - n if t == "y" else n
                sem, dev = {"x": (r.at[n], nx), "y": (r.at[n], ny), "p": (pr.at[0], partner)}[t]
                remote(ref.at[pl.ds(h * H, H)], full.at[rows(me, h)], s.at[0], sem, dev).start()

    def send_on(full, s, r, g, n, dev):
        q = rows(owner(g), half(g), n)
        remote(full.at[q], full.at[q], s.at[0], r, dev).start()

    def relay(full, s, r, pr, p, onward):
        of_rows(full, 2 * H, s.at[0], r.at[p - 1]).wait_recv()
        if onward:
            send_on(full, s, r.at[2], 2, H, ny)
            send_on(full, s, r.at[2], 3, H, nx)
        for g in (2 * p, 2 * p + 1):
            send_on(full, s, pr.at[p], g, H, partner)

    def from_partner(full, s, pr, p):
        of_rows(full, 2 * H, s.at[0], pr.at[p]).wait_recv()

    def load(ref, full, g):
        o, h, slot = owner(g), half(g), g % 2
        pltpu.make_async_copy(full.at[rows(o + other, h)], tok.at[slot, pl.ds(0, H)], t_sem.at[slot]).start()

        @pl.when(g < 2)
        def _():
            src = ref.at[pl.ds(pl.multiple_of(h * H, H), H)]
            pltpu.make_async_copy(src, tok.at[slot, pl.ds(H, H)], t_sem.at[slot]).start()

        @pl.when(g >= 2)
        def _():
            pltpu.make_async_copy(full.at[rows(o, h)], tok.at[slot, pl.ds(H, H)], t_sem.at[slot]).start()

    def loaded(slot):
        pltpu.make_async_copy(dy_all.at[pl.ds(0, B)], tok.at[slot], t_sem.at[slot]).wait()

    def load_gates(g):
        o, h = owner(g), half(g)
        for i, src in enumerate((gate_ref, up_ref)):
            pltpu.make_async_copy(src.at[rows(o + other, h)], guv.at[i, pl.ds(0, H)], g_sem.at[0]).start()
            pltpu.make_async_copy(src.at[rows(o, h)], guv.at[i, pl.ds(H, H)], g_sem.at[0]).start()

    @pl.when(place != 1)
    def _():
        start_own(dy_ref, dy_all, dy_s, dy_r, dyp_r)

    for i, first, then in ((1, "xp", "y"), (0, "yp", "x")):
        @pl.when(jnp.logical_and(place == 1, ix == i))
        def _():
            start_own(dy_ref, dy_all, dy_s, dy_r, dyp_r, first)
            pl.semaphore_wait(go, 1)
            start_own(dy_ref, dy_all, dy_s, dy_r, dyp_r, then)

    pltpu.make_async_copy(wd_ref, wd, w_sem.at[0]).start()
    load_gates(0)
    pltpu.make_async_copy(wg_ref, wgu.at[:, pl.ds(0, F)], w_sem.at[1]).start()
    pltpu.make_async_copy(wu_ref, wgu.at[:, pl.ds(F, F)], w_sem.at[1]).start()
    from_partner(dy_all, dy_s, dyp_r, 0)
    load(dy_ref, dy_all, 0)
    acc[...] = jnp.zeros_like(acc)
    pltpu.make_async_copy(wd_ref, wd, w_sem.at[0]).wait()
    pltpu.make_async_copy(wgu, wgu, w_sem.at[1]).wait()

    def p_slot(g):
        return jnp.where(jnp.logical_or(g == 4, g == 5), g - 2, g % 2)

    def send_p(g):
        return remote(p_out.at[g % 2], p_in.at[p_slot(g)], p_s.at[g % 2], p_r.at[g % 2], partner)

    def send_r(stage, kind, k, dev):
        return remote(rs_out.at[stage], rs_in.at[kind, pl.ds(k * H, H)], r_s.at[kind], r_r.at[kind], dev)

    def both_r(kind):
        return remote(rs_in.at[kind], rs_in.at[kind], r_s.at[kind], r_r.at[kind], nx)

    def send_last(k, dev):
        return remote(rs_out.at[k], last.at[k], l_s.at[0], l_r.at[0], dev)

    def dx_tile(g, r0, j):
        a = dgu[pl.ds(pl.multiple_of(g * B + r0, H), H), :]
        w = wgu[pl.ds(pl.multiple_of(j * 512, 512), 512), :]
        return lax.dot_general(a, w, NT, preferred_element_type=F32)

    def first_pass(g, carry):
        slot = g % 2
        loaded(slot)
        pltpu.make_async_copy(guv, guv, g_sem.at[0]).wait()

        @pl.when(slot == 0)
        def _():
            load(dy_ref, dy_all, g + 1)

        for n0, n in ((0, 256), (256, 256), (512, 128)):
            dh[:, n0:n0 + n] = lax.dot_general(tok[slot], wd[n0:n0 + n, :], NT, preferred_element_type=F32)

        def gates(i, carry):
            r = pl.ds(pl.multiple_of(i * 32, 32), 32)
            a, u, d = guv[0, r, :].astype(F32), guv[1, r, :].astype(F32), dh[r, :]
            a2 = a * a
            t = jnp.tanh(a * (C0 + C1 * a2))
            cdf = 0.5 + 0.5 * t
            gelu = a * cdf
            slope = cdf + (0.5 * a) * ((1.0 - t * t) * (C0 + (3.0 * C1) * a2))
            hid[r, :] = (gelu * u).astype(BF16)
            q = pl.ds(pl.multiple_of(g * B + i * 32, 32), 32)
            dgu[q, 0:F] = (d * u * slope).astype(BF16)
            dgu[q, F:2 * F] = (d * gelu).astype(BF16)
            return carry

        lax.fori_loop(0, B // 32, gates, 0)

        @pl.when(g < 7)
        def _():
            load_gates(g + 1)

        @pl.when(g >= 2)
        def _():
            send_p(g - 2).wait_send()

        def p_rows(j, carry):
            p_out[slot, :, pl.ds(pl.multiple_of(j * 512, 512), 512)] = dx_tile(g, 0, j).astype(BF16)
            return carry

        lax.fori_loop(0, 4, p_rows, 0)
        send_p(g).start()

        def down(j, carry):
            s = pl.ds(pl.multiple_of(j * 512, 512), 512)
            r, c = pl.ds(pl.multiple_of((j // 2) * F, F), F), pl.ds(pl.multiple_of((j % 2) * 512, 512), 512)
            acc[r, c] += lax.dot_general(hid[...], tok[slot, :, s], TN, preferred_element_type=F32)
            return carry

        lax.fori_loop(0, 4, down, 0)

        for p in (1, 2, 3):
            @pl.when(g == 2 * p - 1)
            def _():
                relay(dy_all, dy_s, dy_r, dyp_r, p, p == 1)
                if p == 1:
                    start_own(x_ref, x_all, x_s, x_r, xp_r)
                from_partner(dy_all, dy_s, dyp_r, p)
                load(dy_ref, dy_all, g + 1)

        @pl.when(g == 7)
        def _():
            from_partner(x_all, x_s, xp_r, 0)
            load(x_ref, x_all, 0)

        send_p(g).wait_recv()

        @pl.when(jnp.logical_or(g < 4, g >= 6))
        def _():
            def m_rows(j, carry):
                s = pl.ds(pl.multiple_of(j * 512, 512), 512)
                total = dx_tile(g, H, j) + p_in[p_slot(g), :, s].astype(F32)

                @pl.when(g < 2)
                def _():
                    own[pl.ds(pl.multiple_of(slot * H, H), H), s] = total

                @pl.when(g >= 2)
                def _():
                    rs_out[jnp.where(g >= 6, g - 4, slot), :, s] = total.astype(BF16)

                return carry

            lax.fori_loop(0, 4, m_rows, 0)

        for group, stage, kind, k, dev in ((2, 0, 0, 0, nx), (3, 1, 0, 1, ny), (6, 2, 1, 1, nx), (7, 3, 1, 0, ny)):
            @pl.when(g == group)
            def _():
                send_r(stage, kind, k, dev).start()

        return carry

    lax.fori_loop(0, 8, first_pass, 0)

    for j in range(4):
        dwd_ref[:, j * 512:j * 512 + 512] = acc[j // 2 * F:j // 2 * F + F, j % 2 * 512:j % 2 * 512 + 512].astype(BF16)
    acc[...] = jnp.zeros_like(acc)

    def tail(g):
        return pl.ds(pl.multiple_of((owner(g) - core) * B + half(g) * H + H - SHIFT, 8), SHIFT)

    def send_tail(g, r, dev):
        remote(x_all.at[tail(g)], x_all.at[tail(g)], x_s.at[0], r, dev).start()

    def second_pass(g, carry):
        slot = g % 2
        loaded(slot)

        @pl.when(slot == 0)
        def _():
            load(x_ref, x_all, g + 1)

        @pl.when(g == 1)
        def _():
            relay(x_all, x_s, x_r, xp_r, 1, False)
            for c, n in ((0, H - SHIFT), (1, H)):
                @pl.when(core == c)
                def _():
                    send_on(x_all, x_s, x_r.at[2], 2, n, ny)
                    send_on(x_all, x_s, x_r.at[2], 3, n, nx)

            from_partner(x_all, x_s, xp_r, 1)

            @pl.when(core == 1)
            def _():
                send_tail(2, x_r.at[2], ny)
                send_tail(3, x_r.at[2], nx)

            load(x_ref, x_all, 2)

        @pl.when(g == 3)
        def _():
            relay(x_all, x_s, x_r, xp_r, 2, False)
            from_partner(x_all, x_s, xp_r, 2)
            load(x_ref, x_all, 4)

        def weight(j, carry):
            s = pl.ds(pl.multiple_of(j * 512, 512), 512)
            d = dgu[pl.ds(pl.multiple_of(g * B, B), B), :]
            acc[s, :] += lax.dot_general(tok[slot, :, s], d, TN, preferred_element_type=F32)
            return carry

        lax.fori_loop(0, 4, weight, 0)

        @pl.when(g == 5)
        def _():
            for kind in range(2):
                both_r(kind).wait_recv()
                pltpu.make_async_copy(rs_in.at[kind], tok.at[kind], t_sem.at[kind]).start()
            both_r(0).wait_send()
            loaded(0)

            def add(i, carry):
                r = pl.ds(pl.multiple_of(i * 32, 32), 32)
                own[r, :] += tok[0, r, :].astype(F32)
                return carry

            lax.fori_loop(0, B // 32, add, 0)
            loaded(1)
            for k, dev in enumerate((nx, ny)):
                def late(j, carry):
                    s = pl.ds(pl.multiple_of(j * 512, 512), 512)
                    total = dx_tile(4 + k, H, j) + p_in[2 + k, :, s].astype(F32) + tok[1, k * H:(k + 1) * H, s].astype(F32)
                    rs_out[k, :, s] = total.astype(BF16)
                    return carry

                lax.fori_loop(0, 4, late, 0)
                send_last(k, dev).start()

            for c, n, m in ((0, H - SHIFT, 2 * H + 2 * SHIFT), (1, H, 2 * H - 2 * SHIFT)):
                @pl.when(core == c)
                def _():
                    of_rows(x_all, 4 * H - m, x_s.at[0], x_r.at[2]).wait_recv()
                    send_on(x_all, x_s, xp_r.at[3], 6, n, partner)
                    send_on(x_all, x_s, xp_r.at[3], 7, n, partner)
                    if c == 1:
                        send_tail(6, xp_r.at[3], partner)
                        send_tail(7, xp_r.at[3], partner)
                    of_rows(x_all, m, x_s.at[0], xp_r.at[3]).wait_recv()

            load(x_ref, x_all, 6)

        return carry

    lax.fori_loop(0, 8, second_pass, 0)

    def weight_out(i, carry):
        r = pl.ds(pl.multiple_of(i * 32, 32), 32)
        dwg_ref[r, :] = acc[r, 0:F].astype(BF16)
        dwu_ref[r, :] = acc[r, F:2 * F].astype(BF16)
        return carry

    lax.fori_loop(0, D // 32, weight_out, 0)

    both_r(1).wait_send()
    for g in (6, 7):
        send_p(g).wait_send()
    of_rows(dy_all, 14 * H, dy_s.at[0], dy_r.at[0]).wait_send()
    for c, m in ((0, 14 * H - 4 * SHIFT), (1, 14 * H + 4 * SHIFT)):
        @pl.when(core == c)
        def _():
            of_rows(x_all, m, x_s.at[0], x_r.at[0]).wait_send()

    ends = remote(last, last, l_s.at[0], l_r.at[0], nx)
    ends.wait_send()
    ends.wait_recv()


def finish(own, last, dwg, dwu, dwd, dx_ref, dwg_ref, dwu_ref, dwd_ref, dx, sem, dx_sem):
    copies = [
        pltpu.make_async_copy(src, dst, sem.at[i])
        for i, (src, dst) in enumerate(((dwd, dwd_ref), (dwg, dwg_ref), (dwu, dwu_ref)))
    ]
    for c in copies:
        c.start()
    for q in range(B // LAST):
        k, i = 1 - q * LAST // H, q * LAST % H

        def add(n, carry):
            r = pl.ds(pl.multiple_of(q * LAST + n * 32, 32), 32)
            dx[r, :] = (own[r, :] + last[k, pl.ds(pl.multiple_of(i + n * 32, 32), 32), :].astype(F32)).astype(BF16)
            return carry

        lax.fori_loop(0, LAST // 32, add, 0)
        r = pl.ds(q * LAST, LAST)
        copies.append(pltpu.make_async_copy(dx.at[r], dx_ref.at[r], dx_sem.at[q]))
        copies[-1].start()
    for c in copies:
        c.wait()


def solution(mesh):
    def local(*args):
        any_ = pl.BlockSpec(memory_space=pl.ANY)
        dma = pltpu.SemaphoreType.DMA
        vmem = pl.BlockSpec(memory_space=pltpu.VMEM)
        grads = [(D, F), (D, F), (F, D)]
        kept = pl.pallas_call(
            kernel,
            out_shape=[pltpu.VMEM((B, D), F32), pltpu.VMEM((2, H, D), BF16)]
            + [pltpu.VMEM(s, BF16) for s in grads]
            + [jax.ShapeDtypeStruct(s, BF16) for s in ((8 * B, D), (8 * B, D), (2, B, D))],
            in_specs=[any_] * 7,
            out_specs=[vmem] * 5 + [any_] * 3,
            scratch_shapes=[
                pltpu.VMEM((F, D), BF16),
                pltpu.VMEM((D, 2 * F), BF16),
                pltpu.VMEM((8 * B, 2 * F), BF16),
                pltpu.VMEM((D, 2 * F), F32),
                pltpu.VMEM((2, B, D), BF16),
                pltpu.VMEM((2, B, F), BF16),
                pltpu.VMEM((B, F), F32),
                pltpu.VMEM((B, F), BF16),
                pltpu.VMEM((4, H, D), BF16),
                pltpu.VMEM((2, H, D), BF16),
                pltpu.VMEM((4, H, D), BF16),
            ]
            + [dma((n,)) for n in (1, 3, 4, 1, 3, 4, 2, 2, 2, 2, 1, 1, 2, 2, 1)]
            + [pltpu.SemaphoreType.REGULAR],
            compiler_params=pltpu.CompilerParams(collective_id=0, has_side_effects=True, vmem_limit_bytes=50 * 2**20),
            name="backward",
        )(*args)
        return tuple(
            pl.pallas_call(
                finish,
                out_shape=[jax.ShapeDtypeStruct(s, BF16) for s in [(B, D), *grads]],
                in_specs=[vmem] * 5,
                out_specs=[any_] * 4,
                scratch_shapes=[pltpu.VMEM((B, D), BF16), dma((3,)), dma((B // LAST,))],
                compiler_params=pltpu.CompilerParams(vmem_limit_bytes=24 * 2**20),
                name="finish",
            )(*kept[:5])
        )

    rows, cols = P(("dp", "tp"), None), P("dp", "tp")
    return jax.shard_map(
        local,
        mesh=mesh,
        in_specs=(rows, rows, cols, cols, P(None, "tp"), P(None, "tp"), P("tp", None)),
        out_specs=(rows, cols, cols, rows),
        check_vma=False,
    )
```

```python
import functools

import jax
import jax.numpy as jnp
from jax import lax
from jax.experimental import pallas as pl
from jax.experimental.pallas import tpu as pltpu
from jax.sharding import PartitionSpec as P

D = 2048
F = 640
B = 512
H = 256
LAST = 128
SHIFT = 24
F32 = jnp.float32
BF16 = jnp.bfloat16
NT = (((1,), (1,)), ((), ()))
TN = (((0,), (0,)), ((), ()))
C0 = 0.7978845608028654
C1 = 0.7978845608028654 * 0.044715


def kernel(
    x_ref, dy_ref, gate_ref, up_ref, wg_ref, wu_ref, wd_ref,
    own, last, dwg_ref, dwu_ref, dwd_ref, dy_all, x_all, rs_in,
    wd, wgu, dgu, acc, tok, guv, dh, hid, p_in, p_out, rs_out,
    dy_s, dy_r, dyp_r, x_s, x_r, xp_r, p_s, p_r, r_s, r_r, l_s, l_r, w_sem, t_sem, g_sem, go_chip, go_core,
):
    me = lax.axis_index("tp")
    core, iy, ix = me % 2, (me // 2) % 2, me // 4
    other = 1 - 2 * core
    partner = me + other
    ny = me + 2 - 4 * iy
    nx = me + 4 - 8 * ix
    nd = ny + 4 - 8 * ix

    place = ix + iy
    barrier = pltpu.get_barrier_semaphore()

    def signal(sem, devs):
        for d in devs:
            pl.semaphore_signal(sem, inc=1, device_id={"tp": d}, device_id_type=pl.DeviceIdType.MESH)

    @pl.when(place < 2)
    def _():
        signal(barrier, (nx, ny))

    @pl.when(core == 1)
    def _():
        signal(barrier, (partner,))

    pl.semaphore_wait(barrier, jnp.where(place == 1, 1, 2) + 1 - core)

    @pl.when(core == 0)
    def _():
        signal(go_core, (partner,))

    @pl.when(place == 2)
    def _():
        signal(go_chip, (nx, ny))

    def owner(g):
        return jnp.where(g < 2, me, jnp.where(g >= 6, nd, jnp.where(g % 2 == 0, nx, ny)))

    def half(g):
        return jnp.where(g == 4, 1, jnp.where(g == 5, 0, g % 2))

    def rows(dev, h, n=H):
        return pl.ds(pl.multiple_of(dev * B + h * H, H), n)

    def remote(src, dst, ss, rs, dev):
        return pltpu.make_async_remote_copy(
            src_ref=src, dst_ref=dst, send_sem=ss, recv_sem=rs, device_id={"tp": dev}, device_id_type=pl.DeviceIdType.MESH
        )

    def of_rows(full, n, ss, rs):
        return remote(full.at[pl.ds(0, n)], full.at[pl.ds(0, n)], ss, rs, partner)

    def start_own(ref, full, s, r, pr, to="xyp"):
        for n in range(2):
            for t in to:
                h = 1 - n if t == "y" else n
                sem, dev = {"x": (r.at[n], nx), "y": (r.at[n], ny), "p": (pr.at[0], partner)}[t]
                remote(ref.at[pl.ds(h * H, H)], full.at[rows(me, h)], s.at[0], sem, dev).start()

    def send_on(full, s, r, g, n, dev):
        q = rows(owner(g), half(g), n)
        remote(full.at[q], full.at[q], s.at[0], r, dev).start()

    def relay(full, s, r, pr, p, onward):
        of_rows(full, 2 * H, s.at[0], r.at[p - 1]).wait_recv()
        if onward:
            send_on(full, s, r.at[2], 2, H, ny)
            send_on(full, s, r.at[2], 3, H, nx)
        for g in (2 * p, 2 * p + 1):
            send_on(full, s, pr.at[p], g, H, partner)

    def from_partner(full, s, pr, p):
        of_rows(full, 2 * H, s.at[0], pr.at[p]).wait_recv()

    def load(ref, full, g):
        o, h, slot = owner(g), half(g), g % 2
        pltpu.make_async_copy(full.at[rows(o + other, h)], tok.at[slot, pl.ds(0, H)], t_sem.at[slot]).start()

        @pl.when(g < 2)
        def _():
            src = ref.at[pl.ds(pl.multiple_of(h * H, H), H)]
            pltpu.make_async_copy(src, tok.at[slot, pl.ds(H, H)], t_sem.at[slot]).start()

        @pl.when(g >= 2)
        def _():
            pltpu.make_async_copy(full.at[rows(o, h)], tok.at[slot, pl.ds(H, H)], t_sem.at[slot]).start()

    def loaded(slot):
        pltpu.make_async_copy(dy_all.at[pl.ds(0, B)], tok.at[slot], t_sem.at[slot]).wait()

    def load_gates(g):
        o, h = owner(g), half(g)
        for i, src in enumerate((gate_ref, up_ref)):
            pltpu.make_async_copy(src.at[rows(o + other, h)], guv.at[i, pl.ds(0, H)], g_sem.at[0]).start()
            pltpu.make_async_copy(src.at[rows(o, h)], guv.at[i, pl.ds(H, H)], g_sem.at[0]).start()

    def start_dy(to):
        start_own(dy_ref, dy_all, dy_s, dy_r, dyp_r, to)

    @pl.when(place != 1)
    def _():
        start_dy("xy")

    for i, first in ((1, "x"), (0, "y")):
        @pl.when(jnp.logical_and(place == 1, ix == i))
        def _():
            start_dy(first)

    @pl.when(core == 1)
    def _():
        pl.semaphore_wait(go_core, 1)

    start_dy("p")

    @pl.when(place == 1)
    def _():
        pl.semaphore_wait(go_chip, 1)

    for i, then in ((1, "y"), (0, "x")):
        @pl.when(jnp.logical_and(place == 1, ix == i))
        def _():
            start_dy(then)

    pltpu.make_async_copy(wd_ref, wd, w_sem.at[0]).start()
    load_gates(0)
    pltpu.make_async_copy(wg_ref, wgu.at[:, pl.ds(0, F)], w_sem.at[1]).start()
    pltpu.make_async_copy(wu_ref, wgu.at[:, pl.ds(F, F)], w_sem.at[1]).start()
    from_partner(dy_all, dy_s, dyp_r, 0)
    load(dy_ref, dy_all, 0)
    acc[...] = jnp.zeros_like(acc)
    pltpu.make_async_copy(wd_ref, wd, w_sem.at[0]).wait()
    pltpu.make_async_copy(wgu, wgu, w_sem.at[1]).wait()

    def p_slot(g):
        return jnp.where(jnp.logical_or(g == 4, g == 5), g - 2, g % 2)

    def send_p(g):
        return remote(p_out.at[g % 2], p_in.at[p_slot(g)], p_s.at[g % 2], p_r.at[g % 2], partner)

    def send_r(stage, kind, k, dev):
        return remote(rs_out.at[stage], rs_in.at[kind, pl.ds(k * H, H)], r_s.at[kind], r_r.at[kind], dev)

    def both_r(kind):
        return remote(rs_in.at[kind], rs_in.at[kind], r_s.at[kind], r_r.at[kind], nx)

    def send_last(k, dev):
        return remote(rs_out.at[k], last.at[k], l_s.at[0], l_r.at[0], dev)

    def dx_tile(g, r0, j):
        a = dgu[pl.ds(pl.multiple_of(g * B + r0, H), H), :]
        w = wgu[pl.ds(pl.multiple_of(j * 512, 512), 512), :]
        return lax.dot_general(a, w, NT, preferred_element_type=F32)

    def first_pass(g, carry):
        slot = g % 2
        loaded(slot)
        pltpu.make_async_copy(guv, guv, g_sem.at[0]).wait()

        @pl.when(slot == 0)
        def _():
            load(dy_ref, dy_all, g + 1)

        for n0, n in ((0, 256), (256, 256), (512, 128)):
            dh[:, n0:n0 + n] = lax.dot_general(tok[slot], wd[n0:n0 + n, :], NT, preferred_element_type=F32)

        def gates(i, carry):
            r = pl.ds(pl.multiple_of(i * 32, 32), 32)
            a, u, d = guv[0, r, :].astype(F32), guv[1, r, :].astype(F32), dh[r, :]
            a2 = a * a
            t = jnp.tanh(a * (C0 + C1 * a2))
            cdf = 0.5 + 0.5 * t
            gelu = a * cdf
            slope = cdf + (0.5 * a) * ((1.0 - t * t) * (C0 + (3.0 * C1) * a2))
            hid[r, :] = (gelu * u).astype(BF16)
            q = pl.ds(pl.multiple_of(g * B + i * 32, 32), 32)
            dgu[q, 0:F] = (d * u * slope).astype(BF16)
            dgu[q, F:2 * F] = (d * gelu).astype(BF16)
            return carry

        lax.fori_loop(0, B // 32, gates, 0)

        @pl.when(g < 7)
        def _():
            load_gates(g + 1)

        @pl.when(g >= 2)
        def _():
            send_p(g - 2).wait_send()

        def p_rows(j, carry):
            p_out[slot, :, pl.ds(pl.multiple_of(j * 512, 512), 512)] = dx_tile(g, 0, j).astype(BF16)
            return carry

        lax.fori_loop(0, 4, p_rows, 0)
        send_p(g).start()

        def down(j, carry):
            s = pl.ds(pl.multiple_of(j * 512, 512), 512)
            r, c = pl.ds(pl.multiple_of((j // 2) * F, F), F), pl.ds(pl.multiple_of((j % 2) * 512, 512), 512)
            acc[r, c] += lax.dot_general(hid[...], tok[slot, :, s], TN, preferred_element_type=F32)
            return carry

        lax.fori_loop(0, 4, down, 0)

        for p in (1, 2, 3):
            @pl.when(g == 2 * p - 1)
            def _():
                relay(dy_all, dy_s, dy_r, dyp_r, p, p == 1)
                if p == 1:
                    start_own(x_ref, x_all, x_s, x_r, xp_r)
                from_partner(dy_all, dy_s, dyp_r, p)
                load(dy_ref, dy_all, g + 1)

        @pl.when(g == 7)
        def _():
            from_partner(x_all, x_s, xp_r, 0)
            load(x_ref, x_all, 0)

        send_p(g).wait_recv()

        @pl.when(jnp.logical_or(g < 4, g >= 6))
        def _():
            def m_rows(j, carry):
                s = pl.ds(pl.multiple_of(j * 512, 512), 512)
                total = dx_tile(g, H, j) + p_in[p_slot(g), :, s].astype(F32)

                @pl.when(g < 2)
                def _():
                    own[pl.ds(pl.multiple_of(slot * H, H), H), s] = total

                @pl.when(g >= 2)
                def _():
                    rs_out[jnp.where(g >= 6, g - 4, slot), :, s] = total.astype(BF16)

                return carry

            lax.fori_loop(0, 4, m_rows, 0)

        for group, stage, kind, k, dev in ((2, 0, 0, 0, nx), (3, 1, 0, 1, ny), (6, 2, 1, 1, nx), (7, 3, 1, 0, ny)):
            @pl.when(g == group)
            def _():
                send_r(stage, kind, k, dev).start()

        return carry

    lax.fori_loop(0, 8, first_pass, 0)

    for j in range(4):
        dwd_ref[:, j * 512:j * 512 + 512] = acc[j // 2 * F:j // 2 * F + F, j % 2 * 512:j % 2 * 512 + 512].astype(BF16)
    acc[...] = jnp.zeros_like(acc)

    def tail(g):
        return pl.ds(pl.multiple_of((owner(g) - core) * B + half(g) * H + H - SHIFT, 8), SHIFT)

    def send_tail(g, r, dev):
        remote(x_all.at[tail(g)], x_all.at[tail(g)], x_s.at[0], r, dev).start()

    def second_pass(g, carry):
        slot = g % 2
        loaded(slot)

        @pl.when(slot == 0)
        def _():
            load(x_ref, x_all, g + 1)

        @pl.when(g == 1)
        def _():
            relay(x_all, x_s, x_r, xp_r, 1, False)
            for c, n in ((0, H - SHIFT), (1, H)):
                @pl.when(core == c)
                def _():
                    send_on(x_all, x_s, x_r.at[2], 2, n, ny)
                    send_on(x_all, x_s, x_r.at[2], 3, n, nx)

            from_partner(x_all, x_s, xp_r, 1)

            @pl.when(core == 1)
            def _():
                send_tail(2, x_r.at[2], ny)
                send_tail(3, x_r.at[2], nx)

            load(x_ref, x_all, 2)

        @pl.when(g == 3)
        def _():
            relay(x_all, x_s, x_r, xp_r, 2, False)
            from_partner(x_all, x_s, xp_r, 2)
            load(x_ref, x_all, 4)

        def weight(j, carry):
            s = pl.ds(pl.multiple_of(j * 512, 512), 512)
            d = dgu[pl.ds(pl.multiple_of(g * B, B), B), :]
            acc[s, :] += lax.dot_general(tok[slot, :, s], d, TN, preferred_element_type=F32)
            return carry

        lax.fori_loop(0, 4, weight, 0)

        @pl.when(g == 5)
        def _():
            for kind in range(2):
                both_r(kind).wait_recv()
                pltpu.make_async_copy(rs_in.at[kind], tok.at[kind], t_sem.at[kind]).start()
            both_r(0).wait_send()
            loaded(0)

            def add(i, carry):
                r = pl.ds(pl.multiple_of(i * 32, 32), 32)
                own[r, :] += tok[0, r, :].astype(F32)
                return carry

            lax.fori_loop(0, B // 32, add, 0)
            loaded(1)
            for k, dev in enumerate((nx, ny)):
                def late(j, carry):
                    s = pl.ds(pl.multiple_of(j * 512, 512), 512)
                    total = dx_tile(4 + k, H, j) + p_in[2 + k, :, s].astype(F32) + tok[1, k * H:(k + 1) * H, s].astype(F32)
                    rs_out[k, :, s] = total.astype(BF16)
                    return carry

                lax.fori_loop(0, 4, late, 0)
                send_last(k, dev).start()

            for c, n, m in ((0, H - SHIFT, 2 * H + 2 * SHIFT), (1, H, 2 * H - 2 * SHIFT)):
                @pl.when(core == c)
                def _():
                    of_rows(x_all, 4 * H - m, x_s.at[0], x_r.at[2]).wait_recv()
                    send_on(x_all, x_s, xp_r.at[3], 6, n, partner)
                    send_on(x_all, x_s, xp_r.at[3], 7, n, partner)
                    if c == 1:
                        send_tail(6, xp_r.at[3], partner)
                        send_tail(7, xp_r.at[3], partner)
                    of_rows(x_all, m, x_s.at[0], xp_r.at[3]).wait_recv()

            load(x_ref, x_all, 6)

        return carry

    lax.fori_loop(0, 8, second_pass, 0)

    def weight_out(i, carry):
        r = pl.ds(pl.multiple_of(i * 32, 32), 32)
        dwg_ref[r, :] = acc[r, 0:F].astype(BF16)
        dwu_ref[r, :] = acc[r, F:2 * F].astype(BF16)
        return carry

    lax.fori_loop(0, D // 32, weight_out, 0)

    both_r(1).wait_send()
    for g in (6, 7):
        send_p(g).wait_send()
    of_rows(dy_all, 14 * H, dy_s.at[0], dy_r.at[0]).wait_send()
    for c, m in ((0, 14 * H - 4 * SHIFT), (1, 14 * H + 4 * SHIFT)):
        @pl.when(core == c)
        def _():
            of_rows(x_all, m, x_s.at[0], x_r.at[0]).wait_send()

    ends = remote(last, last, l_s.at[0], l_r.at[0], nx)
    ends.wait_send()
    ends.wait_recv()


def finish(own, last, dwg, dwu, dwd, dx_ref, dwg_ref, dwu_ref, dwd_ref, dx, sem, dx_sem):
    copies = [
        pltpu.make_async_copy(src, dst, sem.at[i])
        for i, (src, dst) in enumerate(((dwd, dwd_ref), (dwg, dwg_ref), (dwu, dwu_ref)))
    ]
    for c in copies:
        c.start()
    for q in range(B // LAST):
        k, i = 1 - q * LAST // H, q * LAST % H

        def add(n, carry):
            r = pl.ds(pl.multiple_of(q * LAST + n * 32, 32), 32)
            dx[r, :] = (own[r, :] + last[k, pl.ds(pl.multiple_of(i + n * 32, 32), 32), :].astype(F32)).astype(BF16)
            return carry

        lax.fori_loop(0, LAST // 32, add, 0)
        r = pl.ds(q * LAST, LAST)
        copies.append(pltpu.make_async_copy(dx.at[r], dx_ref.at[r], dx_sem.at[q]))
        copies[-1].start()
    for c in copies:
        c.wait()


def solution(mesh):
    def local(*args):
        any_ = pl.BlockSpec(memory_space=pl.ANY)
        dma = pltpu.SemaphoreType.DMA
        vmem = pl.BlockSpec(memory_space=pltpu.VMEM)
        grads = [(D, F), (D, F), (F, D)]
        kept = pl.pallas_call(
            kernel,
            out_shape=[pltpu.VMEM((B, D), F32), pltpu.VMEM((2, H, D), BF16)]
            + [pltpu.VMEM(s, BF16) for s in grads]
            + [jax.ShapeDtypeStruct(s, BF16) for s in ((8 * B, D), (8 * B, D), (2, B, D))],
            in_specs=[any_] * 7,
            out_specs=[vmem] * 5 + [any_] * 3,
            scratch_shapes=[
                pltpu.VMEM((F, D), BF16),
                pltpu.VMEM((D, 2 * F), BF16),
                pltpu.VMEM((8 * B, 2 * F), BF16),
                pltpu.VMEM((D, 2 * F), F32),
                pltpu.VMEM((2, B, D), BF16),
                pltpu.VMEM((2, B, F), BF16),
                pltpu.VMEM((B, F), F32),
                pltpu.VMEM((B, F), BF16),
                pltpu.VMEM((4, H, D), BF16),
                pltpu.VMEM((2, H, D), BF16),
                pltpu.VMEM((4, H, D), BF16),
            ]
            + [dma((n,)) for n in (1, 3, 4, 1, 3, 4, 2, 2, 2, 2, 1, 1, 2, 2, 1)]
            + [pltpu.SemaphoreType.REGULAR] * 2,
            compiler_params=pltpu.CompilerParams(collective_id=0, has_side_effects=True, vmem_limit_bytes=50 * 2**20),
            name="backward",
        )(*args)
        return tuple(
            pl.pallas_call(
                finish,
                out_shape=[jax.ShapeDtypeStruct(s, BF16) for s in [(B, D), *grads]],
                in_specs=[vmem] * 5,
                out_specs=[any_] * 4,
                scratch_shapes=[pltpu.VMEM((B, D), BF16), dma((3,)), dma((B // LAST,))],
                compiler_params=pltpu.CompilerParams(vmem_limit_bytes=24 * 2**20),
                name="finish",
            )(*kept[:5])
        )

    rows, cols = P(("dp", "tp"), None), P("dp", "tp")
    return jax.shard_map(
        local,
        mesh=mesh,
        in_specs=(rows, rows, cols, cols, P(None, "tp"), P(None, "tp"), P("tp", None)),
        out_specs=(rows, cols, cols, rows),
        check_vma=False,
    )
```

```python
import functools

import jax
import jax.numpy as jnp
from jax import lax
from jax.experimental import pallas as pl
from jax.experimental.pallas import tpu as pltpu
from jax.sharding import PartitionSpec as P

D = 2048
F = 640
B = 512
H = 256
LAST = 128
RS = ((2, 1, 1, 0), (3, 1, 0, 1), (0, 0, 0, 0), (1, 0, 1, 1))
F32 = jnp.float32
BF16 = jnp.bfloat16
NT = (((1,), (1,)), ((), ()))
TN = (((0,), (0,)), ((), ()))
C0 = 0.7978845608028654
C1 = 0.7978845608028654 * 0.044715


def kernel(
    x_ref, dy_ref, gate_ref, up_ref, wg_ref, wu_ref, wd_ref,
    sums, rs_out, dwg_ref, dwu_ref, dwd_ref, dy_all, x_all, rs_in,
    wd, wgu, dgu, acc, tok, guv, dh, hid, p_in, p_out,
    dy_s, dy_r, dyp_r, x_s, x_r, xp_r, p_s, p_r, r_s, r_r, w_sem, t_sem, g_sem, go_chip, go_core,
):
    me = lax.axis_index("tp")
    core, iy, ix = me % 2, (me // 2) % 2, me // 4
    other = 1 - 2 * core
    partner = me + other
    ny = me + 2 - 4 * iy
    nx = me + 4 - 8 * ix
    nd = ny + 4 - 8 * ix

    place = ix + iy
    barrier = pltpu.get_barrier_semaphore()

    def signal(sem, devs):
        for d in devs:
            pl.semaphore_signal(sem, inc=1, device_id={"tp": d}, device_id_type=pl.DeviceIdType.MESH)

    @pl.when(place < 2)
    def _():
        signal(barrier, (nx, ny))

    @pl.when(core == 1)
    def _():
        signal(barrier, (partner,))

    pl.semaphore_wait(barrier, jnp.where(place == 1, 1, 2) + 1 - core)

    @pl.when(core == 0)
    def _():
        signal(go_core, (partner,))

    @pl.when(place == 2)
    def _():
        signal(go_chip, (nx, ny))

    def owner(g):
        return jnp.where(g < 2, me, jnp.where(g >= 6, nd, jnp.where(g % 2 == 0, nx, ny)))

    def half(g):
        return jnp.where(g == 4, 1, jnp.where(g == 5, 0, g % 2))

    def rows(dev, h, n=H):
        return pl.ds(pl.multiple_of(dev * B + h * H, H), n)

    def remote(src, dst, ss, rs, dev):
        return pltpu.make_async_remote_copy(
            src_ref=src, dst_ref=dst, send_sem=ss, recv_sem=rs, device_id={"tp": dev}, device_id_type=pl.DeviceIdType.MESH
        )

    def of_rows(full, n, ss, rs):
        return remote(full.at[pl.ds(0, n)], full.at[pl.ds(0, n)], ss, rs, partner)

    def start_own(ref, full, s, r, pr, to="xyp"):
        for n in range(2):
            for t in to:
                h = 1 - n if t == "y" else n
                sem, dev = {"x": (r.at[n], nx), "y": (r.at[n], ny), "p": (pr.at[0], partner)}[t]
                remote(ref.at[pl.ds(h * H, H)], full.at[rows(me, h)], s.at[0], sem, dev).start()

    def send_on(full, s, r, g, n, dev):
        q = rows(owner(g), half(g), n)
        remote(full.at[q], full.at[q], s.at[0], r, dev).start()

    def relay(full, s, r, pr, p, onward):
        of_rows(full, 2 * H, s.at[0], r.at[p - 1]).wait_recv()
        if onward:
            send_on(full, s, r.at[2], 2, H, ny)
            send_on(full, s, r.at[2], 3, H, nx)
        for g in (2 * p, 2 * p + 1):
            send_on(full, s, pr.at[p], g, H, partner)

    def from_partner(full, s, pr, p):
        of_rows(full, 2 * H, s.at[0], pr.at[p]).wait_recv()

    def load(ref, full, g):
        o, h, slot = owner(g), half(g), g % 2
        pltpu.make_async_copy(full.at[rows(o + other, h)], tok.at[slot, pl.ds(0, H)], t_sem.at[slot]).start()

        @pl.when(g < 2)
        def _():
            src = ref.at[pl.ds(pl.multiple_of(h * H, H), H)]
            pltpu.make_async_copy(src, tok.at[slot, pl.ds(H, H)], t_sem.at[slot]).start()

        @pl.when(g >= 2)
        def _():
            pltpu.make_async_copy(full.at[rows(o, h)], tok.at[slot, pl.ds(H, H)], t_sem.at[slot]).start()

    def loaded(slot):
        pltpu.make_async_copy(dy_all.at[pl.ds(0, B)], tok.at[slot], t_sem.at[slot]).wait()

    def load_gates(g):
        o, h = owner(g), half(g)
        for i, src in enumerate((gate_ref, up_ref)):
            pltpu.make_async_copy(src.at[rows(o + other, h)], guv.at[i, pl.ds(0, H)], g_sem.at[0]).start()
            pltpu.make_async_copy(src.at[rows(o, h)], guv.at[i, pl.ds(H, H)], g_sem.at[0]).start()

    def start_dy(to):
        start_own(dy_ref, dy_all, dy_s, dy_r, dyp_r, to)

    @pl.when(place != 1)
    def _():
        start_dy("xy")

    for i, first in ((1, "x"), (0, "y")):
        @pl.when(jnp.logical_and(place == 1, ix == i))
        def _():
            start_dy(first)

    @pl.when(core == 1)
    def _():
        pl.semaphore_wait(go_core, 1)

    start_dy("p")

    @pl.when(place == 1)
    def _():
        pl.semaphore_wait(go_chip, 1)

    for i, then in ((1, "y"), (0, "x")):
        @pl.when(jnp.logical_and(place == 1, ix == i))
        def _():
            start_dy(then)

    pltpu.make_async_copy(wd_ref, wd, w_sem.at[0]).start()
    load_gates(0)
    pltpu.make_async_copy(wg_ref, wgu.at[:, pl.ds(0, F)], w_sem.at[1]).start()
    pltpu.make_async_copy(wu_ref, wgu.at[:, pl.ds(F, F)], w_sem.at[1]).start()
    from_partner(dy_all, dy_s, dyp_r, 0)
    load(dy_ref, dy_all, 0)
    acc[...] = jnp.zeros_like(acc)
    pltpu.make_async_copy(wd_ref, wd, w_sem.at[0]).wait()
    pltpu.make_async_copy(wgu, wgu, w_sem.at[1]).wait()

    def send_p(g):
        return remote(p_out.at[g % 2], p_in.at[g % 2], p_s.at[g % 2], p_r.at[g % 2], partner)

    def send_r(stage, kind, k, dev):
        return remote(rs_out.at[stage], rs_in.at[kind, k], r_s.at[kind], r_r.at[kind], dev)

    def both_r(kind):
        return remote(rs_in.at[kind], rs_in.at[kind], r_s.at[kind], r_r.at[kind], nx)

    def dx_tile(g, r0, j):
        a = dgu[pl.ds(pl.multiple_of(g * B + r0, H), H), :]
        w = wgu[pl.ds(pl.multiple_of(j * 512, 512), 512), :]
        return lax.dot_general(a, w, NT, preferred_element_type=F32)

    def first_pass(g, carry):
        slot = g % 2
        loaded(slot)
        pltpu.make_async_copy(guv, guv, g_sem.at[0]).wait()

        @pl.when(slot == 0)
        def _():
            load(dy_ref, dy_all, g + 1)

        for n0, n in ((0, 256), (256, 256), (512, 128)):
            dh[:, n0:n0 + n] = lax.dot_general(tok[slot], wd[n0:n0 + n, :], NT, preferred_element_type=F32)

        def gates(i, carry):
            r = pl.ds(pl.multiple_of(i * 32, 32), 32)
            a, u, d = guv[0, r, :].astype(F32), guv[1, r, :].astype(F32), dh[r, :]
            a2 = a * a
            t = jnp.tanh(a * (C0 + C1 * a2))
            cdf = 0.5 + 0.5 * t
            gelu = a * cdf
            slope = cdf + (0.5 * a) * ((1.0 - t * t) * (C0 + (3.0 * C1) * a2))
            hid[r, :] = (gelu * u).astype(BF16)
            q = pl.ds(pl.multiple_of(g * B + i * 32, 32), 32)
            dgu[q, 0:F] = (d * u * slope).astype(BF16)
            dgu[q, F:2 * F] = (d * gelu).astype(BF16)
            return carry

        lax.fori_loop(0, B // 32, gates, 0)

        @pl.when(g < 7)
        def _():
            load_gates(g + 1)

        @pl.when(g >= 2)
        def _():
            send_p(g - 2).wait_send()

        def p_rows(j, carry):
            p_out[slot, :, pl.ds(pl.multiple_of(j * 512, 512), 512)] = dx_tile(g, 0, j).astype(BF16)
            return carry

        lax.fori_loop(0, 4, p_rows, 0)
        send_p(g).start()

        def down(j, carry):
            s = pl.ds(pl.multiple_of(j * 512, 512), 512)
            r, c = pl.ds(pl.multiple_of((j // 2) * F, F), F), pl.ds(pl.multiple_of((j % 2) * 512, 512), 512)
            acc[r, c] += lax.dot_general(hid[...], tok[slot, :, s], TN, preferred_element_type=F32)
            return carry

        lax.fori_loop(0, 4, down, 0)

        for p in (1, 2, 3):
            @pl.when(g == 2 * p - 1)
            def _():
                relay(dy_all, dy_s, dy_r, dyp_r, p, p == 1)
                if p == 1:
                    start_own(x_ref, x_all, x_s, x_r, xp_r)
                from_partner(dy_all, dy_s, dyp_r, p)
                load(dy_ref, dy_all, g + 1)

        @pl.when(g == 7)
        def _():
            from_partner(x_all, x_s, xp_r, 0)
            load(x_ref, x_all, 0)

        send_p(g).wait_recv()

        def m_rows(j, carry):
            s = pl.ds(pl.multiple_of(j * 512, 512), 512)
            total = dx_tile(g, H, j) + p_in[slot, :, s].astype(F32)

            @pl.when(g // 2 % 2 == 0)
            def _():
                sums[g // 2 + slot, :, s] = total

            @pl.when(g // 2 % 2 == 1)
            def _():
                rs_out[jnp.where(g >= 6, g - 4, slot), :, s] = total.astype(BF16)

            return carry

        lax.fori_loop(0, 4, m_rows, 0)
        return carry

    lax.fori_loop(0, 8, first_pass, 0)

    relay(x_all, x_s, x_r, xp_r, 1, True)

    @pl.when(core == 0)
    def _():
        for stage, kind, k, dev in RS:
            send_r(stage, kind, k, (nx, ny)[dev]).start()

    for j in range(4):
        dwd_ref[:, j * 512:j * 512 + 512] = acc[j // 2 * F:j // 2 * F + F, j % 2 * 512:j % 2 * 512 + 512].astype(BF16)
    acc[...] = jnp.zeros_like(acc)

    def second_pass(g, carry):
        slot = g % 2
        loaded(slot)

        @pl.when(slot == 0)
        def _():
            load(x_ref, x_all, g + 1)

        @pl.when(g == 1)
        def _():
            from_partner(x_all, x_s, xp_r, 1)
            load(x_ref, x_all, 2)

        @pl.when(g == 3)
        def _():
            relay(x_all, x_s, x_r, xp_r, 2, False)
            from_partner(x_all, x_s, xp_r, 2)
            load(x_ref, x_all, 4)

        def weight(j, carry):
            s = pl.ds(pl.multiple_of(j * 512, 512), 512)
            d = dgu[pl.ds(pl.multiple_of(g * B, B), B), :]
            acc[s, :] += lax.dot_general(tok[slot, :, s], d, TN, preferred_element_type=F32)
            return carry

        lax.fori_loop(0, 4, weight, 0)

        @pl.when(g == 5)
        def _():
            relay(x_all, x_s, x_r, xp_r, 3, False)
            from_partner(x_all, x_s, xp_r, 3)
            load(x_ref, x_all, 6)

        return carry

    lax.fori_loop(0, 8, second_pass, 0)

    def weight_out(i, carry):
        r = pl.ds(pl.multiple_of(i * 32, 32), 32)
        dwg_ref[r, :] = acc[r, 0:F].astype(BF16)
        dwu_ref[r, :] = acc[r, F:2 * F].astype(BF16)
        return carry

    lax.fori_loop(0, D // 32, weight_out, 0)

    for g in (6, 7):
        send_p(g).wait_send()
    of_rows(dy_all, 14 * H, dy_s.at[0], dy_r.at[0]).wait_send()
    of_rows(x_all, 14 * H, x_s.at[0], x_r.at[0]).wait_send()

    @pl.when(core == 0)
    def _():
        for kind in range(2):
            both_r(kind).wait_send()
            both_r(kind).wait_recv()


def write_dw(dwg, dwu, dwd, dwg_ref, dwu_ref, dwd_ref, done, sem):
    copies = [
        pltpu.make_async_copy(src, dst, sem.at[i])
        for i, (src, dst) in enumerate(((dwd, dwd_ref), (dwg, dwg_ref), (dwu, dwu_ref)))
    ]
    for c in copies:
        c.start()
    done[...] = jnp.zeros_like(done)
    for c in copies:
        c.wait()


def exchange(sums, rs_out, rs_in, done, got, diag, stage, s_sem, r_sem, t_sem):
    del done
    me = lax.axis_index("tp")
    core, iy, ix = me % 2, (me // 2) % 2, me // 4
    near = (me + 4 - 8 * ix, me + 2 - 4 * iy)

    barrier = pltpu.get_barrier_semaphore()
    for d in near:
        pl.semaphore_signal(barrier, inc=1, device_id={"tp": d}, device_id_type=pl.DeviceIdType.MESH)
    pl.semaphore_wait(barrier, 2)

    def remote(src, dst, i, dev):
        return pltpu.make_async_remote_copy(
            src_ref=src, dst_ref=dst, send_sem=s_sem.at[i], recv_sem=r_sem.at[i],
            device_id={"tp": dev}, device_id_type=pl.DeviceIdType.MESH,
        )

    firsts, diags = got.at[pl.ds(0, 2)], remote(diag, diag, 1, near[0])
    local = [
        pltpu.make_async_copy(rs_in.at[1], diag, t_sem.at[1]),
        pltpu.make_async_copy(rs_in.at[0], firsts, t_sem.at[0]),
    ]

    @pl.when(core == 1)
    def _():
        for st, kind, k, dev in RS:
            remote(rs_out.at[st], (firsts, diag)[kind].at[k], kind, near[dev]).start()
        diags.wait_recv()

    @pl.when(core == 0)
    def _():
        for c in local:
            c.start()
        local[0].wait()

    for k in range(2):
        def add(i, carry):
            r = pl.ds(pl.multiple_of(i * 32, 32), 32)
            stage[k, r, :] = (sums[2 + k, r, :] + diag[k, r, :].astype(F32)).astype(BF16)
            return carry

        lax.fori_loop(0, H // 32, add, 0)
        remote(stage.at[k], got.at[2 + k], 2, near[k]).start()

    @pl.when(core == 1)
    def _():
        diags.wait_send()
        remote(firsts, firsts, 0, near[0]).wait()

    @pl.when(core == 0)
    def _():
        local[1].wait()

    remote(stage, got.at[pl.ds(2, 2)], 2, near[0]).wait()


def write_dx(sums, got, dx_ref, dx, sem):
    copies = []
    for q in range(B // LAST):
        h, i = q * LAST // H, q * LAST % H

        def add(n, carry):
            r = pl.ds(pl.multiple_of(q * LAST + n * 32, 32), 32)
            p = pl.ds(pl.multiple_of(i + n * 32, 32), 32)
            dx[r, :] = (sums[h, p, :] + got[h, p, :].astype(F32) + got[3 - h, p, :].astype(F32)).astype(BF16)
            return carry

        lax.fori_loop(0, LAST // 32, add, 0)
        r = pl.ds(q * LAST, LAST)
        copies.append(pltpu.make_async_copy(dx.at[r], dx_ref.at[r], sem.at[q]))
        copies[-1].start()
    for c in copies:
        c.wait()


def solution(mesh):
    def local(*args):
        any_ = pl.BlockSpec(memory_space=pl.ANY)
        dma = pltpu.SemaphoreType.DMA
        vmem = pl.BlockSpec(memory_space=pltpu.VMEM)
        grads = [(D, F), (D, F), (F, D)]
        def held(a):
            return pltpu.with_memory_space_constraint(a, pltpu.VMEM)

        hbm = [jax.ShapeDtypeStruct(s, BF16) for s in ((8 * B, D), (8 * B, D), (2, 2, H, D))]
        sums, rs_out, *dws, _, _, rs_in = pl.pallas_call(
            kernel,
            out_shape=[pltpu.VMEM((4, H, D), F32), pltpu.VMEM((4, H, D), BF16)]
            + [pltpu.VMEM(s, BF16) for s in grads]
            + hbm,
            in_specs=[any_] * 7,
            out_specs=[vmem] * 5 + [any_] * 3,
            scratch_shapes=[
                pltpu.VMEM((F, D), BF16),
                pltpu.VMEM((D, 2 * F), BF16),
                pltpu.VMEM((8 * B, 2 * F), BF16),
                pltpu.VMEM((D, 2 * F), F32),
                pltpu.VMEM((2, B, D), BF16),
                pltpu.VMEM((2, B, F), BF16),
                pltpu.VMEM((B, F), F32),
                pltpu.VMEM((B, F), BF16),
                pltpu.VMEM((2, H, D), BF16),
                pltpu.VMEM((2, H, D), BF16),
            ]
            + [dma((n,)) for n in (1, 3, 4, 1, 3, 4, 2, 2, 2, 2, 2, 2, 1)]
            + [pltpu.SemaphoreType.REGULAR] * 2,
            compiler_params=pltpu.CompilerParams(collective_id=0, has_side_effects=True, vmem_limit_bytes=42 * 2**20),
            name="backward",
        )(*args)
        *dws, done = pl.pallas_call(
            write_dw,
            out_shape=[jax.ShapeDtypeStruct(s, BF16) for s in grads] + [jax.ShapeDtypeStruct((8, 128), F32)],
            in_specs=[vmem] * 3,
            out_specs=[any_] * 3 + [vmem],
            scratch_shapes=[dma((3,))],
            compiler_params=pltpu.CompilerParams(vmem_limit_bytes=16 * 2**20),
            name="write_dw",
        )(*map(held, dws))
        got = pl.pallas_call(
            exchange,
            out_shape=pltpu.VMEM((4, H, D), BF16),
            in_specs=[vmem, vmem, pl.BlockSpec(memory_space=pltpu.HBM), vmem],
            out_specs=vmem,
            scratch_shapes=[pltpu.VMEM((2, H, D), BF16)] * 2 + [dma((3,)), dma((3,)), dma((2,))],
            compiler_params=pltpu.CompilerParams(collective_id=1, has_side_effects=True, vmem_limit_bytes=24 * 2**20),
            name="exchange",
        )(held(sums), held(rs_out), pltpu.with_memory_space_constraint(rs_in, pltpu.HBM), held(done))
        dx = pl.pallas_call(
            write_dx,
            out_shape=jax.ShapeDtypeStruct((B, D), BF16),
            in_specs=[vmem] * 2,
            out_specs=any_,
            scratch_shapes=[pltpu.VMEM((B, D), BF16), dma((B // LAST,))],
            compiler_params=pltpu.CompilerParams(vmem_limit_bytes=16 * 2**20),
            name="write_dx",
        )(held(sums), held(got))
        return dx, *dws

    rows, cols = P(("dp", "tp"), None), P("dp", "tp")
    return jax.shard_map(
        local,
        mesh=mesh,
        in_specs=(rows, rows, cols, cols, P(None, "tp"), P(None, "tp"), P("tp", None)),
        out_specs=(rows, cols, cols, rows),
        check_vma=False,
    )
```

```python
import functools

import jax
import jax.numpy as jnp
from jax import lax
from jax.experimental import pallas as pl
from jax.experimental.pallas import tpu as pltpu
from jax.sharding import PartitionSpec as P

D = 2048
F = 640
B = 512
H = 256
LAST = 32
RS = ((2, 1, 1, 0), (3, 1, 0, 1), (0, 0, 0, 0), (1, 0, 1, 1))
F32 = jnp.float32
BF16 = jnp.bfloat16
NT = (((1,), (1,)), ((), ()))
TN = (((0,), (0,)), ((), ()))
C0 = 0.7978845608028654
C1 = 0.7978845608028654 * 0.044715


def kernel(
    x_ref, dy_ref, gate_ref, up_ref, wg_ref, wu_ref, wd_ref,
    sums, rs_out, dwg_ref, dwu_ref, dwd_ref, dy_all, x_all, rs_in,
    wd, wgu, dgu, acc, tok, guv, dh, hid, p_in, p_out,
    dy_s, dy_r, dyp_r, x_s, x_r, xp_r, p_s, p_r, r_s, r_r, w_sem, t_sem, g_sem, go_chip, go_core,
):
    me = lax.axis_index("tp")
    core, iy, ix = me % 2, (me // 2) % 2, me // 4
    other = 1 - 2 * core
    partner = me + other
    ny = me + 2 - 4 * iy
    nx = me + 4 - 8 * ix
    nd = ny + 4 - 8 * ix

    place = ix + iy
    barrier = pltpu.get_barrier_semaphore()

    def signal(sem, devs):
        for d in devs:
            pl.semaphore_signal(sem, inc=1, device_id={"tp": d}, device_id_type=pl.DeviceIdType.MESH)

    @pl.when(place < 2)
    def _():
        signal(barrier, (nx, ny))

    @pl.when(core == 1)
    def _():
        signal(barrier, (partner,))

    pl.semaphore_wait(barrier, jnp.where(place == 1, 1, 2) + 1 - core)

    @pl.when(core == 0)
    def _():
        signal(go_core, (partner,))

    @pl.when(place == 2)
    def _():
        signal(go_chip, (nx, ny))

    def owner(g):
        return jnp.where(g < 2, me, jnp.where(g >= 6, nd, jnp.where(g % 2 == 0, nx, ny)))

    def half(g):
        return jnp.where(g == 4, 1, jnp.where(g == 5, 0, g % 2))

    def rows(dev, h, n=H):
        return pl.ds(pl.multiple_of(dev * B + h * H, H), n)

    def remote(src, dst, ss, rs, dev):
        return pltpu.make_async_remote_copy(
            src_ref=src, dst_ref=dst, send_sem=ss, recv_sem=rs, device_id={"tp": dev}, device_id_type=pl.DeviceIdType.MESH
        )

    def of_rows(full, n, ss, rs):
        return remote(full.at[pl.ds(0, n)], full.at[pl.ds(0, n)], ss, rs, partner)

    def start_own(ref, full, s, r, pr, to="xyp"):
        for n in range(2):
            for t in to:
                h = 1 - n if t == "y" else n
                sem, dev = {"x": (r.at[n], nx), "y": (r.at[n], ny), "p": (pr.at[0], partner)}[t]
                remote(ref.at[pl.ds(h * H, H)], full.at[rows(me, h)], s.at[0], sem, dev).start()

    def send_on(full, s, r, g, n, dev):
        q = rows(owner(g), half(g), n)
        remote(full.at[q], full.at[q], s.at[0], r, dev).start()

    def relay(full, s, r, pr, p, onward):
        of_rows(full, 2 * H, s.at[0], r.at[p - 1]).wait_recv()
        if onward:
            send_on(full, s, r.at[2], 2, H, ny)
            send_on(full, s, r.at[2], 3, H, nx)
        for g in (2 * p, 2 * p + 1):
            send_on(full, s, pr.at[p], g, H, partner)

    def from_partner(full, s, pr, p):
        of_rows(full, 2 * H, s.at[0], pr.at[p]).wait_recv()

    def load(ref, full, g):
        o, h, slot = owner(g), half(g), g % 2
        pltpu.make_async_copy(full.at[rows(o + other, h)], tok.at[slot, pl.ds(0, H)], t_sem.at[slot]).start()

        @pl.when(g < 2)
        def _():
            src = ref.at[pl.ds(pl.multiple_of(h * H, H), H)]
            pltpu.make_async_copy(src, tok.at[slot, pl.ds(H, H)], t_sem.at[slot]).start()

        @pl.when(g >= 2)
        def _():
            pltpu.make_async_copy(full.at[rows(o, h)], tok.at[slot, pl.ds(H, H)], t_sem.at[slot]).start()

    def loaded(slot):
        pltpu.make_async_copy(dy_all.at[pl.ds(0, B)], tok.at[slot], t_sem.at[slot]).wait()

    def load_gates(g):
        o, h = owner(g), half(g)
        for i, src in enumerate((gate_ref, up_ref)):
            pltpu.make_async_copy(src.at[rows(o + other, h)], guv.at[i, pl.ds(0, H)], g_sem.at[0]).start()
            pltpu.make_async_copy(src.at[rows(o, h)], guv.at[i, pl.ds(H, H)], g_sem.at[0]).start()

    def start_dy(to):
        start_own(dy_ref, dy_all, dy_s, dy_r, dyp_r, to)

    @pl.when(place != 1)
    def _():
        start_dy("xy")

    for i, first in ((1, "x"), (0, "y")):
        @pl.when(jnp.logical_and(place == 1, ix == i))
        def _():
            start_dy(first)

    @pl.when(core == 1)
    def _():
        pl.semaphore_wait(go_core, 1)

    start_dy("p")

    @pl.when(place == 1)
    def _():
        pl.semaphore_wait(go_chip, 1)

    for i, then in ((1, "y"), (0, "x")):
        @pl.when(jnp.logical_and(place == 1, ix == i))
        def _():
            start_dy(then)

    pltpu.make_async_copy(wd_ref, wd, w_sem.at[0]).start()
    load_gates(0)
    pltpu.make_async_copy(wg_ref, wgu.at[:, pl.ds(0, F)], w_sem.at[1]).start()
    pltpu.make_async_copy(wu_ref, wgu.at[:, pl.ds(F, F)], w_sem.at[1]).start()
    from_partner(dy_all, dy_s, dyp_r, 0)
    load(dy_ref, dy_all, 0)
    acc[...] = jnp.zeros_like(acc)
    pltpu.make_async_copy(wd_ref, wd, w_sem.at[0]).wait()
    pltpu.make_async_copy(wgu, wgu, w_sem.at[1]).wait()

    def send_p(g):
        return remote(p_out.at[g % 2], p_in.at[g % 2], p_s.at[g % 2], p_r.at[g % 2], partner)

    def send_r(stage, kind, k, dev):
        return remote(rs_out.at[stage], rs_in.at[kind, k], r_s.at[kind], r_r.at[kind], dev)

    def both_r(kind):
        return remote(rs_in.at[kind], rs_in.at[kind], r_s.at[kind], r_r.at[kind], nx)

    def dx_tile(g, r0, j):
        a = dgu[pl.ds(pl.multiple_of(g * B + r0, H), H), :]
        w = wgu[pl.ds(pl.multiple_of(j * 512, 512), 512), :]
        return lax.dot_general(a, w, NT, preferred_element_type=F32)

    def first_pass(g, carry):
        slot = g % 2
        loaded(slot)
        pltpu.make_async_copy(guv, guv, g_sem.at[0]).wait()

        @pl.when(slot == 0)
        def _():
            load(dy_ref, dy_all, g + 1)

        for n0, n in ((0, 256), (256, 256), (512, 128)):
            dh[:, n0:n0 + n] = lax.dot_general(tok[slot], wd[n0:n0 + n, :], NT, preferred_element_type=F32)

        def gates(i, carry):
            r = pl.ds(pl.multiple_of(i * 32, 32), 32)
            a, u, d = guv[0, r, :].astype(F32), guv[1, r, :].astype(F32), dh[r, :]
            a2 = a * a
            t = jnp.tanh(a * (C0 + C1 * a2))
            cdf = 0.5 + 0.5 * t
            gelu = a * cdf
            slope = cdf + (0.5 * a) * ((1.0 - t * t) * (C0 + (3.0 * C1) * a2))
            hid[r, :] = (gelu * u).astype(BF16)
            q = pl.ds(pl.multiple_of(g * B + i * 32, 32), 32)
            dgu[q, 0:F] = (d * u * slope).astype(BF16)
            dgu[q, F:2 * F] = (d * gelu).astype(BF16)
            return carry

        lax.fori_loop(0, B // 32, gates, 0)

        @pl.when(g < 7)
        def _():
            load_gates(g + 1)

        @pl.when(g >= 2)
        def _():
            send_p(g - 2).wait_send()

        def p_rows(j, carry):
            p_out[slot, :, pl.ds(pl.multiple_of(j * 512, 512), 512)] = dx_tile(g, 0, j).astype(BF16)
            return carry

        lax.fori_loop(0, 4, p_rows, 0)
        send_p(g).start()

        def down(j, carry):
            s = pl.ds(pl.multiple_of(j * 512, 512), 512)
            r, c = pl.ds(pl.multiple_of((j // 2) * F, F), F), pl.ds(pl.multiple_of((j % 2) * 512, 512), 512)
            acc[r, c] += lax.dot_general(hid[...], tok[slot, :, s], TN, preferred_element_type=F32)
            return carry

        lax.fori_loop(0, 4, down, 0)

        for p in (1, 2, 3):
            @pl.when(g == 2 * p - 1)
            def _():
                relay(dy_all, dy_s, dy_r, dyp_r, p, p == 1)
                if p == 1:
                    start_own(x_ref, x_all, x_s, x_r, xp_r)
                from_partner(dy_all, dy_s, dyp_r, p)
                load(dy_ref, dy_all, g + 1)

        @pl.when(g == 7)
        def _():
            from_partner(x_all, x_s, xp_r, 0)
            load(x_ref, x_all, 0)

        send_p(g).wait_recv()

        def m_rows(j, carry):
            s = pl.ds(pl.multiple_of(j * 512, 512), 512)
            total = dx_tile(g, H, j) + p_in[slot, :, s].astype(F32)

            @pl.when(g // 2 % 2 == 0)
            def _():
                sums[g // 2 + slot, :, s] = total

            @pl.when(g // 2 % 2 == 1)
            def _():
                rs_out[jnp.where(g >= 6, g - 4, slot), :, s] = total.astype(BF16)

            return carry

        lax.fori_loop(0, 4, m_rows, 0)
        return carry

    lax.fori_loop(0, 8, first_pass, 0)

    relay(x_all, x_s, x_r, xp_r, 1, True)

    @pl.when(core == 0)
    def _():
        for stage, kind, k, dev in RS:
            send_r(stage, kind, k, (nx, ny)[dev]).start()

    for j in range(4):
        dwd_ref[:, j * 512:j * 512 + 512] = acc[j // 2 * F:j // 2 * F + F, j % 2 * 512:j % 2 * 512 + 512].astype(BF16)
    acc[...] = jnp.zeros_like(acc)

    def second_pass(g, carry):
        slot = g % 2
        loaded(slot)

        @pl.when(slot == 0)
        def _():
            load(x_ref, x_all, g + 1)

        @pl.when(g == 1)
        def _():
            from_partner(x_all, x_s, xp_r, 1)
            load(x_ref, x_all, 2)

        @pl.when(g == 3)
        def _():
            relay(x_all, x_s, x_r, xp_r, 2, False)
            from_partner(x_all, x_s, xp_r, 2)
            load(x_ref, x_all, 4)

        def weight(j, carry):
            s = pl.ds(pl.multiple_of(j * 512, 512), 512)
            d = dgu[pl.ds(pl.multiple_of(g * B, B), B), :]
            acc[s, :] += lax.dot_general(tok[slot, :, s], d, TN, preferred_element_type=F32)
            return carry

        lax.fori_loop(0, 4, weight, 0)

        @pl.when(g == 5)
        def _():
            relay(x_all, x_s, x_r, xp_r, 3, False)
            from_partner(x_all, x_s, xp_r, 3)
            load(x_ref, x_all, 6)

        return carry

    lax.fori_loop(0, 8, second_pass, 0)

    def weight_out(i, carry):
        r = pl.ds(pl.multiple_of(i * 32, 32), 32)
        dwg_ref[r, :] = acc[r, 0:F].astype(BF16)
        dwu_ref[r, :] = acc[r, F:2 * F].astype(BF16)
        return carry

    lax.fori_loop(0, D // 32, weight_out, 0)

    for g in (6, 7):
        send_p(g).wait_send()
    of_rows(dy_all, 14 * H, dy_s.at[0], dy_r.at[0]).wait_send()
    of_rows(x_all, 14 * H, x_s.at[0], x_r.at[0]).wait_send()

    @pl.when(core == 0)
    def _():
        for kind in range(2):
            both_r(kind).wait_send()
            both_r(kind).wait_recv()


def write_dw(dwg, dwu, dwd, dwg_ref, dwu_ref, dwd_ref, done, sem):
    copies = [
        pltpu.make_async_copy(src, dst, sem.at[i])
        for i, (src, dst) in enumerate(((dwd, dwd_ref), (dwg, dwg_ref), (dwu, dwu_ref)))
    ]
    for c in copies:
        c.start()
    done[...] = jnp.zeros_like(done)
    for c in copies:
        c.wait()


def exchange(sums, rs_out, rs_in, done, got, diag, stage, s_sem, r_sem):
    del done
    me = lax.axis_index("tp")
    core, iy, ix = me % 2, (me // 2) % 2, me // 4
    near = (me + 4 - 8 * ix, me + 2 - 4 * iy)

    barrier = pltpu.get_barrier_semaphore()
    for d in near:
        pl.semaphore_signal(barrier, inc=1, device_id={"tp": d}, device_id_type=pl.DeviceIdType.MESH)
    pl.semaphore_wait(barrier, 2)

    def remote(src, dst, i, dev):
        return pltpu.make_async_remote_copy(
            src_ref=src, dst_ref=dst, send_sem=s_sem.at[0], recv_sem=r_sem.at[i],
            device_id={"tp": dev}, device_id_type=pl.DeviceIdType.MESH,
        )

    firsts, diags = got.at[pl.ds(0, 2)], remote(diag, diag, 1, near[0])
    local = [
        pltpu.make_async_copy(rs_in.at[1], diag, r_sem.at[1]),
        pltpu.make_async_copy(rs_in.at[0], firsts, r_sem.at[0]),
    ]

    @pl.when(core == 1)
    def _():
        for st, kind, k, dev in RS:
            remote(rs_out.at[st], (firsts, diag)[kind].at[k], kind, near[dev]).start()
        diags.wait_recv()

    @pl.when(core == 0)
    def _():
        for c in local:
            c.start()
        local[0].wait()

    for k in range(2):
        def add(i, carry):
            r = pl.ds(pl.multiple_of(i * 32, 32), 32)
            stage[k, r, :] = (sums[2 + k, r, :] + diag[k, r, :].astype(F32)).astype(BF16)
            return carry

        lax.fori_loop(0, H // 32, add, 0)
        remote(stage.at[k], got.at[2 + k], 0, near[k]).start()

    for c, sent in ((0, stage), (1, got)):
        @pl.when(core == c)
        def _():
            remote(sent, sent, 0, near[0]).wait_send()
            if c == 1:
                diags.wait_send()

    remote(got, got, 0, near[0]).wait_recv()


def write_dx(sums, got, dx_ref, dx, sem):
    for q in range(B // LAST):
        h, i = q * LAST // H, q * LAST % H
        r, p = pl.ds(q * LAST, LAST), pl.ds(i, LAST)
        dx[r, :] = (sums[h, p, :] + got[h, p, :].astype(F32) + got[3 - h, p, :].astype(F32)).astype(BF16)
        pltpu.make_async_copy(dx.at[r], dx_ref.at[r], sem).start()
    pltpu.make_async_copy(dx, dx_ref, sem).wait()


def solution(mesh):
    def local(*args):
        any_ = pl.BlockSpec(memory_space=pl.ANY)
        dma = pltpu.SemaphoreType.DMA
        vmem = pl.BlockSpec(memory_space=pltpu.VMEM)
        grads = [(D, F), (D, F), (F, D)]
        def held(a):
            return pltpu.with_memory_space_constraint(a, pltpu.VMEM)

        hbm = [jax.ShapeDtypeStruct(s, BF16) for s in ((8 * B, D), (8 * B, D), (2, 2, H, D))]
        sums, rs_out, *dws, _, _, rs_in = pl.pallas_call(
            kernel,
            out_shape=[pltpu.VMEM((4, H, D), F32), pltpu.VMEM((4, H, D), BF16)]
            + [pltpu.VMEM(s, BF16) for s in grads]
            + hbm,
            in_specs=[any_] * 7,
            out_specs=[vmem] * 5 + [any_] * 3,
            scratch_shapes=[
                pltpu.VMEM((F, D), BF16),
                pltpu.VMEM((D, 2 * F), BF16),
                pltpu.VMEM((8 * B, 2 * F), BF16),
                pltpu.VMEM((D, 2 * F), F32),
                pltpu.VMEM((2, B, D), BF16),
                pltpu.VMEM((2, B, F), BF16),
                pltpu.VMEM((B, F), F32),
                pltpu.VMEM((B, F), BF16),
                pltpu.VMEM((2, H, D), BF16),
                pltpu.VMEM((2, H, D), BF16),
            ]
            + [dma((n,)) for n in (1, 3, 4, 1, 3, 4, 2, 2, 2, 2, 2, 2, 1)]
            + [pltpu.SemaphoreType.REGULAR] * 2,
            compiler_params=pltpu.CompilerParams(collective_id=0, has_side_effects=True, vmem_limit_bytes=42 * 2**20),
            name="backward",
        )(*args)
        *dws, done = pl.pallas_call(
            write_dw,
            out_shape=[jax.ShapeDtypeStruct(s, BF16) for s in grads] + [jax.ShapeDtypeStruct((8, 128), F32)],
            in_specs=[vmem] * 3,
            out_specs=[any_] * 3 + [vmem],
            scratch_shapes=[dma((3,))],
            compiler_params=pltpu.CompilerParams(vmem_limit_bytes=16 * 2**20),
            name="write_dw",
        )(*map(held, dws))
        got = pl.pallas_call(
            exchange,
            out_shape=pltpu.VMEM((4, H, D), BF16),
            in_specs=[vmem, vmem, pl.BlockSpec(memory_space=pltpu.HBM), vmem],
            out_specs=vmem,
            scratch_shapes=[pltpu.VMEM((2, H, D), BF16)] * 2 + [dma((1,)), dma((2,))],
            compiler_params=pltpu.CompilerParams(collective_id=1, has_side_effects=True, vmem_limit_bytes=24 * 2**20),
            name="exchange",
        )(held(sums), held(rs_out), pltpu.with_memory_space_constraint(rs_in, pltpu.HBM), held(done))
        dx = pl.pallas_call(
            write_dx,
            out_shape=jax.ShapeDtypeStruct((B, D), BF16),
            in_specs=[vmem] * 2,
            out_specs=any_,
            scratch_shapes=[pltpu.VMEM((B, D), BF16), dma],
            compiler_params=pltpu.CompilerParams(vmem_limit_bytes=16 * 2**20),
            name="write_dx",
        )(held(sums), held(got))
        return dx, *dws

    rows, cols = P(("dp", "tp"), None), P("dp", "tp")
    return jax.shard_map(
        local,
        mesh=mesh,
        in_specs=(rows, rows, cols, cols, P(None, "tp"), P(None, "tp"), P("tp", None)),
        out_specs=(rows, cols, cols, rows),
        check_vma=False,
    )
```

```python
import functools

import jax
import jax.numpy as jnp
from jax import lax
from jax.experimental import pallas as pl
from jax.experimental.pallas import tpu as pltpu
from jax.sharding import PartitionSpec as P

D = 2048
F = 640
B = 512
H = 256
LAST = 16
RS = ((2, 1, 1, 0), (3, 1, 0, 1), (0, 0, 0, 0), (1, 0, 1, 1))
F32 = jnp.float32
BF16 = jnp.bfloat16
NT = (((1,), (1,)), ((), ()))
TN = (((0,), (0,)), ((), ()))
C0 = 0.7978845608028654
C1 = 0.7978845608028654 * 0.044715


def kernel(
    x_ref, dy_ref, gate_ref, up_ref, wg_ref, wu_ref, wd_ref,
    sums, rs_out, dwg_ref, dwu_ref, dwd_ref, dy_all, x_all, rs_in,
    wd, wgu, dgu, acc, tok, guv, dh, hid, p_in, p_out,
    dy_s, dy_r, dyp_r, x_s, x_r, xp_r, p_s, p_r, r_s, r_r, w_sem, t_sem, g_sem, go_chip, go_core,
):
    me = lax.axis_index("tp")
    core, iy, ix = me % 2, (me // 2) % 2, me // 4
    other = 1 - 2 * core
    partner = me + other
    ny = me + 2 - 4 * iy
    nx = me + 4 - 8 * ix
    nd = ny + 4 - 8 * ix

    place = ix + iy
    barrier = pltpu.get_barrier_semaphore()

    def signal(sem, devs):
        for d in devs:
            pl.semaphore_signal(sem, inc=1, device_id={"tp": d}, device_id_type=pl.DeviceIdType.MESH)

    @pl.when(place < 2)
    def _():
        signal(barrier, (nx, ny))

    @pl.when(core == 1)
    def _():
        signal(barrier, (partner,))

    pl.semaphore_wait(barrier, jnp.where(place == 1, 1, 2) + 1 - core)

    @pl.when(core == 0)
    def _():
        signal(go_core, (partner,))

    @pl.when(place == 2)
    def _():
        signal(go_chip, (nx, ny))

    def owner(g):
        return jnp.where(g < 2, me, jnp.where(g >= 6, nd, jnp.where(g % 2 == 0, nx, ny)))

    def half(g):
        return jnp.where(g == 4, 1, jnp.where(g == 5, 0, g % 2))

    def rows(dev, h, n=H):
        return pl.ds(pl.multiple_of(dev * B + h * H, H), n)

    def remote(src, dst, ss, rs, dev):
        return pltpu.make_async_remote_copy(
            src_ref=src, dst_ref=dst, send_sem=ss, recv_sem=rs, device_id={"tp": dev}, device_id_type=pl.DeviceIdType.MESH
        )

    def of_rows(full, n, ss, rs):
        return remote(full.at[pl.ds(0, n)], full.at[pl.ds(0, n)], ss, rs, partner)

    def start_own(ref, full, s, r, pr, to="xyp"):
        for n in range(2):
            for t in to:
                h = 1 - n if t == "y" else n
                sem, dev = {"x": (r.at[n], nx), "y": (r.at[n], ny), "p": (pr.at[0], partner)}[t]
                remote(ref.at[pl.ds(h * H, H)], full.at[rows(me, h)], s.at[0], sem, dev).start()

    def send_on(full, s, r, g, n, dev):
        q = rows(owner(g), half(g), n)
        remote(full.at[q], full.at[q], s.at[0], r, dev).start()

    def relay(full, s, r, pr, p, onward):
        of_rows(full, 2 * H, s.at[0], r.at[p - 1]).wait_recv()
        if onward:
            send_on(full, s, r.at[2], 2, H, ny)
            send_on(full, s, r.at[2], 3, H, nx)
        for g in (2 * p, 2 * p + 1):
            send_on(full, s, pr.at[p], g, H, partner)

    def from_partner(full, s, pr, p):
        of_rows(full, 2 * H, s.at[0], pr.at[p]).wait_recv()

    def load(ref, full, g):
        o, h, slot = owner(g), half(g), g % 2
        pltpu.make_async_copy(full.at[rows(o + other, h)], tok.at[slot, pl.ds(0, H)], t_sem.at[slot]).start()

        @pl.when(g < 2)
        def _():
            src = ref.at[pl.ds(pl.multiple_of(h * H, H), H)]
            pltpu.make_async_copy(src, tok.at[slot, pl.ds(H, H)], t_sem.at[slot]).start()

        @pl.when(g >= 2)
        def _():
            pltpu.make_async_copy(full.at[rows(o, h)], tok.at[slot, pl.ds(H, H)], t_sem.at[slot]).start()

    def loaded(slot):
        pltpu.make_async_copy(dy_all.at[pl.ds(0, B)], tok.at[slot], t_sem.at[slot]).wait()

    def load_gates(g):
        o, h = owner(g), half(g)
        for i, src in enumerate((gate_ref, up_ref)):
            pltpu.make_async_copy(src.at[rows(o + other, h)], guv.at[i, pl.ds(0, H)], g_sem.at[0]).start()
            pltpu.make_async_copy(src.at[rows(o, h)], guv.at[i, pl.ds(H, H)], g_sem.at[0]).start()

    def start_dy(to):
        start_own(dy_ref, dy_all, dy_s, dy_r, dyp_r, to)

    @pl.when(place != 1)
    def _():
        start_dy("xy")

    for i, first in ((1, "x"), (0, "y")):
        @pl.when(jnp.logical_and(place == 1, ix == i))
        def _():
            start_dy(first)

    @pl.when(core == 1)
    def _():
        pl.semaphore_wait(go_core, 1)

    start_dy("p")

    @pl.when(place == 1)
    def _():
        pl.semaphore_wait(go_chip, 1)

    for i, then in ((1, "y"), (0, "x")):
        @pl.when(jnp.logical_and(place == 1, ix == i))
        def _():
            start_dy(then)

    pltpu.make_async_copy(wd_ref, wd, w_sem.at[0]).start()
    load_gates(0)
    pltpu.make_async_copy(wg_ref, wgu.at[:, pl.ds(0, F)], w_sem.at[1]).start()
    pltpu.make_async_copy(wu_ref, wgu.at[:, pl.ds(F, F)], w_sem.at[1]).start()
    from_partner(dy_all, dy_s, dyp_r, 0)
    load(dy_ref, dy_all, 0)
    acc[...] = jnp.zeros_like(acc)
    pltpu.make_async_copy(wd_ref, wd, w_sem.at[0]).wait()
    pltpu.make_async_copy(wgu, wgu, w_sem.at[1]).wait()

    def send_p(g):
        return remote(p_out.at[g % 2], p_in.at[g % 2], p_s.at[g % 2], p_r.at[g % 2], partner)

    def send_r(stage, kind, k, dev):
        return remote(rs_out.at[stage], rs_in.at[kind, k], r_s.at[kind], r_r.at[kind], dev)

    def both_r(kind):
        return remote(rs_in.at[kind], rs_in.at[kind], r_s.at[kind], r_r.at[kind], nx)

    def dx_tile(g, r0, j):
        a = dgu[pl.ds(pl.multiple_of(g * B + r0, H), H), :]
        w = wgu[pl.ds(pl.multiple_of(j * 512, 512), 512), :]
        return lax.dot_general(a, w, NT, preferred_element_type=F32)

    def first_pass(g, carry):
        slot = g % 2
        loaded(slot)
        pltpu.make_async_copy(guv, guv, g_sem.at[0]).wait()

        @pl.when(slot == 0)
        def _():
            load(dy_ref, dy_all, g + 1)

        for n0, n in ((0, 256), (256, 256), (512, 128)):
            dh[:, n0:n0 + n] = lax.dot_general(tok[slot], wd[n0:n0 + n, :], NT, preferred_element_type=F32)

        def gates(i, carry):
            r = pl.ds(pl.multiple_of(i * 32, 32), 32)
            a, u, d = guv[0, r, :].astype(F32), guv[1, r, :].astype(F32), dh[r, :]
            a2 = a * a
            t = jnp.tanh(a * (C0 + C1 * a2))
            cdf = 0.5 + 0.5 * t
            gelu = a * cdf
            slope = cdf + (0.5 * a) * ((1.0 - t * t) * (C0 + (3.0 * C1) * a2))
            hid[r, :] = (gelu * u).astype(BF16)
            q = pl.ds(pl.multiple_of(g * B + i * 32, 32), 32)
            dgu[q, 0:F] = (d * u * slope).astype(BF16)
            dgu[q, F:2 * F] = (d * gelu).astype(BF16)
            return carry

        lax.fori_loop(0, B // 32, gates, 0)

        @pl.when(g < 7)
        def _():
            load_gates(g + 1)

        @pl.when(g >= 2)
        def _():
            send_p(g - 2).wait_send()

        def p_rows(j, carry):
            p_out[slot, :, pl.ds(pl.multiple_of(j * 512, 512), 512)] = dx_tile(g, 0, j).astype(BF16)
            return carry

        lax.fori_loop(0, 4, p_rows, 0)
        send_p(g).start()

        def down(j, carry):
            s = pl.ds(pl.multiple_of(j * 512, 512), 512)
            r, c = pl.ds(pl.multiple_of((j // 2) * F, F), F), pl.ds(pl.multiple_of((j % 2) * 512, 512), 512)
            acc[r, c] += lax.dot_general(hid[...], tok[slot, :, s], TN, preferred_element_type=F32)
            return carry

        lax.fori_loop(0, 4, down, 0)

        for p in (1, 2, 3):
            @pl.when(g == 2 * p - 1)
            def _():
                relay(dy_all, dy_s, dy_r, dyp_r, p, p == 1)
                if p == 1:
                    start_own(x_ref, x_all, x_s, x_r, xp_r)
                from_partner(dy_all, dy_s, dyp_r, p)
                load(dy_ref, dy_all, g + 1)

        @pl.when(g == 7)
        def _():
            from_partner(x_all, x_s, xp_r, 0)
            load(x_ref, x_all, 0)

        send_p(g).wait_recv()

        def m_rows(j, carry):
            s = pl.ds(pl.multiple_of(j * 512, 512), 512)
            total = dx_tile(g, H, j) + p_in[slot, :, s].astype(F32)

            @pl.when(g // 2 % 2 == 0)
            def _():
                sums[g // 2 + slot, :, s] = total

            @pl.when(g // 2 % 2 == 1)
            def _():
                rs_out[jnp.where(g >= 6, g - 4, slot), :, s] = total.astype(BF16)

            return carry

        lax.fori_loop(0, 4, m_rows, 0)
        return carry

    lax.fori_loop(0, 8, first_pass, 0)

    relay(x_all, x_s, x_r, xp_r, 1, True)

    @pl.when(core == 0)
    def _():
        for stage, kind, k, dev in RS:
            send_r(stage, kind, k, (nx, ny)[dev]).start()

    for j in range(4):
        dwd_ref[:, j * 512:j * 512 + 512] = acc[j // 2 * F:j // 2 * F + F, j % 2 * 512:j % 2 * 512 + 512].astype(BF16)
    acc[...] = jnp.zeros_like(acc)

    def second_pass(g, carry):
        slot = g % 2
        loaded(slot)

        @pl.when(slot == 0)
        def _():
            load(x_ref, x_all, g + 1)

        @pl.when(g == 1)
        def _():
            from_partner(x_all, x_s, xp_r, 1)
            load(x_ref, x_all, 2)

        @pl.when(g == 3)
        def _():
            relay(x_all, x_s, x_r, xp_r, 2, False)
            from_partner(x_all, x_s, xp_r, 2)
            load(x_ref, x_all, 4)

        def weight(j, carry):
            s = pl.ds(pl.multiple_of(j * 512, 512), 512)
            d = dgu[pl.ds(pl.multiple_of(g * B, B), B), :]
            acc[s, :] += lax.dot_general(tok[slot, :, s], d, TN, preferred_element_type=F32)
            return carry

        lax.fori_loop(0, 4, weight, 0)

        @pl.when(g == 5)
        def _():
            relay(x_all, x_s, x_r, xp_r, 3, False)
            from_partner(x_all, x_s, xp_r, 3)
            load(x_ref, x_all, 6)

        return carry

    lax.fori_loop(0, 8, second_pass, 0)

    def weight_out(i, carry):
        r = pl.ds(pl.multiple_of(i * 32, 32), 32)
        dwg_ref[r, :] = acc[r, 0:F].astype(BF16)
        dwu_ref[r, :] = acc[r, F:2 * F].astype(BF16)
        return carry

    lax.fori_loop(0, D // 32, weight_out, 0)

    for g in (6, 7):
        send_p(g).wait_send()
    of_rows(dy_all, 14 * H, dy_s.at[0], dy_r.at[0]).wait_send()
    of_rows(x_all, 14 * H, x_s.at[0], x_r.at[0]).wait_send()

    @pl.when(core == 0)
    def _():
        for kind in range(2):
            both_r(kind).wait_send()
            both_r(kind).wait_recv()


def write_dw(dwg, dwu, dwd, dwg_ref, dwu_ref, dwd_ref, done, sem):
    copies = [
        pltpu.make_async_copy(src, dst, sem.at[i])
        for i, (src, dst) in enumerate(((dwd, dwd_ref), (dwg, dwg_ref), (dwu, dwu_ref)))
    ]
    for c in copies:
        c.start()
    done[...] = jnp.zeros_like(done)
    for c in copies:
        c.wait()


def exchange(sums, rs_out, rs_in, done, got, diag, stage, s_sem, r_sem):
    del done
    me = lax.axis_index("tp")
    core, iy, ix = me % 2, (me // 2) % 2, me // 4
    near = (me + 4 - 8 * ix, me + 2 - 4 * iy)

    barrier = pltpu.get_barrier_semaphore()
    for d in near:
        pl.semaphore_signal(barrier, inc=1, device_id={"tp": d}, device_id_type=pl.DeviceIdType.MESH)
    pl.semaphore_wait(barrier, 2)

    def remote(src, dst, i, dev):
        return pltpu.make_async_remote_copy(
            src_ref=src, dst_ref=dst, send_sem=s_sem.at[0], recv_sem=r_sem.at[i],
            device_id={"tp": dev}, device_id_type=pl.DeviceIdType.MESH,
        )

    firsts, diags = got.at[pl.ds(0, 2)], remote(diag, diag, 1, near[0])
    local = [
        pltpu.make_async_copy(rs_in.at[1], diag, r_sem.at[1]),
        pltpu.make_async_copy(rs_in.at[0], firsts, r_sem.at[0]),
    ]

    @pl.when(core == 1)
    def _():
        for st, kind, k, dev in RS:
            remote(rs_out.at[st], (firsts, diag)[kind].at[k], kind, near[dev]).start()
        diags.wait_recv()

    @pl.when(core == 0)
    def _():
        for c in local:
            c.start()
        local[0].wait()

    for k in range(2):
        def add(i, carry):
            r = pl.ds(pl.multiple_of(i * 32, 32), 32)
            stage[k, r, :] = (sums[2 + k, r, :] + diag[k, r, :].astype(F32)).astype(BF16)
            return carry

        lax.fori_loop(0, H // 32, add, 0)
        remote(stage.at[k], got.at[2 + k], 0, near[k]).start()

    for c, sent in ((0, stage), (1, got)):
        @pl.when(core == c)
        def _():
            remote(sent, sent, 0, near[0]).wait_send()
            if c == 1:
                diags.wait_send()

    remote(got, got, 0, near[0]).wait_recv()


def write_dx(sums, got, dx_ref, dx, sem):
    for q in range(B // LAST):
        h, i = q * LAST // H, q * LAST % H
        r, p = pl.ds(q * LAST, LAST), pl.ds(i, LAST)
        dx[r, :] = (sums[h, p, :] + got[h, p, :].astype(F32) + got[3 - h, p, :].astype(F32)).astype(BF16)
        pltpu.make_async_copy(dx.at[r], dx_ref.at[r], sem).start()
    pltpu.make_async_copy(dx, dx_ref, sem).wait()


def solution(mesh):
    def local(*args):
        any_ = pl.BlockSpec(memory_space=pl.ANY)
        dma = pltpu.SemaphoreType.DMA
        vmem = pl.BlockSpec(memory_space=pltpu.VMEM)
        grads = [(D, F), (D, F), (F, D)]
        def held(a):
            return pltpu.with_memory_space_constraint(a, pltpu.VMEM)

        hbm = [jax.ShapeDtypeStruct(s, BF16) for s in ((8 * B, D), (8 * B, D), (2, 2, H, D))]
        sums, rs_out, *dws, _, _, rs_in = pl.pallas_call(
            kernel,
            out_shape=[pltpu.VMEM((4, H, D), F32), pltpu.VMEM((4, H, D), BF16)]
            + [pltpu.VMEM(s, BF16) for s in grads]
            + hbm,
            in_specs=[any_] * 7,
            out_specs=[vmem] * 5 + [any_] * 3,
            scratch_shapes=[
                pltpu.VMEM((F, D), BF16),
                pltpu.VMEM((D, 2 * F), BF16),
                pltpu.VMEM((8 * B, 2 * F), BF16),
                pltpu.VMEM((D, 2 * F), F32),
                pltpu.VMEM((2, B, D), BF16),
                pltpu.VMEM((2, B, F), BF16),
                pltpu.VMEM((B, F), F32),
                pltpu.VMEM((B, F), BF16),
                pltpu.VMEM((2, H, D), BF16),
                pltpu.VMEM((2, H, D), BF16),
            ]
            + [dma((n,)) for n in (1, 3, 4, 1, 3, 4, 2, 2, 2, 2, 2, 2, 1)]
            + [pltpu.SemaphoreType.REGULAR] * 2,
            compiler_params=pltpu.CompilerParams(collective_id=0, has_side_effects=True, vmem_limit_bytes=42 * 2**20),
            name="backward",
        )(*args)
        *dws, done = pl.pallas_call(
            write_dw,
            out_shape=[jax.ShapeDtypeStruct(s, BF16) for s in grads] + [jax.ShapeDtypeStruct((8, 128), F32)],
            in_specs=[vmem] * 3,
            out_specs=[any_] * 3 + [vmem],
            scratch_shapes=[dma((3,))],
            compiler_params=pltpu.CompilerParams(vmem_limit_bytes=16 * 2**20),
            name="write_dw",
        )(*map(held, dws))
        got = pl.pallas_call(
            exchange,
            out_shape=pltpu.VMEM((4, H, D), BF16),
            in_specs=[vmem, vmem, pl.BlockSpec(memory_space=pltpu.HBM), vmem],
            out_specs=vmem,
            scratch_shapes=[pltpu.VMEM((2, H, D), BF16)] * 2 + [dma((1,)), dma((2,))],
            compiler_params=pltpu.CompilerParams(collective_id=1, has_side_effects=True, vmem_limit_bytes=24 * 2**20),
            name="exchange",
        )(held(sums), held(rs_out), pltpu.with_memory_space_constraint(rs_in, pltpu.HBM), held(done))
        dx = pl.pallas_call(
            write_dx,
            out_shape=jax.ShapeDtypeStruct((B, D), BF16),
            in_specs=[vmem] * 2,
            out_specs=any_,
            scratch_shapes=[pltpu.VMEM((B, D), BF16), dma],
            compiler_params=pltpu.CompilerParams(vmem_limit_bytes=16 * 2**20),
            name="write_dx",
        )(held(sums), held(got))
        return dx, *dws

    rows, cols = P(("dp", "tp"), None), P("dp", "tp")
    return jax.shard_map(
        local,
        mesh=mesh,
        in_specs=(rows, rows, cols, cols, P(None, "tp"), P(None, "tp"), P("tp", None)),
        out_specs=(rows, cols, cols, rows),
        check_vma=False,
    )
```

```python
import functools

import jax
import jax.numpy as jnp
from jax import lax
from jax.experimental import pallas as pl
from jax.experimental.pallas import tpu as pltpu
from jax.sharding import PartitionSpec as P

D = 2048
F = 640
B = 512
H = 256
LAST = 16
RS = ((2, 1, 1, 0), (3, 1, 0, 1), (0, 0, 0, 0), (1, 0, 1, 1))
F32 = jnp.float32
BF16 = jnp.bfloat16
NT = (((1,), (1,)), ((), ()))
TN = (((0,), (0,)), ((), ()))
C0 = 0.7978845608028654
C1 = 0.7978845608028654 * 0.044715


def kernel(
    x_ref, dy_ref, gate_ref, up_ref, wg_ref, wu_ref, wd_ref,
    sums, rs_out, dwg_ref, dwu_ref, dwd_ref, dy_all, x_all, rs_in,
    wd, wgu, dgu, acc, tok, guv, dh, hid, p_in, p_out,
    dy_s, dy_r, dyp_r, x_s, x_r, xp_r, p_s, p_r, r_s, r_r, w_sem, t_sem, g_sem, go_chip, go_core,
):
    me = lax.axis_index("tp")
    core, iy, ix = me % 2, (me // 2) % 2, me // 4
    other = 1 - 2 * core
    partner = me + other
    ny = me + 2 - 4 * iy
    nx = me + 4 - 8 * ix
    nd = ny + 4 - 8 * ix

    place = ix + iy
    barrier = pltpu.get_barrier_semaphore()

    def signal(sem, devs):
        for d in devs:
            pl.semaphore_signal(sem, inc=1, device_id={"tp": d}, device_id_type=pl.DeviceIdType.MESH)

    @pl.when(place < 2)
    def _():
        signal(barrier, (nx, ny))

    @pl.when(core == 1)
    def _():
        signal(barrier, (partner,))

    pl.semaphore_wait(barrier, jnp.where(place == 1, 1, 2) + 1 - core)

    @pl.when(core == 0)
    def _():
        signal(go_core, (partner,))

    @pl.when(place == 2)
    def _():
        signal(go_chip, (nx, ny))

    def owner(g):
        return jnp.where(g < 2, me, jnp.where(g >= 6, nd, jnp.where(g % 2 == 0, nx, ny)))

    def half(g):
        return jnp.where(g == 4, 1, jnp.where(g == 5, 0, g % 2))

    def rows(dev, h, n=H):
        return pl.ds(pl.multiple_of(dev * B + h * H, H), n)

    def remote(src, dst, ss, rs, dev):
        return pltpu.make_async_remote_copy(
            src_ref=src, dst_ref=dst, send_sem=ss, recv_sem=rs, device_id={"tp": dev}, device_id_type=pl.DeviceIdType.MESH
        )

    def of_rows(full, n, ss, rs):
        return remote(full.at[pl.ds(0, n)], full.at[pl.ds(0, n)], ss, rs, partner)

    def start_own(ref, full, s, r, pr, to="xyp"):
        for n in range(2):
            for t in to:
                h = 1 - n if t == "y" else n
                sem, dev = {"x": (r.at[n], nx), "y": (r.at[n], ny), "p": (pr.at[0], partner)}[t]
                remote(ref.at[pl.ds(h * H, H)], full.at[rows(me, h)], s.at[0], sem, dev).start()

    def send_on(full, s, r, g, n, dev):
        q = rows(owner(g), half(g), n)
        remote(full.at[q], full.at[q], s.at[0], r, dev).start()

    def relay(full, s, r, pr, p, onward):
        of_rows(full, 2 * H, s.at[0], r.at[p - 1]).wait_recv()
        if onward:
            send_on(full, s, r.at[2], 2, H, ny)
            send_on(full, s, r.at[2], 3, H, nx)
        for g in (2 * p, 2 * p + 1):
            send_on(full, s, pr.at[p], g, H, partner)

    def from_partner(full, s, pr, p):
        of_rows(full, 2 * H, s.at[0], pr.at[p]).wait_recv()

    def load_theirs(full, g):
        src = full.at[rows(owner(g) + other, half(g))]
        pltpu.make_async_copy(src, tok.at[g % 2, pl.ds(0, H)], t_sem.at[g % 2]).start()

    def load_mine(ref, full, g):
        o, h, slot = owner(g), half(g), g % 2

        @pl.when(g < 2)
        def _():
            src = ref.at[pl.ds(pl.multiple_of(h * H, H), H)]
            pltpu.make_async_copy(src, tok.at[slot, pl.ds(H, H)], t_sem.at[slot]).start()

        @pl.when(g >= 2)
        def _():
            pltpu.make_async_copy(full.at[rows(o, h)], tok.at[slot, pl.ds(H, H)], t_sem.at[slot]).start()

    def load(ref, full, g):
        load_theirs(full, g)
        load_mine(ref, full, g)

    def loaded(slot):
        pltpu.make_async_copy(dy_all.at[pl.ds(0, B)], tok.at[slot], t_sem.at[slot]).wait()

    def load_gates(g):
        o, h = owner(g), half(g)
        for i, src in enumerate((gate_ref, up_ref)):
            pltpu.make_async_copy(src.at[rows(o + other, h)], guv.at[i, pl.ds(0, H)], g_sem.at[0]).start()
            pltpu.make_async_copy(src.at[rows(o, h)], guv.at[i, pl.ds(H, H)], g_sem.at[0]).start()

    def start_dy(to):
        start_own(dy_ref, dy_all, dy_s, dy_r, dyp_r, to)

    @pl.when(place != 1)
    def _():
        start_dy("xy")

    for i, first in ((1, "x"), (0, "y")):
        @pl.when(jnp.logical_and(place == 1, ix == i))
        def _():
            start_dy(first)

    @pl.when(core == 1)
    def _():
        pl.semaphore_wait(go_core, 1)

    start_dy("p")

    @pl.when(place == 1)
    def _():
        pl.semaphore_wait(go_chip, 1)

    for i, then in ((1, "y"), (0, "x")):
        @pl.when(jnp.logical_and(place == 1, ix == i))
        def _():
            start_dy(then)

    pltpu.make_async_copy(wd_ref, wd, w_sem.at[0]).start()
    load_gates(0)
    pltpu.make_async_copy(wg_ref, wgu.at[:, pl.ds(0, F)], w_sem.at[1]).start()
    pltpu.make_async_copy(wu_ref, wgu.at[:, pl.ds(F, F)], w_sem.at[1]).start()
    load_mine(dy_ref, dy_all, 0)
    from_partner(dy_all, dy_s, dyp_r, 0)
    load_theirs(dy_all, 0)
    acc[...] = jnp.zeros_like(acc)
    pltpu.make_async_copy(wd_ref, wd, w_sem.at[0]).wait()
    pltpu.make_async_copy(wgu, wgu, w_sem.at[1]).wait()

    def send_p(g):
        return remote(p_out.at[g % 2], p_in.at[g % 2], p_s.at[g % 2], p_r.at[g % 2], partner)

    def send_r(stage, kind, k, dev):
        return remote(rs_out.at[stage], rs_in.at[kind, k], r_s.at[kind], r_r.at[kind], dev)

    def both_r(kind):
        return remote(rs_in.at[kind], rs_in.at[kind], r_s.at[kind], r_r.at[kind], nx)

    def dx_tile(g, r0, j):
        a = dgu[pl.ds(pl.multiple_of(g * B + r0, H), H), :]
        w = wgu[pl.ds(pl.multiple_of(j * 512, 512), 512), :]
        return lax.dot_general(a, w, NT, preferred_element_type=F32)

    def first_pass(g, carry):
        slot = g % 2
        loaded(slot)
        pltpu.make_async_copy(guv, guv, g_sem.at[0]).wait()

        @pl.when(slot == 0)
        def _():
            load(dy_ref, dy_all, g + 1)

        for n0, n in ((0, 256), (256, 256), (512, 128)):
            dh[:, n0:n0 + n] = lax.dot_general(tok[slot], wd[n0:n0 + n, :], NT, preferred_element_type=F32)

        def gates(i, carry):
            r = pl.ds(pl.multiple_of(i * 32, 32), 32)
            a, u, d = guv[0, r, :].astype(F32), guv[1, r, :].astype(F32), dh[r, :]
            a2 = a * a
            t = jnp.tanh(a * (C0 + C1 * a2))
            cdf = 0.5 + 0.5 * t
            gelu = a * cdf
            slope = cdf + (0.5 * a) * ((1.0 - t * t) * (C0 + (3.0 * C1) * a2))
            hid[r, :] = (gelu * u).astype(BF16)
            q = pl.ds(pl.multiple_of(g * B + i * 32, 32), 32)
            dgu[q, 0:F] = (d * u * slope).astype(BF16)
            dgu[q, F:2 * F] = (d * gelu).astype(BF16)
            return carry

        lax.fori_loop(0, B // 32, gates, 0)

        @pl.when(g < 7)
        def _():
            load_gates(g + 1)

        @pl.when(g >= 2)
        def _():
            send_p(g - 2).wait_send()

        def p_rows(j, carry):
            p_out[slot, :, pl.ds(pl.multiple_of(j * 512, 512), 512)] = dx_tile(g, 0, j).astype(BF16)
            return carry

        lax.fori_loop(0, 4, p_rows, 0)
        send_p(g).start()

        def down(j, carry):
            s = pl.ds(pl.multiple_of(j * 512, 512), 512)
            r, c = pl.ds(pl.multiple_of((j // 2) * F, F), F), pl.ds(pl.multiple_of((j % 2) * 512, 512), 512)
            acc[r, c] += lax.dot_general(hid[...], tok[slot, :, s], TN, preferred_element_type=F32)
            return carry

        lax.fori_loop(0, 4, down, 0)

        for p in (1, 2, 3):
            @pl.when(g == 2 * p - 1)
            def _():
                relay(dy_all, dy_s, dy_r, dyp_r, p, p == 1)
                if p == 1:
                    start_own(x_ref, x_all, x_s, x_r, xp_r)
                from_partner(dy_all, dy_s, dyp_r, p)
                load(dy_ref, dy_all, g + 1)

        @pl.when(g == 7)
        def _():
            from_partner(x_all, x_s, xp_r, 0)
            load(x_ref, x_all, 0)

        send_p(g).wait_recv()

        def m_rows(j, carry):
            s = pl.ds(pl.multiple_of(j * 512, 512), 512)
            total = dx_tile(g, H, j) + p_in[slot, :, s].astype(F32)

            @pl.when(g // 2 % 2 == 0)
            def _():
                sums[g // 2 + slot, :, s] = total

            @pl.when(g // 2 % 2 == 1)
            def _():
                rs_out[jnp.where(g >= 6, g - 4, slot), :, s] = total.astype(BF16)

            return carry

        lax.fori_loop(0, 4, m_rows, 0)
        return carry

    lax.fori_loop(0, 8, first_pass, 0)

    relay(x_all, x_s, x_r, xp_r, 1, True)

    @pl.when(core == 0)
    def _():
        for stage, kind, k, dev in RS:
            send_r(stage, kind, k, (nx, ny)[dev]).start()

    for j in range(4):
        dwd_ref[:, j * 512:j * 512 + 512] = acc[j // 2 * F:j // 2 * F + F, j % 2 * 512:j % 2 * 512 + 512].astype(BF16)
    acc[...] = jnp.zeros_like(acc)

    def second_pass(g, carry):
        slot = g % 2
        loaded(slot)

        @pl.when(slot == 0)
        def _():
            load(x_ref, x_all, g + 1)

        @pl.when(g == 1)
        def _():
            from_partner(x_all, x_s, xp_r, 1)
            load(x_ref, x_all, 2)

        @pl.when(g == 3)
        def _():
            relay(x_all, x_s, x_r, xp_r, 2, False)
            from_partner(x_all, x_s, xp_r, 2)
            load(x_ref, x_all, 4)

        def weight(j, carry):
            s = pl.ds(pl.multiple_of(j * 512, 512), 512)
            d = dgu[pl.ds(pl.multiple_of(g * B, B), B), :]
            acc[s, :] += lax.dot_general(tok[slot, :, s], d, TN, preferred_element_type=F32)
            return carry

        lax.fori_loop(0, 4, weight, 0)

        @pl.when(g == 5)
        def _():
            relay(x_all, x_s, x_r, xp_r, 3, False)
            load_mine(x_ref, x_all, 6)
            from_partner(x_all, x_s, xp_r, 3)
            load_theirs(x_all, 6)

        return carry

    lax.fori_loop(0, 8, second_pass, 0)

    def weight_out(i, carry):
        r = pl.ds(pl.multiple_of(i * 32, 32), 32)
        dwg_ref[r, :] = acc[r, 0:F].astype(BF16)
        dwu_ref[r, :] = acc[r, F:2 * F].astype(BF16)
        return carry

    lax.fori_loop(0, D // 32, weight_out, 0)

    for g in (6, 7):
        send_p(g).wait_send()
    of_rows(dy_all, 14 * H, dy_s.at[0], dy_r.at[0]).wait_send()
    of_rows(x_all, 14 * H, x_s.at[0], x_r.at[0]).wait_send()

    @pl.when(core == 0)
    def _():
        for kind in range(2):
            both_r(kind).wait_send()
            both_r(kind).wait_recv()


def write_dw(dwg, dwu, dwd, dwg_ref, dwu_ref, dwd_ref, done, sem):
    copies = [
        pltpu.make_async_copy(src, dst, sem.at[i])
        for i, (src, dst) in enumerate(((dwd, dwd_ref), (dwg, dwg_ref), (dwu, dwu_ref)))
    ]
    for c in copies:
        c.start()
    done[...] = jnp.zeros_like(done)
    for c in copies:
        c.wait()


def exchange(sums, rs_out, rs_in, done, got, diag, stage, s_sem, r_sem):
    del done
    me = lax.axis_index("tp")
    core, iy, ix = me % 2, (me // 2) % 2, me // 4
    near = (me + 4 - 8 * ix, me + 2 - 4 * iy)

    barrier = pltpu.get_barrier_semaphore()
    for d in near:
        pl.semaphore_signal(barrier, inc=1, device_id={"tp": d}, device_id_type=pl.DeviceIdType.MESH)
    pl.semaphore_wait(barrier, 2)

    def remote(src, dst, i, dev):
        return pltpu.make_async_remote_copy(
            src_ref=src, dst_ref=dst, send_sem=s_sem.at[0], recv_sem=r_sem.at[i],
            device_id={"tp": dev}, device_id_type=pl.DeviceIdType.MESH,
        )

    firsts, diags = got.at[pl.ds(0, 2)], remote(diag, diag, 1, near[0])
    local = [
        pltpu.make_async_copy(rs_in.at[1], diag, r_sem.at[1]),
        pltpu.make_async_copy(rs_in.at[0], firsts, r_sem.at[0]),
    ]

    @pl.when(core == 1)
    def _():
        for st, kind, k, dev in RS:
            remote(rs_out.at[st], (firsts, diag)[kind].at[k], kind, near[dev]).start()
        diags.wait_recv()

    @pl.when(core == 0)
    def _():
        for c in local:
            c.start()
        local[0].wait()

    for k in range(2):
        def add(i, carry):
            r = pl.ds(pl.multiple_of(i * 32, 32), 32)
            stage[k, r, :] = (sums[2 + k, r, :] + diag[k, r, :].astype(F32)).astype(BF16)
            return carry

        lax.fori_loop(0, H // 32, add, 0)
        remote(stage.at[k], got.at[2 + k], 0, near[k]).start()

    for c, sent in ((0, stage), (1, got)):
        @pl.when(core == c)
        def _():
            remote(sent, sent, 0, near[0]).wait_send()
            if c == 1:
                diags.wait_send()

    remote(got, got, 0, near[0]).wait_recv()


def write_dx(sums, got, dx_ref, dx, sem):
    for q in range(B // LAST):
        h, i = q * LAST // H, q * LAST % H
        r, p = pl.ds(q * LAST, LAST), pl.ds(i, LAST)
        dx[r, :] = (sums[h, p, :] + got[h, p, :].astype(F32) + got[3 - h, p, :].astype(F32)).astype(BF16)
        pltpu.make_async_copy(dx.at[r], dx_ref.at[r], sem).start()
    pltpu.make_async_copy(dx, dx_ref, sem).wait()


def solution(mesh):
    def local(*args):
        any_ = pl.BlockSpec(memory_space=pl.ANY)
        dma = pltpu.SemaphoreType.DMA
        vmem = pl.BlockSpec(memory_space=pltpu.VMEM)
        grads = [(D, F), (D, F), (F, D)]
        def held(a):
            return pltpu.with_memory_space_constraint(a, pltpu.VMEM)

        hbm = [jax.ShapeDtypeStruct(s, BF16) for s in ((8 * B, D), (8 * B, D), (2, 2, H, D))]
        sums, rs_out, *dws, _, _, rs_in = pl.pallas_call(
            kernel,
            out_shape=[pltpu.VMEM((4, H, D), F32), pltpu.VMEM((4, H, D), BF16)]
            + [pltpu.VMEM(s, BF16) for s in grads]
            + hbm,
            in_specs=[any_] * 7,
            out_specs=[vmem] * 5 + [any_] * 3,
            scratch_shapes=[
                pltpu.VMEM((F, D), BF16),
                pltpu.VMEM((D, 2 * F), BF16),
                pltpu.VMEM((8 * B, 2 * F), BF16),
                pltpu.VMEM((D, 2 * F), F32),
                pltpu.VMEM((2, B, D), BF16),
                pltpu.VMEM((2, B, F), BF16),
                pltpu.VMEM((B, F), F32),
                pltpu.VMEM((B, F), BF16),
                pltpu.VMEM((2, H, D), BF16),
                pltpu.VMEM((2, H, D), BF16),
            ]
            + [dma((n,)) for n in (1, 3, 4, 1, 3, 4, 2, 2, 2, 2, 2, 2, 1)]
            + [pltpu.SemaphoreType.REGULAR] * 2,
            compiler_params=pltpu.CompilerParams(collective_id=0, has_side_effects=True, vmem_limit_bytes=42 * 2**20),
            name="backward",
        )(*args)
        *dws, done = pl.pallas_call(
            write_dw,
            out_shape=[jax.ShapeDtypeStruct(s, BF16) for s in grads] + [jax.ShapeDtypeStruct((8, 128), F32)],
            in_specs=[vmem] * 3,
            out_specs=[any_] * 3 + [vmem],
            scratch_shapes=[dma((3,))],
            compiler_params=pltpu.CompilerParams(vmem_limit_bytes=16 * 2**20),
            name="write_dw",
        )(*map(held, dws))
        got = pl.pallas_call(
            exchange,
            out_shape=pltpu.VMEM((4, H, D), BF16),
            in_specs=[vmem, vmem, pl.BlockSpec(memory_space=pltpu.HBM), vmem],
            out_specs=vmem,
            scratch_shapes=[pltpu.VMEM((2, H, D), BF16)] * 2 + [dma((1,)), dma((2,))],
            compiler_params=pltpu.CompilerParams(collective_id=1, has_side_effects=True, vmem_limit_bytes=24 * 2**20),
            name="exchange",
        )(held(sums), held(rs_out), pltpu.with_memory_space_constraint(rs_in, pltpu.HBM), held(done))
        dx = pl.pallas_call(
            write_dx,
            out_shape=jax.ShapeDtypeStruct((B, D), BF16),
            in_specs=[vmem] * 2,
            out_specs=any_,
            scratch_shapes=[pltpu.VMEM((B, D), BF16), dma],
            compiler_params=pltpu.CompilerParams(vmem_limit_bytes=16 * 2**20),
            name="write_dx",
        )(held(sums), held(got))
        return dx, *dws

    rows, cols = P(("dp", "tp"), None), P("dp", "tp")
    return jax.shard_map(
        local,
        mesh=mesh,
        in_specs=(rows, rows, cols, cols, P(None, "tp"), P(None, "tp"), P("tp", None)),
        out_specs=(rows, cols, cols, rows),
        check_vma=False,
    )
```

```python
import functools

import jax
import jax.numpy as jnp
from jax import lax
from jax.experimental import pallas as pl
from jax.experimental.pallas import tpu as pltpu
from jax.sharding import PartitionSpec as P

D = 2048
F = 640
B = 512
H = 256
LAST = 16
RS = ((2, 1, 1, 0), (3, 1, 0, 1), (0, 0, 0, 0), (1, 0, 1, 1))
F32 = jnp.float32
BF16 = jnp.bfloat16
NT = (((1,), (1,)), ((), ()))
TN = (((0,), (0,)), ((), ()))
C0 = 0.7978845608028654
C1 = 0.7978845608028654 * 0.044715


def kernel(
    x_ref, dy_ref, gate_ref, up_ref, wg_ref, wu_ref, wd_ref,
    sums, rs_out, dwg_ref, dwu_ref, dwd_ref, dy_all, x_all, rs_in,
    wd, wgu, dgu, acc, tok, guv, dh, hid, p_in, p_out,
    dy_s, dy_r, dyp_r, x_s, x_r, xp_r, p_s, p_r, r_s, r_r, w_sem, t_sem, g_sem, go_chip, go_core,
):
    me = lax.axis_index("tp")
    core, iy, ix = me % 2, (me // 2) % 2, me // 4
    other = 1 - 2 * core
    partner = me + other
    ny = me + 2 - 4 * iy
    nx = me + 4 - 8 * ix
    nd = ny + 4 - 8 * ix

    place = ix + iy
    barrier = pltpu.get_barrier_semaphore()

    def signal(sem, devs):
        for d in devs:
            pl.semaphore_signal(sem, inc=1, device_id={"tp": d}, device_id_type=pl.DeviceIdType.MESH)

    @pl.when(place < 2)
    def _():
        signal(barrier, (nx, ny))

    @pl.when(core == 1)
    def _():
        signal(barrier, (partner,))

    pl.semaphore_wait(barrier, jnp.where(place == 1, 1, 2) + 1 - core)

    @pl.when(core == 0)
    def _():
        signal(go_core, (partner,))

    @pl.when(place == 2)
    def _():
        signal(go_chip, (nx, ny))

    def owner(g):
        return jnp.where(g < 2, me, jnp.where(g >= 6, nd, jnp.where(g % 2 == 0, nx, ny)))

    def half(g):
        return jnp.where(g == 4, 1, jnp.where(g == 5, 0, g % 2))

    def rows(dev, h, n=H):
        return pl.ds(pl.multiple_of(dev * B + h * H, H), n)

    def remote(src, dst, ss, rs, dev):
        return pltpu.make_async_remote_copy(
            src_ref=src, dst_ref=dst, send_sem=ss, recv_sem=rs, device_id={"tp": dev}, device_id_type=pl.DeviceIdType.MESH
        )

    def of_rows(full, n, ss, rs):
        return remote(full.at[pl.ds(0, n)], full.at[pl.ds(0, n)], ss, rs, partner)

    def start_own(ref, full, s, r, pr, to="xyp"):
        for n in range(2):
            for t in to:
                h = 1 - n if t == "y" else n
                sem, dev = {"x": (r.at[n], nx), "y": (r.at[n], ny), "p": (pr.at[0], partner)}[t]
                remote(ref.at[pl.ds(h * H, H)], full.at[rows(me, h)], s.at[0], sem, dev).start()

    def send_on(full, s, r, g, n, dev):
        q = rows(owner(g), half(g), n)
        remote(full.at[q], full.at[q], s.at[0], r, dev).start()

    def relay(full, s, r, pr, p, onward):
        of_rows(full, 2 * H, s.at[0], r.at[p - 1]).wait_recv()
        if onward:
            send_on(full, s, r.at[2], 2, H, ny)
            send_on(full, s, r.at[2], 3, H, nx)
        for g in (2 * p, 2 * p + 1):
            send_on(full, s, pr.at[p], g, H, partner)

    def from_partner(full, s, pr, p):
        of_rows(full, 2 * H, s.at[0], pr.at[p]).wait_recv()

    def load_theirs(full, g):
        src = full.at[rows(owner(g) + other, half(g))]
        pltpu.make_async_copy(src, tok.at[g % 2, pl.ds(0, H)], t_sem.at[g % 2]).start()

    def load_mine(ref, full, g):
        o, h, slot = owner(g), half(g), g % 2

        @pl.when(g < 2)
        def _():
            src = ref.at[pl.ds(pl.multiple_of(h * H, H), H)]
            pltpu.make_async_copy(src, tok.at[slot, pl.ds(H, H)], t_sem.at[slot]).start()

        @pl.when(g >= 2)
        def _():
            pltpu.make_async_copy(full.at[rows(o, h)], tok.at[slot, pl.ds(H, H)], t_sem.at[slot]).start()

    def load(ref, full, g):
        load_theirs(full, g)
        load_mine(ref, full, g)

    def loaded(slot):
        pltpu.make_async_copy(dy_all.at[pl.ds(0, B)], tok.at[slot], t_sem.at[slot]).wait()

    def load_gates(g):
        o, h = owner(g), half(g)
        for i, src in enumerate((gate_ref, up_ref)):
            pltpu.make_async_copy(src.at[rows(o + other, h)], guv.at[i, pl.ds(0, H)], g_sem.at[0]).start()
            pltpu.make_async_copy(src.at[rows(o, h)], guv.at[i, pl.ds(H, H)], g_sem.at[0]).start()

    def start_dy(to):
        start_own(dy_ref, dy_all, dy_s, dy_r, dyp_r, to)

    @pl.when(place != 1)
    def _():
        start_dy("xy")

    for i, first in ((1, "x"), (0, "y")):
        @pl.when(jnp.logical_and(place == 1, ix == i))
        def _():
            start_dy(first)

    @pl.when(core == 1)
    def _():
        pl.semaphore_wait(go_core, 1)

    start_dy("p")

    @pl.when(place == 1)
    def _():
        pl.semaphore_wait(go_chip, 1)

    for i, then in ((1, "y"), (0, "x")):
        @pl.when(jnp.logical_and(place == 1, ix == i))
        def _():
            start_dy(then)

    pltpu.make_async_copy(wd_ref, wd, w_sem.at[0]).start()
    load_gates(0)
    pltpu.make_async_copy(wg_ref, wgu.at[:, pl.ds(0, F)], w_sem.at[1]).start()
    pltpu.make_async_copy(wu_ref, wgu.at[:, pl.ds(F, F)], w_sem.at[1]).start()
    from_partner(dy_all, dy_s, dyp_r, 0)
    load(dy_ref, dy_all, 0)
    acc[...] = jnp.zeros_like(acc)
    pltpu.make_async_copy(wd_ref, wd, w_sem.at[0]).wait()
    pltpu.make_async_copy(wgu, wgu, w_sem.at[1]).wait()

    def send_p(g):
        return remote(p_out.at[g % 2], p_in.at[g % 2], p_s.at[g % 2], p_r.at[g % 2], partner)

    def send_r(stage, kind, k, dev):
        return remote(rs_out.at[stage], rs_in.at[kind, k], r_s.at[kind], r_r.at[kind], dev)

    def both_r(kind):
        return remote(rs_in.at[kind], rs_in.at[kind], r_s.at[kind], r_r.at[kind], nx)

    def dx_tile(g, r0, j):
        a = dgu[pl.ds(pl.multiple_of(g * B + r0, H), H), :]
        w = wgu[pl.ds(pl.multiple_of(j * 512, 512), 512), :]
        return lax.dot_general(a, w, NT, preferred_element_type=F32)

    def first_pass(g, carry):
        slot = g % 2
        loaded(slot)
        pltpu.make_async_copy(guv, guv, g_sem.at[0]).wait()

        @pl.when(slot == 0)
        def _():
            load(dy_ref, dy_all, g + 1)

        for n0, n in ((0, 256), (256, 256), (512, 128)):
            dh[:, n0:n0 + n] = lax.dot_general(tok[slot], wd[n0:n0 + n, :], NT, preferred_element_type=F32)

        def gates(i, carry):
            r = pl.ds(pl.multiple_of(i * 32, 32), 32)
            a, u, d = guv[0, r, :].astype(F32), guv[1, r, :].astype(F32), dh[r, :]
            a2 = a * a
            t = jnp.tanh(a * (C0 + C1 * a2))
            cdf = 0.5 + 0.5 * t
            gelu = a * cdf
            slope = cdf + (0.5 * a) * ((1.0 - t * t) * (C0 + (3.0 * C1) * a2))
            hid[r, :] = (gelu * u).astype(BF16)
            q = pl.ds(pl.multiple_of(g * B + i * 32, 32), 32)
            dgu[q, 0:F] = (d * u * slope).astype(BF16)
            dgu[q, F:2 * F] = (d * gelu).astype(BF16)
            return carry

        lax.fori_loop(0, B // 32, gates, 0)

        @pl.when(g < 7)
        def _():
            load_gates(g + 1)

        @pl.when(g >= 2)
        def _():
            send_p(g - 2).wait_send()

        def p_rows(j, carry):
            p_out[slot, :, pl.ds(pl.multiple_of(j * 512, 512), 512)] = dx_tile(g, 0, j).astype(BF16)
            return carry

        lax.fori_loop(0, 4, p_rows, 0)
        send_p(g).start()

        def down(j, carry):
            s = pl.ds(pl.multiple_of(j * 512, 512), 512)
            r, c = pl.ds(pl.multiple_of((j // 2) * F, F), F), pl.ds(pl.multiple_of((j % 2) * 512, 512), 512)
            acc[r, c] += lax.dot_general(hid[...], tok[slot, :, s], TN, preferred_element_type=F32)
            return carry

        lax.fori_loop(0, 4, down, 0)

        for p in (1, 2, 3):
            @pl.when(g == 2 * p - 1)
            def _():
                relay(dy_all, dy_s, dy_r, dyp_r, p, p == 1)
                if p == 1:
                    start_own(x_ref, x_all, x_s, x_r, xp_r)
                from_partner(dy_all, dy_s, dyp_r, p)
                load(dy_ref, dy_all, g + 1)

        @pl.when(g == 7)
        def _():
            from_partner(x_all, x_s, xp_r, 0)
            load(x_ref, x_all, 0)

        send_p(g).wait_recv()

        def m_rows(j, carry):
            s = pl.ds(pl.multiple_of(j * 512, 512), 512)
            total = dx_tile(g, H, j) + p_in[slot, :, s].astype(F32)

            @pl.when(g // 2 % 2 == 0)
            def _():
                sums[g // 2 + slot, :, s] = total

            @pl.when(g // 2 % 2 == 1)
            def _():
                rs_out[jnp.where(g >= 6, g - 4, slot), :, s] = total.astype(BF16)

            return carry

        lax.fori_loop(0, 4, m_rows, 0)
        return carry

    lax.fori_loop(0, 8, first_pass, 0)

    relay(x_all, x_s, x_r, xp_r, 1, True)

    @pl.when(core == 0)
    def _():
        for stage, kind, k, dev in RS:
            send_r(stage, kind, k, (nx, ny)[dev]).start()

    for j in range(4):
        dwd_ref[:, j * 512:j * 512 + 512] = acc[j // 2 * F:j // 2 * F + F, j % 2 * 512:j % 2 * 512 + 512].astype(BF16)
    acc[...] = jnp.zeros_like(acc)

    def second_pass(g, carry):
        slot = g % 2
        loaded(slot)

        @pl.when(slot == 0)
        def _():
            load(x_ref, x_all, g + 1)

        @pl.when(g == 1)
        def _():
            from_partner(x_all, x_s, xp_r, 1)
            load(x_ref, x_all, 2)

        @pl.when(g == 3)
        def _():
            relay(x_all, x_s, x_r, xp_r, 2, False)
            from_partner(x_all, x_s, xp_r, 2)
            load(x_ref, x_all, 4)

        def weight(j, carry):
            s = pl.ds(pl.multiple_of(j * 512, 512), 512)
            d = dgu[pl.ds(pl.multiple_of(g * B, B), B), :]
            acc[s, :] += lax.dot_general(tok[slot, :, s], d, TN, preferred_element_type=F32)
            return carry

        lax.fori_loop(0, 4, weight, 0)

        @pl.when(g == 5)
        def _():
            relay(x_all, x_s, x_r, xp_r, 3, False)
            load_mine(x_ref, x_all, 6)
            from_partner(x_all, x_s, xp_r, 3)
            load_theirs(x_all, 6)

        return carry

    lax.fori_loop(0, 8, second_pass, 0)

    def weight_out(i, carry):
        r = pl.ds(pl.multiple_of(i * 32, 32), 32)
        dwg_ref[r, :] = acc[r, 0:F].astype(BF16)
        dwu_ref[r, :] = acc[r, F:2 * F].astype(BF16)
        return carry

    lax.fori_loop(0, D // 32, weight_out, 0)

    for g in (6, 7):
        send_p(g).wait_send()
    of_rows(dy_all, 14 * H, dy_s.at[0], dy_r.at[0]).wait_send()
    of_rows(x_all, 14 * H, x_s.at[0], x_r.at[0]).wait_send()

    @pl.when(core == 0)
    def _():
        for kind in range(2):
            both_r(kind).wait_send()
            both_r(kind).wait_recv()


def write_dw(dwg, dwu, dwd, dwg_ref, dwu_ref, dwd_ref, done, sem):
    copies = [
        pltpu.make_async_copy(src, dst, sem.at[i])
        for i, (src, dst) in enumerate(((dwd, dwd_ref), (dwg, dwg_ref), (dwu, dwu_ref)))
    ]
    for c in copies:
        c.start()
    done[...] = jnp.zeros_like(done)
    for c in copies:
        c.wait()


def exchange(sums, rs_out, rs_in, done, got, diag, stage, s_sem, r_sem):
    del done
    me = lax.axis_index("tp")
    core, iy, ix = me % 2, (me // 2) % 2, me // 4
    near = (me + 4 - 8 * ix, me + 2 - 4 * iy)

    barrier = pltpu.get_barrier_semaphore()
    for d in near:
        pl.semaphore_signal(barrier, inc=1, device_id={"tp": d}, device_id_type=pl.DeviceIdType.MESH)
    pl.semaphore_wait(barrier, 2)

    def remote(src, dst, i, dev):
        return pltpu.make_async_remote_copy(
            src_ref=src, dst_ref=dst, send_sem=s_sem.at[0], recv_sem=r_sem.at[i],
            device_id={"tp": dev}, device_id_type=pl.DeviceIdType.MESH,
        )

    firsts, diags = got.at[pl.ds(0, 2)], remote(diag, diag, 1, near[0])
    local = [
        pltpu.make_async_copy(rs_in.at[1], diag, r_sem.at[1]),
        pltpu.make_async_copy(rs_in.at[0], firsts, r_sem.at[0]),
    ]

    @pl.when(core == 1)
    def _():
        for st, kind, k, dev in RS:
            remote(rs_out.at[st], (firsts, diag)[kind].at[k], kind, near[dev]).start()
        diags.wait_recv()

    @pl.when(core == 0)
    def _():
        for c in local:
            c.start()
        local[0].wait()

    for k in range(2):
        def add(i, carry):
            r = pl.ds(pl.multiple_of(i * 32, 32), 32)
            stage[k, r, :] = (sums[2 + k, r, :] + diag[k, r, :].astype(F32)).astype(BF16)
            return carry

        lax.fori_loop(0, H // 32, add, 0)
        remote(stage.at[k], got.at[2 + k], 0, near[k]).start()

    for c, sent in ((0, stage), (1, got)):
        @pl.when(core == c)
        def _():
            remote(sent, sent, 0, near[0]).wait_send()
            if c == 1:
                diags.wait_send()

    remote(got, got, 0, near[0]).wait_recv()


def write_dx(sums, got, dx_ref, dx, sem):
    for q in range(B // LAST):
        h, i = q * LAST // H, q * LAST % H
        r, p = pl.ds(q * LAST, LAST), pl.ds(i, LAST)
        dx[r, :] = (sums[h, p, :] + got[h, p, :].astype(F32) + got[3 - h, p, :].astype(F32)).astype(BF16)
        pltpu.make_async_copy(dx.at[r], dx_ref.at[r], sem).start()
    pltpu.make_async_copy(dx, dx_ref, sem).wait()


def solution(mesh):
    def local(*args):
        any_ = pl.BlockSpec(memory_space=pl.ANY)
        dma = pltpu.SemaphoreType.DMA
        vmem = pl.BlockSpec(memory_space=pltpu.VMEM)
        grads = [(D, F), (D, F), (F, D)]
        def held(a):
            return pltpu.with_memory_space_constraint(a, pltpu.VMEM)

        hbm = [jax.ShapeDtypeStruct(s, BF16) for s in ((8 * B, D), (8 * B, D), (2, 2, H, D))]
        sums, rs_out, *dws, _, _, rs_in = pl.pallas_call(
            kernel,
            out_shape=[pltpu.VMEM((4, H, D), F32), pltpu.VMEM((4, H, D), BF16)]
            + [pltpu.VMEM(s, BF16) for s in grads]
            + hbm,
            in_specs=[any_] * 7,
            out_specs=[vmem] * 5 + [any_] * 3,
            scratch_shapes=[
                pltpu.VMEM((F, D), BF16),
                pltpu.VMEM((D, 2 * F), BF16),
                pltpu.VMEM((8 * B, 2 * F), BF16),
                pltpu.VMEM((D, 2 * F), F32),
                pltpu.VMEM((2, B, D), BF16),
                pltpu.VMEM((2, B, F), BF16),
                pltpu.VMEM((B, F), F32),
                pltpu.VMEM((B, F), BF16),
                pltpu.VMEM((2, H, D), BF16),
                pltpu.VMEM((2, H, D), BF16),
            ]
            + [dma((n,)) for n in (1, 3, 4, 1, 3, 4, 2, 2, 2, 2, 2, 2, 1)]
            + [pltpu.SemaphoreType.REGULAR] * 2,
            compiler_params=pltpu.CompilerParams(collective_id=0, has_side_effects=True, vmem_limit_bytes=42 * 2**20),
            name="backward",
        )(*args)
        *dws, done = pl.pallas_call(
            write_dw,
            out_shape=[jax.ShapeDtypeStruct(s, BF16) for s in grads] + [jax.ShapeDtypeStruct((8, 128), F32)],
            in_specs=[vmem] * 3,
            out_specs=[any_] * 3 + [vmem],
            scratch_shapes=[dma((3,))],
            compiler_params=pltpu.CompilerParams(vmem_limit_bytes=16 * 2**20),
            name="write_dw",
        )(*map(held, dws))
        got = pl.pallas_call(
            exchange,
            out_shape=pltpu.VMEM((4, H, D), BF16),
            in_specs=[vmem, vmem, pl.BlockSpec(memory_space=pltpu.HBM), vmem],
            out_specs=vmem,
            scratch_shapes=[pltpu.VMEM((2, H, D), BF16)] * 2 + [dma((1,)), dma((2,))],
            compiler_params=pltpu.CompilerParams(collective_id=1, has_side_effects=True, vmem_limit_bytes=24 * 2**20),
            name="exchange",
        )(held(sums), held(rs_out), pltpu.with_memory_space_constraint(rs_in, pltpu.HBM), held(done))
        dx = pl.pallas_call(
            write_dx,
            out_shape=jax.ShapeDtypeStruct((B, D), BF16),
            in_specs=[vmem] * 2,
            out_specs=any_,
            scratch_shapes=[pltpu.VMEM((B, D), BF16), dma],
            compiler_params=pltpu.CompilerParams(vmem_limit_bytes=16 * 2**20),
            name="write_dx",
        )(held(sums), held(got))
        return dx, *dws

    rows, cols = P(("dp", "tp"), None), P("dp", "tp")
    return jax.shard_map(
        local,
        mesh=mesh,
        in_specs=(rows, rows, cols, cols, P(None, "tp"), P(None, "tp"), P("tp", None)),
        out_specs=(rows, cols, cols, rows),
        check_vma=False,
    )
```
